512 devices in a mesh: rep: 8 (over x, y_hi), amp: 64 (over y_lo, z, core).
Axes of the slice: x: 4, y: 8 (y_hi: 2, y_lo: 4; y = y_hi * 4 + y_lo), z: 8, core: 2. Of those that a mesh axis runs over, the one named last changes fastest.
Arguments:
- amplitudes: float32 [2, 16777216], P(None, ('rep', 'amp')), parts along dimension 1, may hold values from -12 to 12
- coupling_index: int32 [16, 20], P('rep'), parts along dimension 0, may hold values from 0 to 15
- rotation_index: int32 [16, 21], P('rep'), parts along dimension 0, may hold values from 0 to 15
- chain_order: int32 [21], replicated, may hold values from 0 to 20, each once
- bond_sign: int32 [20], replicated, may hold values 0 or 1
Outputs:
- final_state: float32 [2, 16777216], P(None, ('rep', 'amp')), parts along dimension 1
- energies: float32 [16], P('rep'), parts along dimension 0
The draws below stay inside these ranges and needn't reach their ends.
There are 8 independent parts, one for each index of `rep`. The reference program is written for one: setup_inputs(seed, part) draws one part's arguments, and reference() takes and returns one part's arrays. A program takes and returns all parts, laid end to end along the dimension named above; an argument that names none is the same for every part. Nothing has to cross between parts.
Inputs may be any that keep to these rules, and one draw needn't show every extreme that they name: chain_order holds each of 0 to 20 once.
All inputs are finite; a program needn't handle non-finite values.
Results may differ from the reference program's by a relative error of at most 0.0003.
Values sent between devices are 32-bit elements; how exact they have to be, the bound alone decides.
No kernel may reach another device: no remote copies, remote signals or barrier semaphores. Data moves between devices by JAX's collectives and lax.ppermute only.
A program may use at most 128 MiB of HBM per device.

```python
import jax
import jax.numpy as jnp
from jax import lax

LQ = 15
NQ = 21
AMPS = 2097152
LAYERS = 2
ANGLES = 16


def draw_amplitudes(key, part):
    devices_count = AMPS // 2 ** LQ
    owner = jnp.arange(AMPS, dtype=jnp.int32) // 2 ** LQ
    ramp = owner.astype(jnp.float32) / jnp.float32(max(devices_count - 1, 1))
    values = jnp.clip(jax.random.normal(key, (2, AMPS), jnp.float32), -4.0, 4.0)
    scaling = 1.0 + 2.0 * ramp
    return (values * scaling[None, :]).astype(jnp.float32)


def with_ends(entries, own_key, least, largest):
    extent = entries.shape
    place = [jax.random.randint(jax.random.fold_in(own_key, axis), (), 0, extent[axis]) for axis in range(len(extent))]
    entries = entries.at[tuple(place)].set(least)
    longest = extent.index(max(extent))
    place[longest] = (place[longest] + 1) % extent[longest]
    return entries.at[tuple(place)].set(largest)


def setup_inputs(seed: int = 0, part: int = 0) -> dict:
    key_list = jax.random.split(jax.random.key(seed), 6)
    part_splits = jax.random.split(jax.random.fold_in(key_list[5], part), 6)
    return {
        "amplitudes": draw_amplitudes(jax.random.fold_in(jax.random.fold_in(key_list[5], part), 71), part),
        "coupling_index": with_ends(jax.random.randint(part_splits[1], (LAYERS, NQ - 1), 0, ANGLES), jax.random.fold_in(part_splits[1], 1), 0, ANGLES - 1).astype(jnp.int32),
        "rotation_index": with_ends(jax.random.randint(part_splits[2], (LAYERS, NQ), 0, ANGLES), jax.random.fold_in(part_splits[2], 1), 0, ANGLES - 1).astype(jnp.int32),
        "chain_order": jax.random.permutation(key_list[3], NQ).astype(jnp.int32),
        "bond_sign": with_ends((jax.random.randint(key_list[4], (NQ - 1,), 0, 4) < 3).astype(jnp.int32), jax.random.fold_in(key_list[4], 1), 0, 1),
    }


def angle_table():
    return (jnp.arange(ANGLES, dtype=jnp.float32) + 1.0) * (jnp.float32(jnp.pi) / (2.0 * (ANGLES + 1)))

def lookup(index):
    hits = index[..., None] == jnp.arange(ANGLES, dtype=jnp.int32)
    return lax.optimization_barrier(jnp.sum(jnp.where(hits, angle_table(), jnp.float32(0.0)), axis=-1))

def reference(amplitudes, coupling_index, rotation_index, chain_order, bond_sign):
    bond_signs = (2 * bond_sign - 1).astype(jnp.float32)
    couple_angles = lookup(coupling_index) * bond_signs[None, :]
    turn_angles = lookup(rotation_index)
    positions = jnp.arange(AMPS, dtype=jnp.int32)
    energy_field = jnp.zeros((AMPS,), jnp.float32)
    phase_fields = [jnp.zeros((AMPS,), jnp.float32) for layer_index in range(LAYERS)]
    for bond_index in range(NQ - 1):
        differ = jnp.right_shift(positions, chain_order[bond_index]) ^ jnp.right_shift(positions, chain_order[bond_index + 1])
        parity_sign = (1 - 2 * (differ & 1)).astype(jnp.float32)
        energy_field = energy_field + bond_signs[bond_index] * parity_sign
        for layer_index in range(LAYERS):
            phase_fields[layer_index] = phase_fields[layer_index] + couple_angles[layer_index, bond_index] * parity_sign
    total_norm = jnp.sum(amplitudes * amplitudes)
    factor = 1.0 / jnp.sqrt(total_norm / AMPS + 1e-06)
    real_part = amplitudes[0] * factor
    imag_part = amplitudes[1] * factor
    energies = []
    for layer_index in range(LAYERS):
        cosine = jnp.cos(phase_fields[layer_index])
        sine_part = jnp.sin(phase_fields[layer_index])
        real_part, imag_part = (cosine * real_part + sine_part * imag_part, cosine * imag_part - sine_part * real_part)
        for qubit in range(NQ):
            cosine = jnp.cos(turn_angles[layer_index, qubit])
            sine_part = jnp.sin(turn_angles[layer_index, qubit])
            shape = (AMPS // 2 ** (qubit + 1), 2, 2 ** qubit)
            real_view = real_part.reshape(shape)
            imag_view = imag_part.reshape(shape)
            real_low, real_high = (real_view[:, 0], real_view[:, 1])
            imag_low, imag_high = (imag_view[:, 0], imag_view[:, 1])
            new_real = jnp.stack([cosine * real_low + sine_part * imag_high, cosine * real_high + sine_part * imag_low], axis=1)
            new_imag = jnp.stack([cosine * imag_low - sine_part * real_high, cosine * imag_high - sine_part * real_low], axis=1)
            real_part = new_real.reshape(AMPS)
            imag_part = new_imag.reshape(AMPS)
        weight = real_part * real_part + imag_part * imag_part
        energies.append(jnp.sum(weight * energy_field) / AMPS)
    return (jnp.stack([real_part, imag_part]), jnp.stack(energies))
```

```python
import numpy as np
import jax
import jax.numpy as jnp
from jax import lax
from jax.experimental import pallas as pl
from jax.experimental.pallas import tpu as pltpu
from jax.sharding import PartitionSpec as P

LAYERS = 2
ANGLES = 16
UNITS = 2 * (ANGLES + 1)
LANE_BITS = 7
LANES = 128

F32 = jnp.float32
BF16 = jnp.bfloat16


def angle_tables():
    steps = (np.arange(ANGLES, dtype=np.float64) + 1.0) * (np.pi / UNITS)
    return np.stack([np.cos(steps), np.sin(steps)]).astype(np.float32)


def iota(shape, dimension):
    return lax.broadcasted_iota(jnp.int32, shape, dimension)


def bit_count(values, width):
    total = values & 1
    for bit in range(1, width):
        total = total + ((values >> bit) & 1)
    return total


def split(values):
    high = values.astype(BF16)
    return high, (values - high.astype(F32)).astype(BF16)


def dot(left, right):
    return jnp.dot(left, right, preferred_element_type=F32)


def product(left, right):
    return dot(left[0], right[0]) + (dot(left[0], right[1]) + dot(left[1], right[0]))


def rotation(size, first, pairs):
    row, column = iota((size, size), 0), iota((size, size), 1)
    differ = row ^ column
    matrix = None
    for at, (cosine, sine) in enumerate(pairs):
        bit = first + at
        here = (differ >> bit) & 1
        low = jnp.where(((row >> bit) & 1) == 1, -sine, sine)
        factor = jnp.where(here == 1, low, cosine)
        matrix = factor if matrix is None else matrix * factor
    if first:
        matrix = jnp.where((differ & (2**first - 1)) == 0, matrix, 0.0)
    return matrix


def row_rotation(bits, first, pairs):
    half = rotation(2 ** (bits - 1), first, pairs[:-1])
    cosine, sine = pairs[-1]
    return jnp.concatenate(
        [
            jnp.concatenate([cosine * half, sine * half], axis=1),
            jnp.concatenate([-sine * half, cosine * half], axis=1),
        ],
        axis=0,
    )


def pair_of(layer, rotation_ref, table_ref, qubit):
    index = rotation_ref[layer, qubit]
    return table_ref[0, index], table_ref[1, index]


def signs(index, chain_ref, bonds):
    first, second = chain_ref[:, 0:bonds], chain_ref[:, 1 : bonds + 1]
    differ = (index >> first) ^ (index >> second)
    return (1 - 2 * (differ & 1)).astype(F32)


def fields(weights, index_rows, chain_ref, bonds):
    row_signs = signs(index_rows, chain_ref, bonds)
    lane_signs = signs(iota((LANES, bonds), 0), chain_ref, bonds).astype(BF16)
    rows = index_rows.shape[0]
    stacked = jnp.concatenate([(w * row_signs).astype(BF16) for w in weights], axis=0)
    out = lax.dot_general(
        stacked, lane_signs, (((1,), (1,)), ((), ())), preferred_element_type=F32
    )
    return [out[k * rows : (k + 1) * rows] for k in range(len(weights))]


def cos_sin(steps):
    quarter = UNITS // 2
    turns = jnp.floor(steps * (1.0 / quarter) + 0.5)
    angle = (steps - turns * quarter) * (np.pi / UNITS)
    square = angle * angle
    sine = angle * (
        1.0 + square * (-1.0 / 6 + square * (1.0 / 120 + square * (-1.0 / 5040 + square * (1.0 / 362880))))
    )
    cosine = 1.0 + square * (
        -0.5 + square * (1.0 / 24 + square * (-1.0 / 720 + square * (1.0 / 40320)))
    )
    turns = turns.astype(jnp.int32)
    odd = (turns & 1) == 1
    cosine, sine = jnp.where(odd, sine, cosine), jnp.where(odd, cosine, sine)
    return (
        jnp.where(((turns + 1) & 2) == 2, -cosine, cosine),
        jnp.where((turns & 2) == 2, -sine, sine),
    )


def evens(ref):
    half = ref.shape[0] // 2
    return ref[pl.ds(0, half, stride=2), :], ref[pl.ds(1, half, stride=2), :]


def put(ref, real, imag):
    half = ref.shape[0] // 2
    ref[pl.ds(0, half, stride=2), :] = real
    ref[pl.ds(1, half, stride=2), :] = imag


def by_rows(gate, real, imag):
    both = product(gate, split(jnp.concatenate([real, imag], axis=1)))
    return both[:, :LANES], both[:, LANES:]


def by_lanes(gate, real, imag):
    rows = real.shape[0]
    both = product(split(jnp.concatenate([real, imag], axis=0)), gate)
    return both[:rows], both[rows:]


class Plan:
    def __init__(self, local_bits, global_bits):
        self.local_bits, self.global_bits = local_bits, global_bits
        self.qubits = local_bits + global_bits
        self.rows = 2 ** (local_bits - LANE_BITS)
        self.row_bits = local_bits - LANE_BITS
        self.kept = self.row_bits - global_bits
        self.bonds = self.qubits - 1

    def rows_plain(self, device, bonds):
        return (iota((self.rows, bonds), 0) << LANE_BITS) | (device << self.local_bits)

    def rows_moved(self, device, bonds):
        row = iota((self.rows, bonds), 0)
        low = (row & (2**self.kept - 1)) << LANE_BITS
        return low | ((row >> self.kept) << self.local_bits) | (device << (LANE_BITS + self.kept))

    def row_qubits(self, moved):
        low = [LANE_BITS + k for k in range(self.kept)]
        start = self.local_bits if moved else LANE_BITS + self.kept
        return low + [start + k for k in range(self.global_bits)]


def first_kernel(plan, rotation_ref, table_ref, chain_ref, coupling_ref, bond_ref, amps_ref, out_ref, norm_ref):
    device = lax.axis_index("amp")
    bonds = plan.bonds
    bond_signs = (2 * bond_ref[...] - 1).astype(F32)
    weight = (coupling_ref[0:1, :] + 1).astype(F32) * bond_signs
    (steps,) = fields([weight], plan.rows_plain(device, bonds), chain_ref, bonds)
    ones = bit_count(iota((plan.rows, LANES), 0), plan.row_bits) + bit_count(
        iota((plan.rows, LANES), 1), LANE_BITS
    )
    ones = ones + bit_count(device, plan.global_bits)
    steps = steps + (UNITS // 2) * ones.astype(F32)
    cosine, sine = cos_sin(steps)
    pairs = lambda qs: [pair_of(0, rotation_ref, table_ref, q) for q in qs]
    row_gate = split(row_rotation(plan.row_bits, 0, pairs(plan.row_qubits(False))))
    lane_gate = split(rotation(LANES, 0, [(c, -s) for c, s in pairs(range(LANE_BITS))]))
    real, imag = evens(amps_ref)
    norm_ref[...] = jnp.sum((real * real + imag * imag).reshape(-1, 8, LANES), axis=0)
    real, imag = cosine * real + sine * imag, cosine * imag - sine * real
    real, imag = by_lanes(lane_gate, *by_rows(row_gate, real, imag))
    put(out_ref, real, imag)


def prepare_kernel(
    plan, rotation_ref, table_ref, chain_ref, coupling_ref, bond_ref,
    cosine_ref, sine_ref, moved_ref, plain_ref, *gate_refs,
):
    device = lax.axis_index("amp")
    bonds = plan.bonds
    bond_signs = (2 * bond_ref[...] - 1).astype(F32)
    weight = (coupling_ref[1:2, :] + 1).astype(F32) * bond_signs
    steps, moved = fields([weight, bond_signs], plan.rows_moved(device, bonds), chain_ref, bonds)
    cosine_ref[...], sine_ref[...] = cos_sin(steps)
    moved_ref[...] = moved
    (plain_ref[...],) = fields([bond_signs], plan.rows_plain(device, bonds), chain_ref, bonds)
    pairs = lambda layer, qs: [pair_of(layer, rotation_ref, table_ref, q) for q in qs]
    kept = plan.kept
    gates = [
        row_rotation(plan.row_bits, kept, pairs(0, plan.row_qubits(True)[kept:])),
        row_rotation(plan.row_bits, 0, pairs(1, plan.row_qubits(True))),
        rotation(LANES, 0, [(c, -s) for c, s in pairs(1, range(LANE_BITS))]),
        row_rotation(plan.row_bits, kept, pairs(1, plan.row_qubits(False)[kept:])),
    ]
    for k, gate in enumerate(gates):
        gate_refs[2 * k][...], gate_refs[2 * k + 1][...] = split(gate)


def energy(real, imag, field):
    return jnp.sum(((real * real + imag * imag) * field).reshape(-1, 8, LANES), axis=0)


def middle_kernel(state_ref, cosine_ref, sine_ref, moved_ref, *refs):
    (ga, gb, ha, hb, la, lb), (out_ref, energy_ref) = refs[:6], refs[6:]
    real, imag = by_rows((ga[...], gb[...]), *evens(state_ref))
    energy_ref[...] = energy(real, imag, moved_ref[...])
    cosine, sine = cosine_ref[...], sine_ref[...]
    real, imag = cosine * real + sine * imag, cosine * imag - sine * real
    real, imag = by_rows((ha[...], hb[...]), real, imag)
    real, imag = by_lanes((la[...], lb[...]), real, imag)
    put(out_ref, real, imag)


def last_kernel(plan, state_ref, plain_ref, ga, gb, norm_ref, energy_ref, out_ref, sums_ref):
    device = lax.axis_index("amp")
    real, imag = by_rows((ga[...], gb[...]), *evens(state_ref))
    second = energy(real, imag, plain_ref[...])
    lane = iota((1, LANES), 1)
    sums = jnp.zeros((1, LANES), F32)
    for k, part in enumerate((norm_ref[...], energy_ref[...], second)):
        sums = jnp.where(lane == k, jnp.sum(part), sums)
    sums_ref[...] = jnp.broadcast_to(sums[None], sums_ref.shape)
    ones = bit_count(iota((plan.rows, LANES), 0), plan.row_bits) + bit_count(
        iota((plan.rows, LANES), 1), LANE_BITS
    )
    ones = ones + bit_count(device, plan.global_bits)
    odd = (ones & 1) == 1
    real, imag = jnp.where(odd, imag, real), jnp.where(odd, real, imag)
    put(
        out_ref,
        jnp.where(((ones + 1) & 2) == 2, -real, real),
        jnp.where((ones & 2) == 2, -imag, imag),
    )


def finish_kernel(plan, state_ref, sums_ref, out_ref, energies_ref):
    total = jnp.sum(sums_ref[...], axis=0)
    amps = float(2**plan.qubits)
    square = 1.0 / (total[:, 0:1] / amps + 1e-06)
    out_ref[...] = state_ref[...] * lax.rsqrt(total[:, 0:1] / amps + 1e-06)
    energies_ref[...] = total[:, 1 : 1 + LAYERS] * square / amps


def spec(space):
    return pl.BlockSpec(memory_space=space)


def call(kernel, shapes, scalars, arrays, name):
    return pl.pallas_call(
        kernel,
        out_shape=shapes,
        in_specs=[spec(pltpu.SMEM)] * len(scalars) + [spec(pltpu.VMEM)] * len(arrays),
        out_specs=jax.tree.map(lambda _: spec(pltpu.VMEM), shapes),
        name=name,
    )(*scalars, *arrays)


def local(amplitudes, coupling_index, rotation_index, chain_order, bond_sign):
    local_bits = amplitudes.shape[1].bit_length() - 1
    size = lax.axis_size("amp")
    plan = Plan(local_bits, size.bit_length() - 1)
    rows = plan.rows
    shape = jax.ShapeDtypeStruct
    bind = lambda kernel: lambda *refs: kernel(plan, *refs)

    state = amplitudes.reshape(2, rows, LANES).transpose(1, 0, 2).reshape(2 * rows, LANES)
    table = jnp.asarray(angle_tables())
    chain, bond = chain_order.reshape(1, -1), bond_sign.reshape(1, -1)
    scalars = (rotation_index, table)
    small = (chain, coupling_index, bond)
    whole = shape((2 * rows, LANES), F32)
    part = shape((8, LANES), F32)
    field = shape((rows, LANES), F32)
    row_gate = shape((rows, rows), BF16)
    lane_gate = shape((LANES, LANES), BF16)

    def trade(array):
        blocks = array.reshape(size, 2 * rows // size, LANES)
        return lax.all_to_all(blocks, "amp", 0, 0, tiled=True).reshape(2 * rows, LANES)

    state, norm = call(bind(first_kernel), (whole, part), scalars, (*small, state), "first")
    cosine, sine, moved, plain, *gates = call(
        bind(prepare_kernel),
        (field, field, field, field, row_gate, row_gate, row_gate, row_gate, lane_gate, lane_gate, row_gate, row_gate),
        scalars, small, "prepare",
    )
    state = trade(state)
    state, first_energy = call(middle_kernel, (whole, part), (), (state, cosine, sine, moved, *gates[:6]), "middle")
    state = trade(state)
    state, sums = call(
        bind(last_kernel), (whole, shape((size, 1, LANES), F32)), (),
        (state, plain, *gates[6:], norm, first_energy), "last",
    )
    sums = lax.all_to_all(sums, "amp", 0, 0, tiled=True)
    state, energies = call(bind(finish_kernel), (whole, shape((1, LAYERS), F32)), (), (state, sums), "finish")
    final = state.reshape(rows, 2, LANES).transpose(1, 0, 2).reshape(2, rows * LANES)
    return final, energies.reshape(LAYERS)


def solution(mesh):
    in_specs = (P(None, ("rep", "amp")), P("rep", None), P("rep", None), P(), P())
    out_specs = (P(None, ("rep", "amp")), P("rep"))
    return jax.shard_map(local, mesh=mesh, in_specs=in_specs, out_specs=out_specs, check_vma=False)
```

```python
import numpy as np
import jax
import jax.numpy as jnp
from jax import lax
from jax.experimental import pallas as pl
from jax.experimental.pallas import tpu as pltpu
from jax.sharding import PartitionSpec as P

LAYERS = 2
ANGLES = 16
UNITS = 2 * (ANGLES + 1)
LANE_BITS = 7
LANES = 128

F32 = jnp.float32
BF16 = jnp.bfloat16


def angle_tables():
    steps = (np.arange(ANGLES, dtype=np.float64) + 1.0) * (np.pi / UNITS)
    return np.stack([np.cos(steps), np.sin(steps)]).astype(np.float32)


def iota(shape, dimension):
    return lax.broadcasted_iota(jnp.int32, shape, dimension)


def bit_count(values, width):
    total = values & 1
    for bit in range(1, width):
        total = total + ((values >> bit) & 1)
    return total


def split(values):
    high = values.astype(BF16)
    return high, (values - high.astype(F32)).astype(BF16)


def dot(left, right):
    return jnp.dot(left, right, preferred_element_type=F32)


def product(left, right):
    return dot(left[0], right[0]) + (dot(left[0], right[1]) + dot(left[1], right[0]))


SWAPS = 3
ROWQ, LANEQ, FREE_ROWS, SWAPPED, EARLY_ROWS, ALL_EARLY, PLAN = 0, 8, 11, 12, 13, 14, 16


def gate(bits, width):
    column = iota((1, width), 1)
    lines = []
    for place, cosine, sine in bits:
        one = ((column >> place) & 1) == 1
        lines.append((jnp.where(one, sine, cosine), jnp.where(one, cosine, -sine)))
    row = iota((8, width), 0)
    matrix = None
    for bit, (zero_line, one_line) in enumerate(lines[:3]):
        factor = jnp.where(((row >> bit) & 1) == 1, one_line, zero_line)
        matrix = factor if matrix is None else matrix * factor
    for zero_line, one_line in lines[3:]:
        matrix = jnp.concatenate([matrix * zero_line, matrix * one_line], axis=0)
    return matrix


def lane_bits(pairs):
    return [(place, cosine, -sine) for place, (cosine, sine) in enumerate(pairs)]


def pair_of(layer, rotation_ref, table_ref, qubit, keep=None):
    index = rotation_ref[layer, qubit]
    cosine, sine = table_ref[0, index], table_ref[1, index]
    if keep is None:
        return cosine, sine
    return jnp.where(keep, cosine, F32(1.0)), jnp.where(keep, sine, F32(0.0))


def cos_sin(steps):
    quarter = UNITS // 2
    turns = jnp.floor(steps * (1.0 / quarter) + 0.5)
    angle = (steps - turns * quarter) * (np.pi / UNITS)
    square = angle * angle
    sine = angle * (
        1.0 + square * (-1.0 / 6 + square * (1.0 / 120 + square * (-1.0 / 5040 + square * (1.0 / 362880))))
    )
    cosine = 1.0 + square * (
        -0.5 + square * (1.0 / 24 + square * (-1.0 / 720 + square * (1.0 / 40320)))
    )
    turns = turns.astype(jnp.int32)
    odd = (turns & 1) == 1
    cosine, sine = jnp.where(odd, sine, cosine), jnp.where(odd, cosine, sine)
    return (
        jnp.where(((turns + 1) & 2) == 2, -cosine, cosine),
        jnp.where((turns & 2) == 2, -sine, sine),
    )


def turned(cosine, sine, real, imag):
    return cosine * real + sine * imag, cosine * imag - sine * real


def parity(positions, index, bonds):
    differ = (index >> positions[:, 0:bonds]) ^ (index >> positions[:, 1 : bonds + 1])
    return (1 - 2 * (differ & 1)).astype(F32)


def fields(weights, positions, device_bits, bonds, rows):
    row_signs = parity(positions, (iota((rows, bonds), 0) << LANE_BITS) | device_bits, bonds)
    lane_signs = parity(positions, iota((LANES, bonds), 0), bonds).astype(BF16)
    stacked = jnp.concatenate([(w * row_signs).astype(BF16) for w in weights], axis=0)
    out = lax.dot_general(
        stacked, lane_signs, (((1,), (1,)), ((), ())), preferred_element_type=F32
    )
    return [out[k * rows : (k + 1) * rows] for k in range(len(weights))]


def energy(real, imag, field):
    return jnp.sum((real * real + imag * imag) * field)


def in_lanes(parts):
    lane = iota((1, LANES), 1)
    row = jnp.zeros((1, LANES), F32)
    for k, part in enumerate(parts):
        row = jnp.where(lane == k, part, row)
    return row


def evens(ref):
    half = ref.shape[0] // 2
    return ref[pl.ds(0, half, stride=2), :], ref[pl.ds(1, half, stride=2), :]


def take_blocks(ref, blocks, height, kept):
    def part(component):
        return jnp.concatenate(
            [ref[pl.ds(2 * k + component, blocks, stride=height), :] for k in range(kept)], axis=0
        )

    return part(0), part(1)


def put_blocks(ref, blocks, height, kept, real, imag):
    for k in range(kept):
        here = slice(k * blocks, (k + 1) * blocks)
        ref[pl.ds(2 * k, blocks, stride=height), :] = real[here]
        ref[pl.ds(2 * k + 1, blocks, stride=height), :] = imag[here]


def by_rows(gates, real, imag):
    both = product(gates, split(jnp.concatenate([real, imag], axis=1)))
    return both[:, :LANES], both[:, LANES:]


def by_blocks(gates, real, imag):
    size = gates[0].shape[0]
    pieces = [p[k : k + size] for p in (real, imag) for k in range(0, real.shape[0], size)]
    out = product(gates, split(jnp.concatenate(pieces, axis=1)))
    pieces = [out[:, k * LANES : (k + 1) * LANES] for k in range(len(pieces))]
    half = len(pieces) // 2
    return jnp.concatenate(pieces[:half], axis=0), jnp.concatenate(pieces[half:], axis=0)


def by_lanes(gates, real, imag):
    rows = real.shape[0]
    both = product(split(jnp.concatenate([real, imag], axis=0)), gates)
    return both[:rows], both[rows:]


def swap(buffer, plan_ref, slots):
    for i in range(SWAPS):
        @pl.when(i < plan_ref[0, SWAPPED])
        def _(i=i):
            height = 2 ** (slots - 1 - i)
            place = plan_ref[0, LANEQ + i]
            step = jnp.left_shift(jnp.int32(1), place)
            whole = buffer[...].reshape(-1, 2, height, LANES)
            low, high = whole[:, 0].reshape(-1, LANES), whole[:, 1].reshape(-1, LANES)
            one = ((iota((1, LANES), 1) >> place) & 1) == 1
            new_low = jnp.where(one, pltpu.roll(high, step, 1), low)
            new_high = jnp.where(one, high, pltpu.roll(low, LANES - step, 1))
            pairs = (new_low.reshape(-1, 1, height, LANES), new_high.reshape(-1, 1, height, LANES))
            buffer[...] = jnp.concatenate(pairs, axis=1).reshape(buffer.shape)


class Plan:
    def __init__(self, local_bits, global_bits):
        self.local_bits, self.global_bits = local_bits, global_bits
        self.qubits = local_bits + global_bits
        self.row_bits = local_bits - LANE_BITS
        self.rows = 2**self.row_bits
        self.blocks = 2**global_bits
        self.kept_bits = self.row_bits - global_bits
        self.kept = 2**self.kept_bits
        self.bonds = self.qubits - 1


def choose(plan, chain_ref, plan_ref):
    order = [chain_ref[0, k] for k in range(plan.qubits)]
    away = [(q >= plan.local_bits).astype(jnp.int32) for q in order]
    free = jnp.int32(0)
    for k, q in enumerate(order):
        near = away[k]
        if k:
            near = near | away[k - 1]
        if k + 1 < plan.qubits:
            near = near | away[k + 1]
        free = free | jnp.left_shift(1 - near, q)
    bit = lambda q: (free >> q) & 1
    row_qubits = range(LANE_BITS, plan.local_bits)
    free_rows = sum(bit(q) for q in row_qubits)
    seen = jnp.int32(0)
    for k, q in enumerate(row_qubits):
        rank = jnp.where(bit(q) == 1, seen, free_rows + k - seen)
        plan_ref[0, ROWQ + rank] = jnp.int32(q)
        seen = seen + bit(q)
    slots = plan.global_bits
    free_lanes = sum(bit(q) for q in range(LANE_BITS))
    swapped = jnp.minimum(jnp.minimum(free_lanes, SWAPS), jnp.maximum(slots - free_rows, 0))
    for i in range(SWAPS):
        plan_ref[0, LANEQ + i] = jnp.int32(-1)
    seen = jnp.int32(0)
    for q in range(LANE_BITS):
        taken = (bit(q) == 1) & (seen < swapped)
        plan_ref[0, jnp.where(taken, LANEQ + seen, PLAN - 1)] = jnp.int32(q)
        seen = seen + bit(q)
    plan_ref[0, FREE_ROWS] = free_rows
    plan_ref[0, SWAPPED] = swapped
    plan_ref[0, EARLY_ROWS] = jnp.minimum(free_rows, slots - swapped)
    plan_ref[0, ALL_EARLY] = (free_rows + swapped >= slots).astype(jnp.int32)


def touches(plan, chain, plan_ref, rows_from, rows_to, lanes):
    hit = jnp.zeros(chain.shape, jnp.int32)
    for b in range(plan.global_bits):
        wanted = (b >= rows_from) & (b < rows_to)
        hit = hit | (chain == jnp.where(wanted, plan_ref[0, ROWQ + b], -1)).astype(jnp.int32)
    if lanes:
        for i in range(SWAPS):
            hit = hit | (chain == plan_ref[0, LANEQ + i]).astype(jnp.int32)
    return (hit[:, 0 : plan.bonds] | hit[:, 1 : plan.bonds + 1]).astype(F32)


def ordered_positions(plan, chain, plan_ref):
    places = chain
    for b in range(plan.row_bits):
        places = jnp.where(chain == plan_ref[0, ROWQ + b], LANE_BITS + b, places)
    return places


def moved_positions(plan, chain, plan_ref):
    slots, swapped = plan.global_bits, plan_ref[0, SWAPPED]
    places = jnp.where(chain >= plan.local_bits, chain - plan.local_bits + LANE_BITS, chain)
    for b in range(plan.row_bits):
        target = jnp.int32(LANE_BITS + b)
        if b < slots:
            target = jnp.int32(plan.local_bits + b)
            i = slots - 1 - b
            if i < SWAPS:
                target = jnp.where(i < swapped, plan_ref[0, LANEQ + i], target)
        places = jnp.where(chain == plan_ref[0, ROWQ + b], target, places)
    for i in range(SWAPS):
        places = jnp.where(chain == plan_ref[0, LANEQ + i], plan.local_bits + slots - 1 - i, places)
    return places


def row_ones(plan, device):
    ones = bit_count(iota((plan.rows, LANES), 0), plan.row_bits)
    return ones + bit_count(iota((plan.rows, LANES), 1), LANE_BITS) + bit_count(device, plan.global_bits)


def first_kernel(
    plan, rotation_ref, table_ref, order_ref, chain_ref, coupling_ref, bond_ref, amps_ref,
    out_ref, sums_ref, plan_ref, buffer,
):
    device = lax.axis_index("amp")
    bonds, rows = plan.bonds, plan.rows
    choose(plan, order_ref, plan_ref)
    chain = chain_ref[...]
    device_bits = device << plan.local_bits
    bond_signs = (2 * bond_ref[...] - 1).astype(F32)
    (steps,) = fields(
        [(coupling_ref[0:1, :] + 1).astype(F32) * bond_signs], chain, device_bits, bonds, rows
    )
    steps = steps + (UNITS // 2) * row_ones(plan, device).astype(F32)
    pair = lambda layer, q, keep=None: pair_of(layer, rotation_ref, table_ref, q, keep)

    real, imag = evens(amps_ref)
    norm = jnp.sum(real * real + imag * imag)
    real, imag = turned(*cos_sin(steps), real, imag)
    ranked = [plan_ref[0, ROWQ + b] for b in range(plan.row_bits)]
    row_gate = gate([(q - LANE_BITS, *pair(0, q)) for q in ranked], rows)
    lane_gate = gate(lane_bits([pair(0, q) for q in range(LANE_BITS)]), LANES)
    real, imag = by_rows(split(row_gate), real, imag)
    real, imag = by_lanes(split(lane_gate), real, imag)

    early = touches(plan, chain, plan_ref, 0, plan_ref[0, EARLY_ROWS], True)
    weight = early * bond_signs
    steps, signs = fields(
        [(coupling_ref[1:2, :] + 1).astype(F32) * weight, weight],
        ordered_positions(plan, chain, plan_ref), device_bits, bonds, rows,
    )
    sums_ref[...] = in_lanes([norm, energy(real, imag, signs)])
    real, imag = turned(*cos_sin(steps), real, imag)
    bits = []
    for b in range(plan.global_bits):
        bits.append((b, *pair(1, ranked[b], b < plan_ref[0, EARLY_ROWS])))
    real, imag = by_blocks(split(gate(bits, plan.blocks)), real, imag)
    pairs = []
    for q in range(LANE_BITS):
        keep = q == plan_ref[0, LANEQ]
        for i in range(1, SWAPS):
            keep = keep | (q == plan_ref[0, LANEQ + i])
        pairs.append(pair(1, q, keep))
    real, imag = by_lanes(split(gate(lane_bits(pairs), LANES)), real, imag)
    buffer[...] = jnp.concatenate([real, imag], axis=0)
    swap(buffer, plan_ref, plan.global_bits)
    put_blocks(out_ref, plan.blocks, 2 * plan.kept, plan.kept, buffer[:rows], buffer[rows:])


def prepare_kernel(
    plan, rotation_ref, table_ref, plan_ref, chain_ref, coupling_ref, bond_ref,
    cosine_ref, sine_ref, before_ref, after_ref, late_ref, *gate_refs,
):
    device = lax.axis_index("amp")
    bonds, rows, slots = plan.bonds, plan.rows, plan.global_bits
    chain = chain_ref[...]
    bond_signs = (2 * bond_ref[...] - 1).astype(F32)
    early_rows, swapped = plan_ref[0, EARLY_ROWS], plan_ref[0, SWAPPED]
    rest = bond_signs * (1.0 - touches(plan, chain, plan_ref, 0, early_rows, True))
    late = bond_signs * touches(plan, chain, plan_ref, early_rows, slots - swapped, False)
    steps, before_ref[...], after_ref[...] = fields(
        [(coupling_ref[1:2, :] + 1).astype(F32) * rest, rest, bond_signs - late],
        moved_positions(plan, chain, plan_ref), device << plan.local_bits, bonds, rows,
    )
    cosine_ref[...], sine_ref[...] = cos_sin(steps)
    (late_ref[...],) = fields([late], chain, device << plan.local_bits, bonds, rows)
    pair = lambda layer, q, keep=None: pair_of(layer, rotation_ref, table_ref, q, keep)
    ranked = [plan_ref[0, ROWQ + b] for b in range(plan.row_bits)]
    far = [plan.local_bits + b for b in range(slots)]
    lane_pairs = []
    for q in range(LANE_BITS):
        held = jnp.int32(q)
        for i in range(SWAPS):
            held = jnp.where(plan_ref[0, LANEQ + i] == q, ranked[slots - 1 - i], held)
        lane_pairs.append(pair(1, held))
    back = []
    for b in range(plan.row_bits):
        wanted = (b >= early_rows) & (b < slots - swapped)
        cosine, sine = pair(1, ranked[b], wanted)
        back.append((ranked[b] - LANE_BITS, cosine, -sine))
    gates = [
        gate([(b, *pair(0, q)) for b, q in enumerate(far)], plan.blocks),
        gate([(b, *pair(1, q)) for b, q in enumerate(far + ranked[slots:])], rows),
        gate(lane_bits(lane_pairs), LANES),
        gate(back, rows).T,
    ]
    for k, made in enumerate(gates):
        gate_refs[2 * k][...], gate_refs[2 * k + 1][...] = split(made)


def middle_kernel(plan, state_ref, cosine_ref, sine_ref, before_ref, after_ref, sums_ref, *refs):
    (ga, gb, ha, hb, la, lb), (out_ref,) = refs[:6], refs[6:]
    blocks, kept = plan.blocks, plan.kept
    real, imag = take_blocks(state_ref, blocks, 2 * kept, kept)
    real, imag = by_blocks((ga[...], gb[...]), real, imag)
    before = energy(real, imag, before_ref[...])
    real, imag = turned(cosine_ref[...], sine_ref[...], real, imag)
    real, imag = by_rows((ha[...], hb[...]), real, imag)
    real, imag = by_lanes((la[...], lb[...]), real, imag)
    after = energy(real, imag, after_ref[...])
    height = 2 * kept + 1
    put_blocks(out_ref, blocks, height, kept, real, imag)
    sums = sums_ref[...] + in_lanes([F32(0.0), before, after])
    out_ref[pl.ds(2 * kept, blocks, stride=height), :] = jnp.broadcast_to(sums, (blocks, LANES))


def last_kernel(plan, plan_ref, state_ref, late_ref, ga, gb, out_ref, energies_ref, late_out_ref, buffer):
    device = lax.axis_index("amp")
    blocks, kept, rows = plan.blocks, plan.kept, plan.rows
    height = 2 * kept + 1
    sums = jnp.sum(state_ref[pl.ds(2 * kept, blocks, stride=height), :], axis=0, keepdims=True)
    amps = float(2**plan.qubits)
    mean = sums[:, 0:1] / amps + 1e-06
    factor = 1.0 / jnp.sqrt(mean)
    square = factor * factor / amps
    energies_ref[...] = sums[:, 1 : 1 + LAYERS] * square
    real, imag = take_blocks(state_ref, blocks, height, kept)
    buffer[...] = jnp.concatenate([real, imag], axis=0)
    swap(buffer, plan_ref, plan.global_bits)
    real, imag = by_rows((ga[...], gb[...]), buffer[:rows], buffer[rows:])
    late_out_ref[...] = in_lanes([0.0, energy(real, imag, late_ref[...])])[:, 0:LAYERS] * square
    ones = row_ones(plan, device)
    odd = (ones & 1) == 1
    real, imag = jnp.where(odd, imag, real), jnp.where(odd, real, imag)
    real = jnp.where(((ones + 1) & 2) == 2, -factor, factor) * real
    imag = jnp.where((ones & 2) == 2, -factor, factor) * imag
    out_ref[pl.ds(0, rows, stride=2), :] = real
    out_ref[pl.ds(1, rows, stride=2), :] = imag


def spec(space):
    return pl.BlockSpec(memory_space=space)


def call(kernel, shapes, scalars, arrays, name, spaces=None, scratch=()):
    return pl.pallas_call(
        kernel,
        out_shape=shapes,
        in_specs=[spec(pltpu.SMEM)] * len(scalars) + [spec(pltpu.VMEM)] * len(arrays),
        out_specs=tuple(spec(s) for s in spaces or (pltpu.VMEM,) * len(shapes)),
        scratch_shapes=scratch,
        name=name,
    )(*scalars, *arrays)


def local(amplitudes, coupling_index, rotation_index, chain_order, bond_sign):
    local_bits = amplitudes.shape[1].bit_length() - 1
    size = lax.axis_size("amp")
    plan = Plan(local_bits, size.bit_length() - 1)
    rows = plan.rows
    shape = jax.ShapeDtypeStruct
    bind = lambda kernel: lambda *refs: kernel(plan, *refs)

    state = amplitudes.reshape(2, rows, LANES).transpose(1, 0, 2).reshape(2 * rows, LANES)
    table = jnp.asarray(angle_tables())
    chain, bond = chain_order.reshape(1, -1), bond_sign.reshape(1, -1)
    small = (chain, coupling_index, bond)
    whole = shape((2 * rows, LANES), F32)
    field = shape((rows, LANES), F32)
    square_of = lambda n: shape((n, n), BF16)
    buffer = (pltpu.VMEM((2 * rows, LANES), F32),)

    state, sums, chosen = call(
        bind(first_kernel),
        (whole, shape((1, LANES), F32), shape((1, PLAN), jnp.int32)),
        (rotation_index, table, chain), (*small, state), "first",
        (pltpu.VMEM, pltpu.VMEM, pltpu.SMEM), buffer,
    )
    sizes = (size, rows, LANES, rows)
    made = call(
        bind(prepare_kernel), (field,) * 5 + tuple(square_of(n) for n in sizes for _ in range(2)),
        (rotation_index, table, chosen), small, "prepare",
    )
    fields_made, late, gates = made[:4], made[4], made[5:]
    state = lax.all_to_all(state.reshape(size, 2 * plan.kept, LANES), "amp", 0, 0, tiled=True)
    height = 2 * plan.kept + 1
    (state,) = call(
        bind(middle_kernel), (shape((size * height, LANES), F32),), (),
        (state.reshape(2 * rows, LANES), *fields_made, sums, *gates[:6]), "middle",
    )
    state = lax.all_to_all(state.reshape(size, height, 1, LANES), "amp", 0, 0, tiled=True)
    pair = shape((1, LAYERS), F32)
    state, energies, extra = call(
        bind(last_kernel), (whole, pair, pair), (chosen,),
        (state.reshape(size * height, LANES), late, *gates[6:]), "last", scratch=buffer,
    )

    def with_late(energies, extra):
        sent = jnp.broadcast_to(extra[None], (size, 1, LAYERS))
        return energies + lax.all_to_all(sent, "amp", 0, 0, tiled=True).sum(axis=0)

    energies = lax.cond(
        chosen[0, ALL_EARLY] == 1, lambda energies, extra: energies, with_late, energies, extra
    )
    final = state.reshape(rows, 2, LANES).transpose(1, 0, 2).reshape(2, rows * LANES)
    return final, energies.reshape(LAYERS)


def solution(mesh):
    in_specs = (P(None, ("rep", "amp")), P("rep", None), P("rep", None), P(), P())
    out_specs = (P(None, ("rep", "amp")), P("rep"))
    return jax.shard_map(local, mesh=mesh, in_specs=in_specs, out_specs=out_specs, check_vma=False)
```

```python
import numpy as np
import jax
import jax.numpy as jnp
from jax import lax
from jax.experimental import pallas as pl
from jax.experimental.pallas import tpu as pltpu
from jax.sharding import PartitionSpec as P

LAYERS = 2
ANGLES = 16
UNITS = 2 * (ANGLES + 1)
LANE_BITS = 7
LANES = 128

F32 = jnp.float32
BF16 = jnp.bfloat16


def angle_tables():
    steps = (np.arange(ANGLES, dtype=np.float64) + 1.0) * (np.pi / UNITS)
    return np.stack([np.cos(steps), np.sin(steps)]).astype(np.float32)


def iota(shape, dimension):
    return lax.broadcasted_iota(jnp.int32, shape, dimension)


def bit_count(values, width):
    total = values & 1
    for bit in range(1, width):
        total = total + ((values >> bit) & 1)
    return total


def split(values):
    high = values.astype(BF16)
    return high, (values - high.astype(F32)).astype(BF16)


def dot(left, right):
    return jnp.dot(left, right, preferred_element_type=F32)


def product(left, right):
    return dot(left[0], right[0]) + (dot(left[0], right[1]) + dot(left[1], right[0]))


SWAPS = 3
ROWQ, LANEQ, FREE_ROWS, SWAPPED, EARLY_ROWS, ALL_EARLY, PLAN = 0, 8, 11, 12, 13, 14, 16


def gate(bits, width):
    column = iota((1, width), 1)
    lines = []
    for place, cosine, sine in bits:
        one = ((column >> place) & 1) == 1
        lines.append((jnp.where(one, sine, cosine), jnp.where(one, cosine, -sine)))
    row = iota((8, width), 0)
    matrix = None
    for bit, (zero_line, one_line) in enumerate(lines[:3]):
        factor = jnp.where(((row >> bit) & 1) == 1, one_line, zero_line)
        matrix = factor if matrix is None else matrix * factor
    for zero_line, one_line in lines[3:]:
        matrix = jnp.concatenate([matrix * zero_line, matrix * one_line], axis=0)
    return matrix


def lane_bits(pairs):
    return [(place, cosine, -sine) for place, (cosine, sine) in enumerate(pairs)]


def pair_of(layer, rotation_ref, table_ref, qubit, keep=None):
    index = rotation_ref[layer, qubit]
    cosine, sine = table_ref[0, index], table_ref[1, index]
    if keep is None:
        return cosine, sine
    return jnp.where(keep, cosine, F32(1.0)), jnp.where(keep, sine, F32(0.0))


def cos_sin(steps):
    quarter = UNITS // 2
    turns = jnp.floor(steps * (1.0 / quarter) + 0.5)
    angle = (steps - turns * quarter) * (np.pi / UNITS)
    square = angle * angle
    sine = angle * (
        1.0 + square * (-1.0 / 6 + square * (1.0 / 120 + square * (-1.0 / 5040 + square * (1.0 / 362880))))
    )
    cosine = 1.0 + square * (
        -0.5 + square * (1.0 / 24 + square * (-1.0 / 720 + square * (1.0 / 40320)))
    )
    turns = turns.astype(jnp.int32)
    odd = (turns & 1) == 1
    cosine, sine = jnp.where(odd, sine, cosine), jnp.where(odd, cosine, sine)
    return (
        jnp.where(((turns + 1) & 2) == 2, -cosine, cosine),
        jnp.where((turns & 2) == 2, -sine, sine),
    )


def turned(cosine, sine, real, imag):
    return cosine * real + sine * imag, cosine * imag - sine * real


def parity(positions, index, bonds):
    differ = (index >> positions[:, 0:bonds]) ^ (index >> positions[:, 1 : bonds + 1])
    return (1 - 2 * (differ & 1)).astype(F32)


def fields(weights, positions, device_bits, bonds, rows):
    row_signs = parity(positions, (iota((rows, bonds), 0) << LANE_BITS) | device_bits, bonds)
    lane_signs = parity(positions, iota((LANES, bonds), 0), bonds).astype(BF16)
    stacked = jnp.concatenate([(w * row_signs).astype(BF16) for w in weights], axis=0)
    out = lax.dot_general(
        stacked, lane_signs, (((1,), (1,)), ((), ())), preferred_element_type=F32
    )
    return [out[k * rows : (k + 1) * rows] for k in range(len(weights))]


def energy(real, imag, field):
    return jnp.sum((real * real + imag * imag) * field)


def in_lanes(parts):
    lane = iota((1, LANES), 1)
    row = jnp.zeros((1, LANES), F32)
    for k, part in enumerate(parts):
        row = jnp.where(lane == k, part, row)
    return row


def evens(ref):
    half = ref.shape[0] // 2
    return ref[pl.ds(0, half, stride=2), :], ref[pl.ds(1, half, stride=2), :]


def take_blocks(ref, blocks, height, kept):
    def part(component):
        return jnp.concatenate(
            [ref[pl.ds(2 * k + component, blocks, stride=height), :] for k in range(kept)], axis=0
        )

    return part(0), part(1)


def put_blocks(ref, blocks, height, kept, real, imag):
    for k in range(kept):
        here = slice(k * blocks, (k + 1) * blocks)
        ref[pl.ds(2 * k, blocks, stride=height), :] = real[here]
        ref[pl.ds(2 * k + 1, blocks, stride=height), :] = imag[here]


def by_rows(gates, real, imag):
    both = product(gates, split(jnp.concatenate([real, imag], axis=1)))
    return both[:, :LANES], both[:, LANES:]


def by_blocks(gates, real, imag):
    size = gates[0].shape[0]
    pieces = [p[k : k + size] for p in (real, imag) for k in range(0, real.shape[0], size)]
    out = product(gates, split(jnp.concatenate(pieces, axis=1)))
    pieces = [out[:, k * LANES : (k + 1) * LANES] for k in range(len(pieces))]
    half = len(pieces) // 2
    return jnp.concatenate(pieces[:half], axis=0), jnp.concatenate(pieces[half:], axis=0)


def by_lanes(gates, real, imag):
    rows = real.shape[0]
    both = product(split(jnp.concatenate([real, imag], axis=0)), gates)
    return both[:rows], both[rows:]


def swap(buffer, plan_ref, slots):
    for i in range(SWAPS):
        @pl.when(i < plan_ref[0, SWAPPED])
        def _(i=i):
            height = 2 ** (slots - 1 - i)
            place = plan_ref[0, LANEQ + i]
            step = jnp.left_shift(jnp.int32(1), place)
            whole = buffer[...].reshape(-1, 2, height, LANES)
            low, high = whole[:, 0].reshape(-1, LANES), whole[:, 1].reshape(-1, LANES)
            one = ((iota((1, LANES), 1) >> place) & 1) == 1
            new_low = jnp.where(one, pltpu.roll(high, step, 1), low)
            new_high = jnp.where(one, high, pltpu.roll(low, LANES - step, 1))
            pairs = (new_low.reshape(-1, 1, height, LANES), new_high.reshape(-1, 1, height, LANES))
            buffer[...] = jnp.concatenate(pairs, axis=1).reshape(buffer.shape)


class Plan:
    def __init__(self, local_bits, global_bits):
        self.local_bits, self.global_bits = local_bits, global_bits
        self.qubits = local_bits + global_bits
        self.row_bits = local_bits - LANE_BITS
        self.rows = 2**self.row_bits
        self.blocks = 2**global_bits
        self.kept_bits = self.row_bits - global_bits
        self.kept = 2**self.kept_bits
        self.bonds = self.qubits - 1


def choose(plan, chain_ref, plan_ref):
    order = [chain_ref[0, k] for k in range(plan.qubits)]
    away = [(q >= plan.local_bits).astype(jnp.int32) for q in order]
    free = jnp.int32(0)
    for k, q in enumerate(order):
        near = away[k]
        if k:
            near = near | away[k - 1]
        if k + 1 < plan.qubits:
            near = near | away[k + 1]
        free = free | jnp.left_shift(1 - near, q)
    bit = lambda q: (free >> q) & 1
    row_qubits = range(LANE_BITS, plan.local_bits)
    free_rows = sum(bit(q) for q in row_qubits)
    seen = jnp.int32(0)
    for k, q in enumerate(row_qubits):
        rank = jnp.where(bit(q) == 1, seen, free_rows + k - seen)
        plan_ref[0, ROWQ + rank] = jnp.int32(q)
        seen = seen + bit(q)
    slots = plan.global_bits
    free_lanes = sum(bit(q) for q in range(LANE_BITS))
    swapped = jnp.minimum(jnp.minimum(free_lanes, SWAPS), jnp.maximum(slots - free_rows, 0))
    for i in range(SWAPS):
        plan_ref[0, LANEQ + i] = jnp.int32(-1)
    seen = jnp.int32(0)
    for q in range(LANE_BITS):
        taken = (bit(q) == 1) & (seen < swapped)
        plan_ref[0, jnp.where(taken, LANEQ + seen, PLAN - 1)] = jnp.int32(q)
        seen = seen + bit(q)
    plan_ref[0, FREE_ROWS] = free_rows
    plan_ref[0, SWAPPED] = swapped
    plan_ref[0, EARLY_ROWS] = jnp.minimum(free_rows, slots - swapped)
    plan_ref[0, ALL_EARLY] = (free_rows + swapped >= slots).astype(jnp.int32)


def touches(plan, chain, plan_ref, rows_from, rows_to, lanes):
    hit = jnp.zeros(chain.shape, jnp.int32)
    for b in range(plan.global_bits):
        wanted = (b >= rows_from) & (b < rows_to)
        hit = hit | (chain == jnp.where(wanted, plan_ref[0, ROWQ + b], -1)).astype(jnp.int32)
    if lanes:
        for i in range(SWAPS):
            hit = hit | (chain == plan_ref[0, LANEQ + i]).astype(jnp.int32)
    return (hit[:, 0 : plan.bonds] | hit[:, 1 : plan.bonds + 1]).astype(F32)


def ordered_positions(plan, chain, plan_ref):
    places = chain
    for b in range(plan.row_bits):
        places = jnp.where(chain == plan_ref[0, ROWQ + b], LANE_BITS + b, places)
    return places


def moved_positions(plan, chain, plan_ref):
    slots, swapped = plan.global_bits, plan_ref[0, SWAPPED]
    places = jnp.where(chain >= plan.local_bits, chain - plan.local_bits + LANE_BITS, chain)
    for b in range(plan.row_bits):
        target = jnp.int32(LANE_BITS + b)
        if b < slots:
            target = jnp.int32(plan.local_bits + b)
            i = slots - 1 - b
            if i < SWAPS:
                target = jnp.where(i < swapped, plan_ref[0, LANEQ + i], target)
        places = jnp.where(chain == plan_ref[0, ROWQ + b], target, places)
    for i in range(SWAPS):
        places = jnp.where(chain == plan_ref[0, LANEQ + i], plan.local_bits + slots - 1 - i, places)
    return places


def row_ones(plan, device):
    ones = bit_count(iota((plan.rows, LANES), 0), plan.row_bits)
    return ones + bit_count(iota((plan.rows, LANES), 1), LANE_BITS) + bit_count(device, plan.global_bits)


def first_kernel(
    plan, rotation_ref, table_ref, order_ref, chain_ref, coupling_ref, bond_ref, amps_ref,
    out_ref, sums_ref, plan_ref, buffer,
):
    device = lax.axis_index("amp")
    bonds, rows = plan.bonds, plan.rows
    choose(plan, order_ref, plan_ref)
    chain = chain_ref[...]
    device_bits = device << plan.local_bits
    bond_signs = (2 * bond_ref[...] - 1).astype(F32)
    (steps,) = fields(
        [(coupling_ref[0:1, :] + 1).astype(F32) * bond_signs], chain, device_bits, bonds, rows
    )
    steps = steps + (UNITS // 2) * row_ones(plan, device).astype(F32)
    pair = lambda layer, q, keep=None: pair_of(layer, rotation_ref, table_ref, q, keep)

    real, imag = evens(amps_ref)
    norm = jnp.sum(real * real + imag * imag)
    real, imag = turned(*cos_sin(steps), real, imag)
    ranked = [plan_ref[0, ROWQ + b] for b in range(plan.row_bits)]
    row_gate = gate([(q - LANE_BITS, *pair(0, q)) for q in ranked], rows)
    lane_gate = gate(lane_bits([pair(0, q) for q in range(LANE_BITS)]), LANES)
    real, imag = by_rows(split(row_gate), real, imag)
    real, imag = by_lanes(split(lane_gate), real, imag)

    early = touches(plan, chain, plan_ref, 0, plan_ref[0, EARLY_ROWS], True)
    weight = early * bond_signs
    steps, signs = fields(
        [(coupling_ref[1:2, :] + 1).astype(F32) * weight, weight],
        ordered_positions(plan, chain, plan_ref), device_bits, bonds, rows,
    )
    sums_ref[...] = in_lanes([norm, energy(real, imag, signs)])
    real, imag = turned(*cos_sin(steps), real, imag)
    bits = []
    for b in range(plan.global_bits):
        bits.append((b, *pair(1, ranked[b], b < plan_ref[0, EARLY_ROWS])))
    real, imag = by_blocks(split(gate(bits, plan.blocks)), real, imag)
    pairs = []
    for q in range(LANE_BITS):
        keep = q == plan_ref[0, LANEQ]
        for i in range(1, SWAPS):
            keep = keep | (q == plan_ref[0, LANEQ + i])
        pairs.append(pair(1, q, keep))
    real, imag = by_lanes(split(gate(lane_bits(pairs), LANES)), real, imag)
    buffer[...] = jnp.concatenate([real, imag], axis=0)
    swap(buffer, plan_ref, plan.global_bits)
    put_blocks(out_ref, plan.blocks, 2 * plan.kept, plan.kept, buffer[:rows], buffer[rows:])


def prepare_kernel(
    plan, rotation_ref, table_ref, plan_ref, chain_ref, coupling_ref, bond_ref,
    done_ref, cosine_ref, sine_ref, before_ref, after_ref, late_ref, *gate_refs,
):
    done_ref[0, 0] = plan_ref[0, ALL_EARLY]
    device = lax.axis_index("amp")
    bonds, rows, slots = plan.bonds, plan.rows, plan.global_bits
    chain = chain_ref[...]
    bond_signs = (2 * bond_ref[...] - 1).astype(F32)
    early_rows, swapped = plan_ref[0, EARLY_ROWS], plan_ref[0, SWAPPED]
    rest = bond_signs * (1.0 - touches(plan, chain, plan_ref, 0, early_rows, True))
    late = bond_signs * touches(plan, chain, plan_ref, early_rows, slots - swapped, False)
    steps, before_ref[...], after_ref[...] = fields(
        [(coupling_ref[1:2, :] + 1).astype(F32) * rest, rest, bond_signs - late],
        moved_positions(plan, chain, plan_ref), device << plan.local_bits, bonds, rows,
    )
    cosine_ref[...], sine_ref[...] = cos_sin(steps)
    (late_ref[...],) = fields([late], chain, device << plan.local_bits, bonds, rows)
    pair = lambda layer, q, keep=None: pair_of(layer, rotation_ref, table_ref, q, keep)
    ranked = [plan_ref[0, ROWQ + b] for b in range(plan.row_bits)]
    far = [plan.local_bits + b for b in range(slots)]
    lane_pairs = []
    for q in range(LANE_BITS):
        held = jnp.int32(q)
        for i in range(SWAPS):
            held = jnp.where(plan_ref[0, LANEQ + i] == q, ranked[slots - 1 - i], held)
        lane_pairs.append(pair(1, held))
    back = []
    for b in range(plan.row_bits):
        wanted = (b >= early_rows) & (b < slots - swapped)
        cosine, sine = pair(1, ranked[b], wanted)
        back.append((ranked[b] - LANE_BITS, cosine, -sine))
    gates = [
        gate([(b, *pair(0, q)) for b, q in enumerate(far)], plan.blocks),
        gate([(b, *pair(1, q)) for b, q in enumerate(far + ranked[slots:])], rows),
        gate(lane_bits(lane_pairs), LANES),
        gate(back, rows).T,
    ]
    for k, made in enumerate(gates):
        gate_refs[2 * k][...], gate_refs[2 * k + 1][...] = split(made)


def middle_kernel(plan, state_ref, cosine_ref, sine_ref, before_ref, after_ref, sums_ref, *refs):
    (ga, gb, ha, hb, la, lb), (out_ref,) = refs[:6], refs[6:]
    blocks, kept = plan.blocks, plan.kept
    real, imag = take_blocks(state_ref, blocks, 2 * kept, kept)
    real, imag = by_blocks((ga[...], gb[...]), real, imag)
    before = energy(real, imag, before_ref[...])
    real, imag = turned(cosine_ref[...], sine_ref[...], real, imag)
    real, imag = by_rows((ha[...], hb[...]), real, imag)
    real, imag = by_lanes((la[...], lb[...]), real, imag)
    after = energy(real, imag, after_ref[...])
    height = 2 * kept + 1
    put_blocks(out_ref, blocks, height, kept, real, imag)
    sums = sums_ref[...] + in_lanes([F32(0.0), before, after])
    out_ref[pl.ds(2 * kept, blocks, stride=height), :] = jnp.broadcast_to(sums, (blocks, LANES))


def last_kernel(plan, plan_ref, state_ref, ga, gb, *refs):
    late_ref, (out_ref, energies_ref, *late_out_ref, buffer) = refs[:-3][:1], refs[-4 if len(refs) == 5 else -3 :]
    device = lax.axis_index("amp")
    blocks, kept, rows = plan.blocks, plan.kept, plan.rows
    height = 2 * kept + 1
    sums = jnp.sum(state_ref[pl.ds(2 * kept, blocks, stride=height), :], axis=0, keepdims=True)
    amps = float(2**plan.qubits)
    mean = sums[:, 0:1] / amps + 1e-06
    factor = 1.0 / jnp.sqrt(mean)
    square = factor * factor / amps
    energies_ref[...] = sums[:, 1 : 1 + LAYERS] * square
    real, imag = take_blocks(state_ref, blocks, height, kept)
    buffer[...] = jnp.concatenate([real, imag], axis=0)
    swap(buffer, plan_ref, plan.global_bits)
    real, imag = by_rows((ga[...], gb[...]), buffer[:rows], buffer[rows:])
    if late_ref:
        late_out_ref[0][...] = in_lanes([0.0, energy(real, imag, late_ref[0][...])])[:, 0:LAYERS] * square
    ones = row_ones(plan, device)
    odd = (ones & 1) == 1
    real, imag = jnp.where(odd, imag, real), jnp.where(odd, real, imag)
    real = jnp.where(((ones + 1) & 2) == 2, -factor, factor) * real
    imag = jnp.where((ones & 2) == 2, -factor, factor) * imag
    out_ref[pl.ds(0, rows, stride=2), :] = real
    out_ref[pl.ds(1, rows, stride=2), :] = imag


def spec(space):
    return pl.BlockSpec(memory_space=space)


def call(kernel, shapes, scalars, arrays, name, spaces=None, scratch=(), near=0, held=()):
    kept = len(arrays) - near
    arrays = tuple(
        pltpu.with_memory_space_constraint(a, pltpu.VMEM) if k >= kept else a
        for k, a in enumerate(arrays)
    )
    shapes = tuple(pltpu.VMEM(s.shape, s.dtype) if k in held else s for k, s in enumerate(shapes))
    return pl.pallas_call(
        kernel,
        out_shape=shapes,
        in_specs=[spec(pltpu.SMEM)] * len(scalars) + [spec(pltpu.VMEM)] * len(arrays),
        out_specs=tuple(spec(s) for s in spaces or (pltpu.VMEM,) * len(shapes)),
        scratch_shapes=scratch,
        name=name,
    )(*scalars, *arrays)


def local(amplitudes, coupling_index, rotation_index, chain_order, bond_sign):
    local_bits = amplitudes.shape[1].bit_length() - 1
    size = lax.axis_size("amp")
    plan = Plan(local_bits, size.bit_length() - 1)
    rows = plan.rows
    shape = jax.ShapeDtypeStruct
    bind = lambda kernel: lambda *refs: kernel(plan, *refs)

    state = amplitudes.reshape(2, rows, LANES).transpose(1, 0, 2).reshape(2 * rows, LANES)
    table = jnp.asarray(angle_tables())
    chain, bond = chain_order.reshape(1, -1), bond_sign.reshape(1, -1)
    small = (chain, coupling_index, bond)
    whole = shape((2 * rows, LANES), F32)
    field = shape((rows, LANES), F32)
    square_of = lambda n: shape((n, n), BF16)
    buffer = (pltpu.VMEM((2 * rows, LANES), F32),)

    state, sums, chosen = call(
        bind(first_kernel),
        (whole, shape((1, LANES), F32), shape((1, PLAN), jnp.int32)),
        (rotation_index, table, chain), (*small, state), "first",
        (pltpu.VMEM, pltpu.VMEM, pltpu.SMEM), buffer, held=(0, 1),
    )
    sizes = (size, rows, LANES, rows)
    made = call(
        bind(prepare_kernel),
        (shape((1, 1), jnp.int32),) + (field,) * 5 + tuple(square_of(n) for n in sizes for _ in range(2)),
        (rotation_index, table, chosen), small, "prepare",
        (pltpu.SMEM,) + (pltpu.VMEM,) * 13, held=range(1, 14),
    )
    done, fields_made, late, gates = made[0], made[1:5], made[5], made[6:]
    state = lax.all_to_all(state.reshape(size, 2 * plan.kept, LANES), "amp", 0, 0, tiled=True)
    height = 2 * plan.kept + 1
    (state,) = call(
        bind(middle_kernel), (shape((size * height, LANES), F32),), (),
        (state.reshape(2 * rows, LANES), *fields_made, sums, *gates[:6]), "middle", near=12, held=(0,),
    )
    state = lax.all_to_all(state.reshape(size, height, 1, LANES), "amp", 0, 0, tiled=True)
    pair = shape((1, LAYERS), F32)

    def end(chosen, state, ga, gb, *late):
        return call(
            bind(last_kernel), (whole, pair) + (pair,) * len(late), (chosen,),
            (state, ga, gb, *late), "last", scratch=buffer, near=3 + len(late),
        )

    def apart(final):
        return final.reshape(rows, 2, LANES).transpose(1, 0, 2).reshape(2, rows * LANES)

    def early_end(*operands):
        final, energies = end(*operands[:-1])
        return apart(final), energies.reshape(LAYERS)

    def late_end(*operands):
        final, energies, extra = end(*operands)
        sent = jnp.broadcast_to(extra[None], (size, 1, LAYERS))
        total = energies + lax.all_to_all(sent, "amp", 0, 0, tiled=True).sum(axis=0)
        return apart(final), total.reshape(LAYERS)

    return lax.cond(
        done[0, 0] == 1, early_end, late_end,
        chosen, state.reshape(size * height, LANES), *gates[6:], late,
    )


def solution(mesh):
    in_specs = (P(None, ("rep", "amp")), P("rep", None), P("rep", None), P(), P())
    out_specs = (P(None, ("rep", "amp")), P("rep"))
    return jax.shard_map(local, mesh=mesh, in_specs=in_specs, out_specs=out_specs, check_vma=False)
```

```python
import numpy as np
import jax
import jax.numpy as jnp
from jax import lax
from jax.experimental import pallas as pl
from jax.experimental.pallas import tpu as pltpu
from jax.sharding import PartitionSpec as P

LAYERS = 2
ANGLES = 16
UNITS = 2 * (ANGLES + 1)
LANE_BITS = 7
LANES = 128

F32 = jnp.float32
BF16 = jnp.bfloat16


def angle_tables():
    steps = (np.arange(ANGLES, dtype=np.float64) + 1.0) * (np.pi / UNITS)
    return np.stack([np.cos(steps), np.sin(steps)]).astype(np.float32)


def iota(shape, dimension):
    return lax.broadcasted_iota(jnp.int32, shape, dimension)


def bit_count(values, width):
    total = values & 1
    for bit in range(1, width):
        total = total + ((values >> bit) & 1)
    return total


def split(values):
    high = values.astype(BF16)
    return high, (values - high.astype(F32)).astype(BF16)


def dot(left, right):
    return jnp.dot(left, right, preferred_element_type=F32)


def product(left, right):
    return dot(
        jnp.concatenate([left[0], left[0], left[1]], axis=1),
        jnp.concatenate([right[0], right[1], right[0]], axis=0),
    )


SWAPS = 4
ROWQ, LANEQ, SWAPPED, LATE, SPARE, PLAN = 0, 8, 12, 13, 14, 16


def gate(bits, width):
    column = iota((1, width), 1)
    lines = []
    for place, cosine, sine in bits:
        one = ((column >> place) & 1) == 1
        lines.append((jnp.where(one, sine, cosine), jnp.where(one, cosine, -sine)))
    row = iota((8, width), 0)
    matrix = None
    for bit, (zero_line, one_line) in enumerate(lines[:3]):
        factor = jnp.where(((row >> bit) & 1) == 1, one_line, zero_line)
        matrix = factor if matrix is None else matrix * factor
    for zero_line, one_line in lines[3:]:
        matrix = jnp.concatenate([matrix * zero_line, matrix * one_line], axis=0)
    return matrix


def lane_bits(pairs):
    return [(place, cosine, -sine) for place, (cosine, sine) in enumerate(pairs)]


def pair_of(layer, rotation_ref, table_ref, qubit, keep=None):
    index = rotation_ref[layer, qubit]
    cosine, sine = table_ref[0, index], table_ref[1, index]
    if keep is None:
        return cosine, sine
    return jnp.where(keep, cosine, F32(1.0)), jnp.where(keep, sine, F32(0.0))


def cos_sin(steps):
    quarter = UNITS // 2
    turns = jnp.floor(steps * (1.0 / quarter) + 0.5)
    angle = (steps - turns * quarter) * (np.pi / UNITS)
    square = angle * angle
    sine = angle * (
        1.0 + square * (-1.0 / 6 + square * (1.0 / 120 + square * (-1.0 / 5040 + square * (1.0 / 362880))))
    )
    cosine = 1.0 + square * (
        -0.5 + square * (1.0 / 24 + square * (-1.0 / 720 + square * (1.0 / 40320)))
    )
    turns = turns.astype(jnp.int32)
    odd = (turns & 1) == 1
    cosine, sine = jnp.where(odd, sine, cosine), jnp.where(odd, cosine, sine)
    return (
        jnp.where(((turns + 1) & 2) == 2, -cosine, cosine),
        jnp.where((turns & 2) == 2, -sine, sine),
    )


def looked_up(steps):
    period = 2 * UNITS
    place = (steps - period * jnp.floor(steps * (1.0 / period) + 0.25 / period)).astype(jnp.int32)
    cosine, sine = cos_sin(iota((8, LANES), 1).astype(F32))
    tiles = place.reshape(-1, 8, LANES)
    pick = lambda table: jnp.concatenate(
        [jnp.take_along_axis(table, tiles[k], axis=1, mode="promise_in_bounds") for k in range(tiles.shape[0])],
        axis=0,
    )
    return pick(cosine), pick(sine)


def turned(cosine, sine, real, imag):
    return cosine * real + sine * imag, cosine * imag - sine * real


def sign_rows(start, first, low, high, line):
    row = iota((8, start.shape[1]), 0)
    rows = jnp.broadcast_to(start, row.shape)
    for bit in range(low):
        rows = jnp.where(((row >> bit) & 1) == 1, rows * line(first + bit), rows)
    for bit in range(low, low + high):
        rows = jnp.concatenate([rows, rows * line(first + bit)], axis=0)
    return rows


def flips(positions, bonds):
    first, second = positions[:, 0:bonds], positions[:, 1 : bonds + 1]
    return lambda bit: jnp.where((first == bit) | (second == bit), F32(-1.0), F32(1.0))


def lane_part(positions, bonds):
    ones = jnp.ones((1, bonds), F32)
    return sign_rows(ones, 0, 3, LANE_BITS - 3, flips(positions, bonds)).astype(BF16)


def fields(weights, positions, lanes, device_bits, bonds, row_bits):
    differ = (device_bits >> positions[:, 0:bonds]) ^ (device_bits >> positions[:, 1 : bonds + 1])
    device_sign = (1 - 2 * (differ & 1)).astype(F32)
    line = flips(positions, bonds)
    stacked = jnp.concatenate(
        [sign_rows(w * device_sign, LANE_BITS, 3, row_bits - 3, line).astype(BF16) for w in weights],
        axis=0,
    )
    out = lax.dot_general(
        stacked, lanes, (((1,), (1,)), ((), ())), preferred_element_type=F32
    )
    rows = 2**row_bits
    return [out[k * rows : (k + 1) * rows] for k in range(len(weights))]


def energy(real, imag, field):
    return jnp.sum((real * real + imag * imag) * field)


def in_lanes(parts):
    lane = iota((1, LANES), 1)
    row = jnp.zeros((1, LANES), F32)
    for k, part in enumerate(parts):
        row = jnp.where(lane == k, part, row)
    return row


def evens(ref):
    half = ref.shape[0] // 2
    return ref[pl.ds(0, half, stride=2), :], ref[pl.ds(1, half, stride=2), :]


def take_blocks(ref, blocks, height, kept):
    def part(component):
        return jnp.concatenate(
            [ref[pl.ds(2 * k + component, blocks, stride=height), :] for k in range(kept)], axis=0
        )

    return part(0), part(1)


def put_blocks(ref, blocks, height, kept, real, imag):
    for k in range(kept):
        here = slice(k * blocks, (k + 1) * blocks)
        ref[pl.ds(2 * k, blocks, stride=height), :] = real[here]
        ref[pl.ds(2 * k + 1, blocks, stride=height), :] = imag[here]


def by_rows(gates, real, imag):
    both = product(gates, split(jnp.concatenate([real, imag], axis=1)))
    return both[:, :LANES], both[:, LANES:]


def by_blocks(gates, real, imag):
    size = gates[0].shape[0]
    pieces = [p[k : k + size] for p in (real, imag) for k in range(0, real.shape[0], size)]
    out = product(gates, split(jnp.concatenate(pieces, axis=1)))
    pieces = [out[:, k * LANES : (k + 1) * LANES] for k in range(len(pieces))]
    half = len(pieces) // 2
    return jnp.concatenate(pieces[:half], axis=0), jnp.concatenate(pieces[half:], axis=0)


def by_lanes(gates, real, imag):
    rows = real.shape[0]
    both = product(split(jnp.concatenate([real, imag], axis=0)), gates)
    return both[:rows], both[rows:]


def swap(buffer, plan_ref, slots):
    for i in range(SWAPS):
        @pl.when(i < plan_ref[0, SWAPPED])
        def _(i=i):
            height = 2 ** (slots - 1 - i)
            place = plan_ref[0, LANEQ + i]
            step = jnp.left_shift(jnp.int32(1), place)
            if height == 4:
                tiles = buffer[...].reshape(-1, 8, LANES)
                other = pltpu.roll(tiles, 4, 1)
                one = (iota((1, 8, LANES), 2) >> place) & 1
                same = one == (iota((1, 8, LANES), 1) >> 2)
                moved = jnp.where(one == 1, pltpu.roll(other, step, 2), pltpu.roll(other, LANES - step, 2))
                buffer[...] = jnp.where(same, tiles, moved).reshape(buffer.shape)
                return
            whole = buffer[...].reshape(-1, 2, height, LANES)
            low, high = whole[:, 0].reshape(-1, LANES), whole[:, 1].reshape(-1, LANES)
            one = ((iota((1, LANES), 1) >> place) & 1) == 1
            new_low = jnp.where(one, pltpu.roll(high, step, 1), low)
            new_high = jnp.where(one, high, pltpu.roll(low, LANES - step, 1))
            pairs = (new_low.reshape(-1, 1, height, LANES), new_high.reshape(-1, 1, height, LANES))
            buffer[...] = jnp.concatenate(pairs, axis=1).reshape(buffer.shape)


class Plan:
    def __init__(self, local_bits, global_bits):
        self.local_bits, self.global_bits = local_bits, global_bits
        self.qubits = local_bits + global_bits
        self.row_bits = local_bits - LANE_BITS
        self.rows = 2**self.row_bits
        self.blocks = 2**global_bits
        self.kept_bits = self.row_bits - global_bits
        self.kept = 2**self.kept_bits
        self.bonds = self.qubits - 1


def choose(plan, chain_ref, plan_ref):
    order = [chain_ref[0, k] for k in range(plan.qubits)]
    away = [(q >= plan.local_bits).astype(jnp.int32) for q in order]
    free = jnp.int32(0)
    for k, q in enumerate(order):
        near = away[k]
        if k:
            near = near | away[k - 1]
        if k + 1 < plan.qubits:
            near = near | away[k + 1]
        free = free | jnp.left_shift(1 - near, q)
    bit = lambda q: (free >> q) & 1
    row_qubits = range(LANE_BITS, plan.local_bits)
    free_rows = sum(bit(q) for q in row_qubits)
    slots = plan.global_bits
    free_lanes = sum(bit(q) for q in range(LANE_BITS))
    swapped = jnp.minimum(jnp.minimum(free_lanes, SWAPS), jnp.maximum(slots - free_rows, 0))
    late = jnp.maximum(slots - swapped - free_rows, 0)
    seen = jnp.int32(0)
    for k, q in enumerate(row_qubits):
        held = k - seen
        rank = jnp.where(bit(q) == 1, late + seen, jnp.where(held < late, held, free_rows + held))
        plan_ref[0, ROWQ + rank] = jnp.int32(q)
        seen = seen + bit(q)
    for i in range(SWAPS):
        plan_ref[0, LANEQ + i] = jnp.int32(-1)
    seen = jnp.int32(0)
    for q in range(LANE_BITS):
        taken = (bit(q) == 1) & (seen < swapped)
        plan_ref[0, jnp.where(taken, LANEQ + seen, SPARE)] = jnp.int32(q)
        seen = seen + bit(q)
    plan_ref[0, SWAPPED] = swapped
    plan_ref[0, LATE] = late


def touches(plan, chain, plan_ref, rows_from, rows_to, lanes):
    hit = jnp.zeros(chain.shape, jnp.int32)
    for b in range(plan.global_bits):
        wanted = (b >= rows_from) & (b < rows_to)
        hit = hit | (chain == jnp.where(wanted, plan_ref[0, ROWQ + b], -1)).astype(jnp.int32)
    if lanes:
        for i in range(SWAPS):
            hit = hit | (chain == plan_ref[0, LANEQ + i]).astype(jnp.int32)
    return (hit[:, 0 : plan.bonds] | hit[:, 1 : plan.bonds + 1]).astype(F32)


def ordered_positions(plan, chain, plan_ref):
    places = chain
    for b in range(plan.row_bits):
        places = jnp.where(chain == plan_ref[0, ROWQ + b], LANE_BITS + b, places)
    return places


def moved_positions(plan, chain, plan_ref):
    slots, swapped = plan.global_bits, plan_ref[0, SWAPPED]
    places = jnp.where(chain >= plan.local_bits, chain - plan.local_bits + LANE_BITS, chain)
    for b in range(plan.row_bits):
        target = jnp.int32(LANE_BITS + b)
        if b < slots:
            target = jnp.int32(plan.local_bits + b)
            i = slots - 1 - b
            if i < SWAPS:
                target = jnp.where(i < swapped, plan_ref[0, LANEQ + i], target)
        places = jnp.where(chain == plan_ref[0, ROWQ + b], target, places)
    for i in range(SWAPS):
        places = jnp.where(chain == plan_ref[0, LANEQ + i], plan.local_bits + slots - 1 - i, places)
    return places


def row_ones(plan, device):
    tile = bit_count(iota((8, LANES), 0), 3) + bit_count(iota((8, LANES), 1), LANE_BITS)
    tile = tile + bit_count(device, plan.global_bits)
    return jnp.concatenate([tile + k.bit_count() for k in range(plan.rows // 8)], axis=0)


def first_kernel(
    plan, rotation_ref, table_ref, order_ref, chain_ref, coupling_ref, bond_ref, amps_ref,
    out_ref, sums_ref, plan_ref, buffer,
):
    device = lax.axis_index("amp")
    bonds, rows = plan.bonds, plan.rows
    choose(plan, order_ref, plan_ref)
    chain = chain_ref[...]
    device_bits = device << plan.local_bits
    bond_signs = (2 * bond_ref[...] - 1).astype(F32)
    lanes = lane_part(chain, bonds)
    (steps,) = fields(
        [(coupling_ref[0:1, :] + 1).astype(F32) * bond_signs],
        chain, lanes, device_bits, bonds, plan.row_bits,
    )
    steps = steps + (UNITS // 2) * row_ones(plan, device).astype(F32)
    pair = lambda layer, q, keep=None: pair_of(layer, rotation_ref, table_ref, q, keep)

    real, imag = evens(amps_ref)
    norm = jnp.sum(real * real + imag * imag)
    real, imag = turned(*looked_up(steps), real, imag)
    ranked = [plan_ref[0, ROWQ + b] for b in range(plan.row_bits)]
    row_gate = gate([(q - LANE_BITS, *pair(0, q)) for q in ranked], rows)
    lane_gate = gate(lane_bits([pair(0, q) for q in range(LANE_BITS)]), LANES)
    real, imag = by_rows(split(row_gate), real, imag)
    real, imag = by_lanes(split(lane_gate), real, imag)

    late, slots = plan_ref[0, LATE], plan.global_bits - plan_ref[0, SWAPPED]
    early = touches(plan, chain, plan_ref, late, slots, True)
    weight = early * bond_signs
    steps, signs = fields(
        [(coupling_ref[1:2, :] + 1).astype(F32) * weight, weight],
        ordered_positions(plan, chain, plan_ref), lanes, device_bits, bonds, plan.row_bits,
    )
    sums_ref[...] = in_lanes([norm, energy(real, imag, signs)])
    real, imag = turned(*looked_up(steps), real, imag)
    bits = []
    for b in range(plan.global_bits):
        bits.append((b, *pair(1, ranked[b], (b >= late) & (b < slots))))
    real, imag = by_blocks(split(gate(bits, plan.blocks)), real, imag)
    pairs = []
    for q in range(LANE_BITS):
        keep = q == plan_ref[0, LANEQ]
        for i in range(1, SWAPS):
            keep = keep | (q == plan_ref[0, LANEQ + i])
        pairs.append(pair(1, q, keep))
    real, imag = by_lanes(split(gate(lane_bits(pairs), LANES)), real, imag)
    buffer[...] = jnp.concatenate([real, imag], axis=0)
    swap(buffer, plan_ref, plan.global_bits)
    put_blocks(out_ref, plan.blocks, 2 * plan.kept, plan.kept, buffer[:rows], buffer[rows:])


def prepare_kernel(
    plan, rotation_ref, table_ref, plan_ref, chain_ref, coupling_ref, bond_ref,
    mode_ref, cosine_ref, sine_ref, before_ref, after_ref, late_ref, *gate_refs,
):
    late_rows = plan_ref[0, LATE]
    mode_ref[0, 0] = jnp.minimum(late_rows, 2)
    device = lax.axis_index("amp")
    bonds, rows, slots = plan.bonds, plan.rows, plan.global_bits
    chain = chain_ref[...]
    bond_signs = (2 * bond_ref[...] - 1).astype(F32)
    rest = bond_signs * (1.0 - touches(plan, chain, plan_ref, late_rows, slots - plan_ref[0, SWAPPED], True))
    after_trade = jnp.where(late_rows >= 2, late_rows, 0)
    late = bond_signs * touches(plan, chain, plan_ref, 0, after_trade, False)
    moved = moved_positions(plan, chain, plan_ref)
    device_bits = device << plan.local_bits
    steps, before_ref[...], after_ref[...] = fields(
        [(coupling_ref[1:2, :] + 1).astype(F32) * rest, rest, bond_signs - late],
        moved, lane_part(moved, bonds), device_bits, bonds, plan.row_bits,
    )
    cosine_ref[...], sine_ref[...] = looked_up(steps)
    (late_ref[...],) = fields([late], chain, lane_part(chain, bonds), device_bits, bonds, plan.row_bits)
    pair = lambda layer, q, keep=None: pair_of(layer, rotation_ref, table_ref, q, keep)
    ranked = [plan_ref[0, ROWQ + b] for b in range(plan.row_bits)]
    far = [plan.local_bits + b for b in range(slots)]
    lane_pairs = []
    for q in range(LANE_BITS):
        held = jnp.int32(q)
        for i in range(SWAPS):
            held = jnp.where(plan_ref[0, LANEQ + i] == q, ranked[slots - 1 - i], held)
        lane_pairs.append(pair(1, held))
    back = []
    for b in range(plan.row_bits):
        cosine, sine = pair(1, ranked[b], b < after_trade)
        back.append((ranked[b] - LANE_BITS, cosine, -sine))
    gates = [
        gate([(b, *pair(0, q)) for b, q in enumerate(far)], plan.blocks),
        gate([(b, *pair(1, q)) for b, q in enumerate(far + ranked[slots:])], rows),
        gate(lane_bits(lane_pairs), LANES),
        gate(back, rows).T,
    ]
    for k, made in enumerate(gates):
        gate_refs[2 * k][...], gate_refs[2 * k + 1][...] = split(made)


def middle(plan, state_ref, cosine_ref, sine_ref, before_ref, gates):
    ga, gb, ha, hb, la, lb = gates
    real, imag = take_blocks(state_ref, plan.blocks, 2 * plan.kept, plan.kept)
    real, imag = by_blocks((ga[...], gb[...]), real, imag)
    before = energy(real, imag, before_ref[...])
    real, imag = turned(cosine_ref[...], sine_ref[...], real, imag)
    real, imag = by_rows((ha[...], hb[...]), real, imag)
    return *by_lanes((la[...], lb[...]), real, imag), before


def pack(plan, out_ref, real, imag, sums):
    blocks, kept = plan.blocks, plan.kept
    height = 2 * kept + 1
    put_blocks(out_ref, blocks, height, kept, real, imag)
    out_ref[pl.ds(2 * kept, blocks, stride=height), :] = jnp.broadcast_to(sums, (blocks, LANES))


def middle_kernel(plan, state_ref, cosine_ref, sine_ref, before_ref, after_ref, sums_ref, *refs):
    real, imag, before = middle(plan, state_ref, cosine_ref, sine_ref, before_ref, refs[:6])
    after = energy(real, imag, after_ref[...])
    pack(plan, refs[6], real, imag, sums_ref[...] + in_lanes([F32(0.0), before, after]))


def open_kernel(plan, state_ref, cosine_ref, sine_ref, before_ref, sums_ref, *refs):
    gates, (out_ref, sums_out_ref) = refs[:6], refs[6:]
    real, imag, before = middle(plan, state_ref, cosine_ref, sine_ref, before_ref, gates)
    out_ref[...] = jnp.concatenate([real, imag], axis=0)
    sums_out_ref[...] = sums_ref[...] + in_lanes([F32(0.0), before])


def close_kernel(plan, rotation_ref, table_ref, plan_ref, own_ref, other_ref, after_ref, sums_ref, out_ref):
    cosine, sine = pair_of(1, rotation_ref, table_ref, plan_ref[0, ROWQ])
    sine = jnp.where((lax.axis_index("amp") & 1) == 1, -sine, sine)
    both = cosine * own_ref[...] + sine * other_ref[...]
    real, imag = both[: plan.rows], both[plan.rows :]
    after = energy(real, imag, after_ref[...])
    pack(plan, out_ref, real, imag, sums_ref[...] + in_lanes([F32(0.0), F32(0.0), after]))


def last_kernel(plan, plan_ref, state_ref, ga, gb, *refs):
    late_ref, (out_ref, energies_ref, *late_out_ref, buffer) = refs[:-3][:1], refs[-4 if len(refs) == 5 else -3 :]
    device = lax.axis_index("amp")
    blocks, kept, rows = plan.blocks, plan.kept, plan.rows
    height = 2 * kept + 1
    sums = jnp.sum(state_ref[pl.ds(2 * kept, blocks, stride=height), :], axis=0, keepdims=True)
    amps = float(2**plan.qubits)
    mean = sums[:, 0:1] / amps + 1e-06
    factor = 1.0 / jnp.sqrt(mean)
    square = factor * factor / amps
    energies_ref[...] = sums[:, 1 : 1 + LAYERS] * square
    real, imag = take_blocks(state_ref, blocks, height, kept)
    buffer[...] = jnp.concatenate([real, imag], axis=0)
    swap(buffer, plan_ref, plan.global_bits)
    real, imag = by_rows((ga[...], gb[...]), buffer[:rows], buffer[rows:])
    if late_ref:
        late_out_ref[0][...] = in_lanes([0.0, energy(real, imag, late_ref[0][...])])[:, 0:LAYERS] * square
    ones = row_ones(plan, device)
    odd = (ones & 1) == 1
    real, imag = jnp.where(odd, imag, real), jnp.where(odd, real, imag)
    real = jnp.where(((ones + 1) & 2) == 2, -factor, factor) * real
    imag = jnp.where((ones & 2) == 2, -factor, factor) * imag
    out_ref[pl.ds(0, rows, stride=2), :] = real
    out_ref[pl.ds(1, rows, stride=2), :] = imag


def spec(space):
    return pl.BlockSpec(memory_space=space)


def call(kernel, shapes, scalars, arrays, name, spaces=None, scratch=(), near=0, held=(), far=()):
    kept = len(arrays) - near
    arrays = tuple(
        pltpu.with_memory_space_constraint(a, pltpu.VMEM) if k >= kept else a
        for k, a in enumerate(arrays)
    )
    shapes = tuple(
        pltpu.VMEM(s.shape, s.dtype) if k in held else pltpu.HBM(s.shape, s.dtype) if k in far else s
        for k, s in enumerate(shapes)
    )
    return pl.pallas_call(
        kernel,
        out_shape=shapes,
        in_specs=[spec(pltpu.SMEM)] * len(scalars) + [spec(pltpu.VMEM)] * len(arrays),
        out_specs=tuple(spec(s) for s in spaces or (pltpu.VMEM,) * len(shapes)),
        scratch_shapes=scratch,
        name=name,
    )(*scalars, *arrays)


def local(amplitudes, coupling_index, rotation_index, chain_order, bond_sign):
    local_bits = amplitudes.shape[1].bit_length() - 1
    size = lax.axis_size("amp")
    plan = Plan(local_bits, size.bit_length() - 1)
    rows = plan.rows
    shape = jax.ShapeDtypeStruct
    bind = lambda kernel: lambda *refs: kernel(plan, *refs)

    state = amplitudes.reshape(2, rows, LANES).transpose(1, 0, 2).reshape(2 * rows, LANES)
    table = jnp.asarray(angle_tables())
    chain, bond = chain_order.reshape(1, -1), bond_sign.reshape(1, -1)
    small = (chain, coupling_index, bond)
    whole = shape((2 * rows, LANES), F32)
    field = shape((rows, LANES), F32)
    square_of = lambda n: shape((n, n), BF16)
    buffer = (pltpu.VMEM((2 * rows, LANES), F32),)

    state, sums, chosen = call(
        bind(first_kernel),
        (whole, shape((1, LANES), F32), shape((1, PLAN), jnp.int32)),
        (rotation_index, table, chain), (*small, state), "first",
        (pltpu.VMEM, pltpu.VMEM, pltpu.SMEM), buffer, held=(0, 1),
    )
    sizes = (size, rows, LANES, rows)
    made = call(
        bind(prepare_kernel),
        (shape((1, 1), jnp.int32),) + (field,) * 5 + tuple(square_of(n) for n in sizes for _ in range(2)),
        (rotation_index, table, chosen), small, "prepare",
        (pltpu.SMEM,) + (pltpu.VMEM,) * 13, held=range(1, 14),
    )
    mode, fields_made, late, gates = made[0], made[1:5], made[5], made[6:]
    state = lax.all_to_all(state.reshape(size, 2 * plan.kept, LANES), "amp", 0, 0, tiled=True)
    state = state.reshape(2 * rows, LANES)
    height = 2 * plan.kept + 1
    pair = shape((1, LAYERS), F32)

    packed = (shape((size * height, LANES), F32),)

    def straight(state, sums, chosen, made):
        return call(
            bind(middle_kernel), packed, (), (state, *made[:4], sums, *made[4:10]),
            "middle", near=12, held=(0,),
        )

    def paired(state, sums, chosen, made):
        own, sums = call(
            bind(open_kernel), (whole, shape((1, LANES), F32)), (),
            (state, *made[:3], sums, *made[4:10]), "open", near=11, held=(0, 1),
        )
        other = lax.ppermute(own, "amp", [(k, k ^ 1) for k in range(size)])
        return call(
            bind(close_kernel), packed, (rotation_index, table, chosen),
            (own, other, made[3], sums), "close", near=4, held=(0,),
        )

    def end(middle_of, state, sums, chosen, made, *late):
        (state,) = middle_of(state, sums, chosen, made)
        state = lax.all_to_all(state.reshape(size, height, 1, LANES), "amp", 0, 0, tiled=True)
        return call(
            bind(last_kernel), (whole, pair) + (pair,) * len(late), (chosen,),
            (state.reshape(size * height, LANES), *made[10:], *late), "last",
            scratch=buffer, near=3 + len(late), far=() if late else (0, 1),
        )

    def apart(final):
        return final.reshape(rows, 2, LANES).transpose(1, 0, 2).reshape(2, rows * LANES)

    def none_late(*operands):
        final, energies = end(straight, *operands[:-1])
        return apart(final), energies.reshape(LAYERS)

    def one_late(*operands):
        final, energies = end(paired, *operands[:-1])
        return apart(final), energies.reshape(LAYERS)

    def more_late(*operands):
        final, energies, extra = end(straight, *operands)
        sent = jnp.broadcast_to(extra[None], (size, 1, LAYERS))
        total = energies + lax.all_to_all(sent, "amp", 0, 0, tiled=True).sum(axis=0)
        return apart(final), total.reshape(LAYERS)

    return lax.switch(
        mode[0, 0], (none_late, one_late, more_late),
        state, sums, chosen, (*fields_made, *gates), late,
    )


def solution(mesh):
    in_specs = (P(None, ("rep", "amp")), P("rep", None), P("rep", None), P(), P())
    out_specs = (P(None, ("rep", "amp")), P("rep"))
    return jax.shard_map(local, mesh=mesh, in_specs=in_specs, out_specs=out_specs, check_vma=False)
```

```python
import numpy as np
import jax
import jax.numpy as jnp
from jax import lax
from jax.experimental import pallas as pl
from jax.experimental.pallas import tpu as pltpu
from jax.sharding import PartitionSpec as P

LAYERS = 2
ANGLES = 16
UNITS = 2 * (ANGLES + 1)
LANE_BITS = 7
LANES = 128

F32 = jnp.float32
BF16 = jnp.bfloat16


def angle_tables():
    steps = (np.arange(ANGLES, dtype=np.float64) + 1.0) * (np.pi / UNITS)
    return np.stack([np.cos(steps), np.sin(steps)]).astype(np.float32)


def iota(shape, dimension):
    return lax.broadcasted_iota(jnp.int32, shape, dimension)


def bit_count(values, width):
    total = values & 1
    for bit in range(1, width):
        total = total + ((values >> bit) & 1)
    return total


def split(values):
    high = values.astype(BF16)
    return high, (values - high.astype(F32)).astype(BF16)


def dot(left, right):
    return jnp.dot(left, right, preferred_element_type=F32)


def product(left, right):
    return dot(
        jnp.concatenate([left[0], left[0], left[1]], axis=1),
        jnp.concatenate([right[0], right[1], right[0]], axis=0),
    )


SWAPS = 4
ROWQ, LANEQ, SWAPPED, LATE, SPARE, PLAN = 0, 8, 12, 13, 14, 16


def gate(bits, width):
    column = iota((1, width), 1)
    lines = []
    for place, cosine, sine in bits:
        one = ((column >> place) & 1) == 1
        lines.append((jnp.where(one, sine, cosine), jnp.where(one, cosine, -sine)))
    row = iota((8, width), 0)
    matrix = None
    for bit, (zero_line, one_line) in enumerate(lines[:3]):
        factor = jnp.where(((row >> bit) & 1) == 1, one_line, zero_line)
        matrix = factor if matrix is None else matrix * factor
    for zero_line, one_line in lines[3:]:
        matrix = jnp.concatenate([matrix * zero_line, matrix * one_line], axis=0)
    return matrix


def lane_bits(pairs):
    return [(place, cosine, -sine) for place, (cosine, sine) in enumerate(pairs)]


def pair_of(layer, rotation_ref, table_ref, qubit, keep=None):
    index = rotation_ref[layer, qubit]
    cosine, sine = table_ref[0, index], table_ref[1, index]
    if keep is None:
        return cosine, sine
    return jnp.where(keep, cosine, F32(1.0)), jnp.where(keep, sine, F32(0.0))


def cos_sin(steps):
    quarter = UNITS // 2
    turns = jnp.floor(steps * (1.0 / quarter) + 0.5)
    angle = (steps - turns * quarter) * (np.pi / UNITS)
    square = angle * angle
    sine = angle * (
        1.0 + square * (-1.0 / 6 + square * (1.0 / 120 + square * (-1.0 / 5040 + square * (1.0 / 362880))))
    )
    cosine = 1.0 + square * (
        -0.5 + square * (1.0 / 24 + square * (-1.0 / 720 + square * (1.0 / 40320)))
    )
    turns = turns.astype(jnp.int32)
    odd = (turns & 1) == 1
    cosine, sine = jnp.where(odd, sine, cosine), jnp.where(odd, cosine, sine)
    return (
        jnp.where(((turns + 1) & 2) == 2, -cosine, cosine),
        jnp.where((turns & 2) == 2, -sine, sine),
    )


def looked_up(steps):
    period = 2 * UNITS
    place = (steps - period * jnp.floor(steps * (1.0 / period) + 0.25 / period)).astype(jnp.int32)
    cosine, sine = cos_sin(iota((8, LANES), 1).astype(F32))
    tiles = place.reshape(-1, 8, LANES)
    pick = lambda table: jnp.concatenate(
        [jnp.take_along_axis(table, tiles[k], axis=1, mode="promise_in_bounds") for k in range(tiles.shape[0])],
        axis=0,
    )
    return pick(cosine), pick(sine)


def turned(cosine, sine, real, imag):
    return cosine * real + sine * imag, cosine * imag - sine * real


def sign_rows(start, first, low, high, line):
    row = iota((8, start.shape[1]), 0)
    rows = jnp.broadcast_to(start, row.shape)
    for bit in range(low):
        rows = jnp.where(((row >> bit) & 1) == 1, rows * line(first + bit), rows)
    for bit in range(low, low + high):
        rows = jnp.concatenate([rows, rows * line(first + bit)], axis=0)
    return rows


def flips(positions, bonds):
    first, second = positions[:, 0:bonds], positions[:, 1 : bonds + 1]
    return lambda bit: jnp.where((first == bit) | (second == bit), F32(-1.0), F32(1.0))


def lane_part(positions, bonds):
    ones = jnp.ones((1, bonds), F32)
    return sign_rows(ones, 0, 3, LANE_BITS - 3, flips(positions, bonds)).astype(BF16)


def fields(weights, positions, lanes, device_bits, bonds, row_bits):
    differ = (device_bits >> positions[:, 0:bonds]) ^ (device_bits >> positions[:, 1 : bonds + 1])
    device_sign = (1 - 2 * (differ & 1)).astype(F32)
    line = flips(positions, bonds)
    stacked = jnp.concatenate(
        [sign_rows(w * device_sign, LANE_BITS, 3, row_bits - 3, line).astype(BF16) for w in weights],
        axis=0,
    )
    out = lax.dot_general(
        stacked, lanes, (((1,), (1,)), ((), ())), preferred_element_type=F32
    )
    rows = 2**row_bits
    return [out[k * rows : (k + 1) * rows] for k in range(len(weights))]


def energy(real, imag, field):
    return jnp.sum((real * real + imag * imag) * field)


def in_lanes(parts):
    lane = iota((1, LANES), 1)
    row = jnp.zeros((1, LANES), F32)
    for k, part in enumerate(parts):
        row = jnp.where(lane == k, part, row)
    return row


def evens(ref):
    half = ref.shape[0] // 2
    return ref[pl.ds(0, half, stride=2), :], ref[pl.ds(1, half, stride=2), :]


def take_blocks(ref, blocks, height, kept):
    def part(component):
        return jnp.concatenate(
            [ref[pl.ds(2 * k + component, blocks, stride=height), :] for k in range(kept)], axis=0
        )

    return part(0), part(1)


def put_blocks(ref, blocks, height, kept, real, imag):
    for k in range(kept):
        here = slice(k * blocks, (k + 1) * blocks)
        ref[pl.ds(2 * k, blocks, stride=height), :] = real[here]
        ref[pl.ds(2 * k + 1, blocks, stride=height), :] = imag[here]


def by_rows(gates, real, imag):
    both = product(gates, split(jnp.concatenate([real, imag], axis=1)))
    return both[:, :LANES], both[:, LANES:]


def by_blocks(gates, real, imag):
    size = gates[0].shape[0]
    pieces = [p[k : k + size] for p in (real, imag) for k in range(0, real.shape[0], size)]
    out = product(gates, split(jnp.concatenate(pieces, axis=1)))
    pieces = [out[:, k * LANES : (k + 1) * LANES] for k in range(len(pieces))]
    half = len(pieces) // 2
    return jnp.concatenate(pieces[:half], axis=0), jnp.concatenate(pieces[half:], axis=0)


def by_lanes(gates, real, imag):
    rows = real.shape[0]
    both = product(split(jnp.concatenate([real, imag], axis=0)), gates)
    return both[:rows], both[rows:]


def swap(buffer, plan_ref, slots):
    for i in range(SWAPS):
        @pl.when(i < plan_ref[0, SWAPPED])
        def _(i=i):
            height = 2 ** (slots - 1 - i)
            place = plan_ref[0, LANEQ + i]
            step = jnp.left_shift(jnp.int32(1), place)
            if height == 4:
                tiles = buffer[...].reshape(-1, 8, LANES)
                other = pltpu.roll(tiles, 4, 1)
                one = (iota((1, 8, LANES), 2) >> place) & 1
                same = one == (iota((1, 8, LANES), 1) >> 2)
                moved = jnp.where(one == 1, pltpu.roll(other, step, 2), pltpu.roll(other, LANES - step, 2))
                buffer[...] = jnp.where(same, tiles, moved).reshape(buffer.shape)
                return
            whole = buffer[...].reshape(-1, 2, height, LANES)
            low, high = whole[:, 0].reshape(-1, LANES), whole[:, 1].reshape(-1, LANES)
            one = ((iota((1, LANES), 1) >> place) & 1) == 1
            new_low = jnp.where(one, pltpu.roll(high, step, 1), low)
            new_high = jnp.where(one, high, pltpu.roll(low, LANES - step, 1))
            pairs = (new_low.reshape(-1, 1, height, LANES), new_high.reshape(-1, 1, height, LANES))
            buffer[...] = jnp.concatenate(pairs, axis=1).reshape(buffer.shape)


class Plan:
    def __init__(self, local_bits, global_bits):
        self.local_bits, self.global_bits = local_bits, global_bits
        self.qubits = local_bits + global_bits
        self.row_bits = local_bits - LANE_BITS
        self.rows = 2**self.row_bits
        self.blocks = 2**global_bits
        self.kept_bits = self.row_bits - global_bits
        self.kept = 2**self.kept_bits
        self.bonds = self.qubits - 1


def choose(plan, chain_ref, plan_ref):
    order = [chain_ref[0, k] for k in range(plan.qubits)]
    away = [(q >= plan.local_bits).astype(jnp.int32) for q in order]
    free = jnp.int32(0)
    for k, q in enumerate(order):
        near = away[k]
        if k:
            near = near | away[k - 1]
        if k + 1 < plan.qubits:
            near = near | away[k + 1]
        free = free | jnp.left_shift(1 - near, q)
    bit = lambda q: (free >> q) & 1
    row_qubits = range(LANE_BITS, plan.local_bits)
    free_rows = sum(bit(q) for q in row_qubits)
    slots = plan.global_bits
    free_lanes = sum(bit(q) for q in range(LANE_BITS))
    swapped = jnp.minimum(jnp.minimum(free_lanes, SWAPS), jnp.maximum(slots - free_rows, 0))
    late = jnp.maximum(slots - swapped - free_rows, 0)
    seen = jnp.int32(0)
    for k, q in enumerate(row_qubits):
        held = k - seen
        rank = jnp.where(bit(q) == 1, late + seen, jnp.where(held < late, held, free_rows + held))
        plan_ref[0, ROWQ + rank] = jnp.int32(q)
        seen = seen + bit(q)
    for i in range(SWAPS):
        plan_ref[0, LANEQ + i] = jnp.int32(-1)
    seen = jnp.int32(0)
    for q in range(LANE_BITS):
        taken = (bit(q) == 1) & (seen < swapped)
        plan_ref[0, jnp.where(taken, LANEQ + seen, SPARE)] = jnp.int32(q)
        seen = seen + bit(q)
    plan_ref[0, SWAPPED] = swapped
    plan_ref[0, LATE] = late


def touches(plan, chain, plan_ref, rows_from, rows_to, lanes):
    hit = jnp.zeros(chain.shape, jnp.int32)
    for b in range(plan.global_bits):
        wanted = (b >= rows_from) & (b < rows_to)
        hit = hit | (chain == jnp.where(wanted, plan_ref[0, ROWQ + b], -1)).astype(jnp.int32)
    if lanes:
        for i in range(SWAPS):
            hit = hit | (chain == plan_ref[0, LANEQ + i]).astype(jnp.int32)
    return (hit[:, 0 : plan.bonds] | hit[:, 1 : plan.bonds + 1]).astype(F32)


def ordered_positions(plan, chain, plan_ref):
    places = chain
    for b in range(plan.row_bits):
        places = jnp.where(chain == plan_ref[0, ROWQ + b], LANE_BITS + b, places)
    return places


def moved_positions(plan, chain, plan_ref):
    slots, swapped = plan.global_bits, plan_ref[0, SWAPPED]
    places = jnp.where(chain >= plan.local_bits, chain - plan.local_bits + LANE_BITS, chain)
    for b in range(plan.row_bits):
        target = jnp.int32(LANE_BITS + b)
        if b < slots:
            target = jnp.int32(plan.local_bits + b)
            i = slots - 1 - b
            if i < SWAPS:
                target = jnp.where(i < swapped, plan_ref[0, LANEQ + i], target)
        places = jnp.where(chain == plan_ref[0, ROWQ + b], target, places)
    for i in range(SWAPS):
        places = jnp.where(chain == plan_ref[0, LANEQ + i], plan.local_bits + slots - 1 - i, places)
    return places


def row_ones(plan, device):
    tile = bit_count(iota((8, LANES), 0), 3) + bit_count(iota((8, LANES), 1), LANE_BITS)
    tile = tile + bit_count(device, plan.global_bits)
    return jnp.concatenate([tile + k.bit_count() for k in range(plan.rows // 8)], axis=0)


def first_kernel(
    plan, rotation_ref, table_ref, order_ref, chain_ref, coupling_ref, bond_ref, amps_ref,
    out_ref, sums_ref, plan_ref, buffer,
):
    device = lax.axis_index("amp")
    bonds, rows = plan.bonds, plan.rows
    choose(plan, order_ref, plan_ref)
    chain = chain_ref[...]
    device_bits = device << plan.local_bits
    bond_signs = (2 * bond_ref[...] - 1).astype(F32)
    lanes = lane_part(chain, bonds)
    (steps,) = fields(
        [(coupling_ref[0:1, :] + 1).astype(F32) * bond_signs],
        chain, lanes, device_bits, bonds, plan.row_bits,
    )
    steps = steps + (UNITS // 2) * row_ones(plan, device).astype(F32)
    pair = lambda layer, q, keep=None: pair_of(layer, rotation_ref, table_ref, q, keep)

    real, imag = evens(amps_ref)
    norm = jnp.sum(real * real + imag * imag)
    real, imag = turned(*looked_up(steps), real, imag)
    ranked = [plan_ref[0, ROWQ + b] for b in range(plan.row_bits)]
    row_gate = gate([(q - LANE_BITS, *pair(0, q)) for q in ranked], rows)
    lane_gate = gate(lane_bits([pair(0, q) for q in range(LANE_BITS)]), LANES)
    real, imag = by_rows(split(row_gate), real, imag)
    real, imag = by_lanes(split(lane_gate), real, imag)

    late, slots = plan_ref[0, LATE], plan.global_bits - plan_ref[0, SWAPPED]
    early = touches(plan, chain, plan_ref, late, slots, True)
    weight = early * bond_signs
    steps, signs = fields(
        [(coupling_ref[1:2, :] + 1).astype(F32) * weight, weight],
        ordered_positions(plan, chain, plan_ref), lanes, device_bits, bonds, plan.row_bits,
    )
    sums_ref[...] = in_lanes([norm, energy(real, imag, signs)])
    real, imag = turned(*looked_up(steps), real, imag)
    bits = []
    for b in range(plan.global_bits):
        bits.append((b, *pair(1, ranked[b], (b >= late) & (b < slots))))
    real, imag = by_blocks(split(gate(bits, plan.blocks)), real, imag)
    pairs = []
    for q in range(LANE_BITS):
        keep = q == plan_ref[0, LANEQ]
        for i in range(1, SWAPS):
            keep = keep | (q == plan_ref[0, LANEQ + i])
        pairs.append(pair(1, q, keep))
    real, imag = by_lanes(split(gate(lane_bits(pairs), LANES)), real, imag)
    buffer[...] = jnp.concatenate([real, imag], axis=0)
    swap(buffer, plan_ref, plan.global_bits)
    put_blocks(out_ref, plan.blocks, 2 * plan.kept, plan.kept, buffer[:rows], buffer[rows:])


def prepare_kernel(
    plan, rotation_ref, table_ref, plan_ref, chain_ref, coupling_ref, bond_ref,
    mode_ref, cosine_ref, sine_ref, before_ref, after_ref, late_ref, turn_ref, *gate_refs,
):
    late_rows = plan_ref[0, LATE]
    mode_ref[0, 0] = jnp.minimum(late_rows, 2)
    device = lax.axis_index("amp")
    bonds, rows, slots = plan.bonds, plan.rows, plan.global_bits
    chain = chain_ref[...]
    bond_signs = (2 * bond_ref[...] - 1).astype(F32)
    rest = bond_signs * (1.0 - touches(plan, chain, plan_ref, late_rows, slots - plan_ref[0, SWAPPED], True))
    after_trade = jnp.where(late_rows >= 2, late_rows, 0)
    late = bond_signs * touches(plan, chain, plan_ref, 0, after_trade, False)
    moved = moved_positions(plan, chain, plan_ref)
    device_bits = device << plan.local_bits
    steps, before_ref[...], after_ref[...] = fields(
        [(coupling_ref[1:2, :] + 1).astype(F32) * rest, rest, bond_signs - late],
        moved, lane_part(moved, bonds), device_bits, bonds, plan.row_bits,
    )
    cosine_ref[...], sine_ref[...] = looked_up(steps)
    (late_ref[...],) = fields([late], chain, lane_part(chain, bonds), device_bits, bonds, plan.row_bits)
    pair = lambda layer, q, keep=None: pair_of(layer, rotation_ref, table_ref, q, keep)
    ranked = [plan_ref[0, ROWQ + b] for b in range(plan.row_bits)]
    cosine, sine = pair(1, ranked[0])
    turn_ref[...] = in_lanes([cosine, jnp.where((device & 1) == 1, -sine, sine)])
    far = [plan.local_bits + b for b in range(slots)]
    lane_pairs = []
    for q in range(LANE_BITS):
        held = jnp.int32(q)
        for i in range(SWAPS):
            held = jnp.where(plan_ref[0, LANEQ + i] == q, ranked[slots - 1 - i], held)
        lane_pairs.append(pair(1, held))
    back = []
    for b in range(plan.row_bits):
        cosine, sine = pair(1, ranked[b], b < after_trade)
        back.append((ranked[b] - LANE_BITS, cosine, -sine))
    gates = [
        gate([(b, *pair(0, q)) for b, q in enumerate(far)], plan.blocks),
        gate([(b, *pair(1, q)) for b, q in enumerate(far + ranked[slots:])], rows),
        gate(lane_bits(lane_pairs), LANES),
        gate(back, rows).T,
    ]
    for k, made in enumerate(gates):
        gate_refs[2 * k][...], gate_refs[2 * k + 1][...] = split(made)


def middle(plan, state_ref, cosine_ref, sine_ref, before_ref, gates):
    ga, gb, ha, hb, la, lb = gates
    real, imag = take_blocks(state_ref, plan.blocks, 2 * plan.kept, plan.kept)
    real, imag = by_blocks((ga[...], gb[...]), real, imag)
    before = energy(real, imag, before_ref[...])
    real, imag = turned(cosine_ref[...], sine_ref[...], real, imag)
    real, imag = by_rows((ha[...], hb[...]), real, imag)
    return *by_lanes((la[...], lb[...]), real, imag), before


def pack(plan, out_ref, real, imag, sums):
    blocks, kept = plan.blocks, plan.kept
    height = 2 * kept + 1
    put_blocks(out_ref, blocks, height, kept, real, imag)
    out_ref[pl.ds(2 * kept, blocks, stride=height), :] = jnp.broadcast_to(sums, (blocks, LANES))


def middle_kernel(plan, state_ref, cosine_ref, sine_ref, before_ref, after_ref, sums_ref, *refs):
    real, imag, before = middle(plan, state_ref, cosine_ref, sine_ref, before_ref, refs[:6])
    after = energy(real, imag, after_ref[...])
    pack(plan, refs[6], real, imag, sums_ref[...] + in_lanes([F32(0.0), before, after]))


def open_kernel(plan, state_ref, cosine_ref, sine_ref, before_ref, sums_ref, *refs):
    gates, (out_ref, sums_out_ref) = refs[:6], refs[6:]
    real, imag, before = middle(plan, state_ref, cosine_ref, sine_ref, before_ref, gates)
    out_ref[...] = jnp.concatenate([real, imag], axis=0)
    sums_out_ref[...] = sums_ref[...] + in_lanes([F32(0.0), before])


def close_kernel(plan, own_ref, other_ref, turn_ref, after_ref, sums_ref, out_ref):
    both = turn_ref[0:1, 0:1] * own_ref[...] + turn_ref[0:1, 1:2] * other_ref[...]
    real, imag = both[: plan.rows], both[plan.rows :]
    after = energy(real, imag, after_ref[...])
    pack(plan, out_ref, real, imag, sums_ref[...] + in_lanes([F32(0.0), F32(0.0), after]))


def last_kernel(plan, plan_ref, state_ref, ga, gb, *refs):
    late_ref, (out_ref, energies_ref, *late_out_ref, buffer) = refs[:-3][:1], refs[-4 if len(refs) == 5 else -3 :]
    device = lax.axis_index("amp")
    blocks, kept, rows = plan.blocks, plan.kept, plan.rows
    height = 2 * kept + 1
    sums = jnp.sum(state_ref[pl.ds(2 * kept, blocks, stride=height), :], axis=0, keepdims=True)
    amps = float(2**plan.qubits)
    mean = sums[:, 0:1] / amps + 1e-06
    factor = 1.0 / jnp.sqrt(mean)
    square = factor * factor / amps
    energies_ref[...] = sums[:, 1 : 1 + LAYERS] * square
    real, imag = take_blocks(state_ref, blocks, height, kept)
    buffer[...] = jnp.concatenate([real, imag], axis=0)
    swap(buffer, plan_ref, plan.global_bits)
    real, imag = by_rows((ga[...], gb[...]), buffer[:rows], buffer[rows:])
    if late_ref:
        late_out_ref[0][...] = in_lanes([0.0, energy(real, imag, late_ref[0][...])])[:, 0:LAYERS] * square
    ones = row_ones(plan, device)
    odd = (ones & 1) == 1
    real, imag = jnp.where(odd, imag, real), jnp.where(odd, real, imag)
    real = jnp.where(((ones + 1) & 2) == 2, -factor, factor) * real
    imag = jnp.where((ones & 2) == 2, -factor, factor) * imag
    out_ref[pl.ds(0, rows, stride=2), :] = real
    out_ref[pl.ds(1, rows, stride=2), :] = imag


def spec(space):
    return pl.BlockSpec(memory_space=space)


def call(kernel, shapes, scalars, arrays, name, spaces=None, scratch=(), near=0, held=(), far=(), plan=None):
    kept = len(arrays) - near
    arrays = tuple(
        pltpu.with_memory_space_constraint(a, pltpu.VMEM) if k >= kept else a
        for k, a in enumerate(arrays)
    )
    if plan is not None:
        scalars = (*scalars, pltpu.with_memory_space_constraint(plan, pltpu.SMEM))
    spaces = spaces or (pltpu.VMEM,) * len(shapes)
    shapes = tuple(
        spaces[k](s.shape, s.dtype) if k in held else pltpu.HBM(s.shape, s.dtype) if k in far else s
        for k, s in enumerate(shapes)
    )
    return pl.pallas_call(
        kernel,
        out_shape=shapes,
        in_specs=[spec(pltpu.SMEM)] * len(scalars) + [spec(pltpu.VMEM)] * len(arrays),
        out_specs=tuple(spec(s) for s in spaces),
        scratch_shapes=scratch,
        name=name,
    )(*scalars, *arrays)


def local(amplitudes, coupling_index, rotation_index, chain_order, bond_sign):
    local_bits = amplitudes.shape[1].bit_length() - 1
    size = lax.axis_size("amp")
    plan = Plan(local_bits, size.bit_length() - 1)
    rows = plan.rows
    shape = jax.ShapeDtypeStruct
    bind = lambda kernel: lambda *refs: kernel(plan, *refs)

    state = amplitudes.reshape(2, rows, LANES).transpose(1, 0, 2).reshape(2 * rows, LANES)
    table = jnp.asarray(angle_tables())
    chain, bond = chain_order.reshape(1, -1), bond_sign.reshape(1, -1)
    small = (chain, coupling_index, bond)
    whole = shape((2 * rows, LANES), F32)
    field, line = shape((rows, LANES), F32), shape((1, LANES), F32)
    square_of = lambda n: shape((n, n), BF16)
    buffer = (pltpu.VMEM((2 * rows, LANES), F32),)

    state, sums, chosen = call(
        bind(first_kernel),
        (whole, line, shape((1, PLAN), jnp.int32)),
        (rotation_index, table, chain), (*small, state), "first",
        (pltpu.VMEM, pltpu.VMEM, pltpu.SMEM), buffer, held=(0, 1, 2),
    )
    sizes = (size, rows, LANES, rows)
    made = call(
        bind(prepare_kernel),
        (shape((1, 1), jnp.int32),) + (field,) * 5 + (line,)
        + tuple(square_of(n) for n in sizes for _ in range(2)),
        (rotation_index, table), small, "prepare",
        (pltpu.SMEM,) + (pltpu.VMEM,) * 14, held=range(1, 15), plan=chosen,
    )
    mode, fields_made, late, turn, gates = made[0], made[1:5], made[5], made[6], made[7:]
    state = lax.all_to_all(state.reshape(size, 2 * plan.kept, LANES), "amp", 0, 0, tiled=True)
    state = state.reshape(2 * rows, LANES)
    height = 2 * plan.kept + 1
    pair = shape((1, LAYERS), F32)

    packed = (shape((size * height, LANES), F32),)

    def straight(state, sums, turn, made):
        return call(
            bind(middle_kernel), packed, (), (state, *made[:4], sums, *made[4:10]),
            "middle", near=12, held=(0,),
        )

    def paired(state, sums, turn, made):
        own, sums = call(
            bind(open_kernel), (whole, line), (),
            (state, *made[:3], sums, *made[4:10]), "open", near=11, held=(0, 1),
        )
        other = lax.ppermute(own, "amp", [(k, k ^ 1) for k in range(size)])
        return call(
            bind(close_kernel), packed, (),
            (own, other, turn, made[3], sums), "close", near=5, held=(0,),
        )

    def end(middle_of, state, sums, turn, chosen, made, *late):
        (state,) = middle_of(state, sums, turn, made)
        state = lax.all_to_all(state.reshape(size, height, 1, LANES), "amp", 0, 0, tiled=True)
        return call(
            bind(last_kernel), (whole, pair) + (pair,) * len(late), (),
            (state.reshape(size * height, LANES), *made[10:], *late), "last",
            scratch=buffer, near=3 + len(late), far=() if late else (0, 1), plan=chosen,
        )

    def apart(final):
        return final.reshape(rows, 2, LANES).transpose(1, 0, 2).reshape(2, rows * LANES)

    def none_late(*operands):
        final, energies = end(straight, *operands[:-1])
        return apart(final), energies.reshape(LAYERS)

    def one_late(*operands):
        final, energies = end(paired, *operands[:-1])
        return apart(final), energies.reshape(LAYERS)

    def more_late(*operands):
        final, energies, extra = end(straight, *operands)
        sent = jnp.broadcast_to(extra[None], (size, 1, LAYERS))
        total = energies + lax.all_to_all(sent, "amp", 0, 0, tiled=True).sum(axis=0)
        return apart(final), total.reshape(LAYERS)

    return lax.switch(
        mode[0, 0], (none_late, one_late, more_late),
        state, sums, turn, chosen, (*fields_made, *gates), late,
    )


def solution(mesh):
    in_specs = (P(None, ("rep", "amp")), P("rep", None), P("rep", None), P(), P())
    out_specs = (P(None, ("rep", "amp")), P("rep"))
    return jax.shard_map(local, mesh=mesh, in_specs=in_specs, out_specs=out_specs, check_vma=False)
```

```python
import numpy as np
import jax
import jax.numpy as jnp
from jax import lax
from jax.experimental import pallas as pl
from jax.experimental.pallas import tpu as pltpu
from jax.sharding import PartitionSpec as P

LAYERS = 2
ANGLES = 16
UNITS = 2 * (ANGLES + 1)
LANE_BITS = 7
LANES = 128

F32 = jnp.float32
BF16 = jnp.bfloat16


def angle_tables():
    steps = (np.arange(ANGLES, dtype=np.float64) + 1.0) * (np.pi / UNITS)
    return np.stack([np.cos(steps), np.sin(steps)]).astype(np.float32)


def iota(shape, dimension):
    return lax.broadcasted_iota(jnp.int32, shape, dimension)


def bit_count(values, width):
    total = values & 1
    for bit in range(1, width):
        total = total + ((values >> bit) & 1)
    return total


def split(values):
    high = values.astype(BF16)
    return high, (values - high.astype(F32)).astype(BF16)


def dot(left, right):
    return jnp.dot(left, right, preferred_element_type=F32)


def product(left, right):
    return dot(
        jnp.concatenate([left[0], left[0], left[1]], axis=1),
        jnp.concatenate([right[0], right[1], right[0]], axis=0),
    )


SWAPS = 4
ROWQ, LANEQ, SWAPPED, LATE, SPARE, PLAN = 0, 8, 12, 13, 14, 16


def gate(bits, width):
    column = iota((1, width), 1)
    lines = []
    for place, cosine, sine in bits:
        one = ((column >> place) & 1) == 1
        lines.append((jnp.where(one, sine, cosine), jnp.where(one, cosine, -sine)))
    row = iota((8, width), 0)
    matrix = None
    for bit, (zero_line, one_line) in enumerate(lines[:3]):
        factor = jnp.where(((row >> bit) & 1) == 1, one_line, zero_line)
        matrix = factor if matrix is None else matrix * factor
    for zero_line, one_line in lines[3:]:
        matrix = jnp.concatenate([matrix * zero_line, matrix * one_line], axis=0)
    return matrix


def lane_bits(pairs):
    return [(place, cosine, -sine) for place, (cosine, sine) in enumerate(pairs)]


def pair_of(layer, rotation_ref, table_ref, qubit, keep=None):
    index = rotation_ref[layer, qubit]
    cosine, sine = table_ref[0, index], table_ref[1, index]
    if keep is None:
        return cosine, sine
    return jnp.where(keep, cosine, F32(1.0)), jnp.where(keep, sine, F32(0.0))


def cos_sin(steps):
    quarter = UNITS // 2
    turns = jnp.floor(steps * (1.0 / quarter) + 0.5)
    angle = (steps - turns * quarter) * (np.pi / UNITS)
    square = angle * angle
    sine = angle * (
        1.0 + square * (-1.0 / 6 + square * (1.0 / 120 + square * (-1.0 / 5040 + square * (1.0 / 362880))))
    )
    cosine = 1.0 + square * (
        -0.5 + square * (1.0 / 24 + square * (-1.0 / 720 + square * (1.0 / 40320)))
    )
    turns = turns.astype(jnp.int32)
    odd = (turns & 1) == 1
    cosine, sine = jnp.where(odd, sine, cosine), jnp.where(odd, cosine, sine)
    return (
        jnp.where(((turns + 1) & 2) == 2, -cosine, cosine),
        jnp.where((turns & 2) == 2, -sine, sine),
    )


def looked_up(steps):
    period = 2 * UNITS
    place = (steps - period * jnp.floor(steps * (1.0 / period) + 0.25 / period)).astype(jnp.int32)
    cosine, sine = cos_sin(iota((8, LANES), 1).astype(F32))
    tiles = place.reshape(-1, 8, LANES)
    pick = lambda table: jnp.concatenate(
        [jnp.take_along_axis(table, tiles[k], axis=1, mode="promise_in_bounds") for k in range(tiles.shape[0])],
        axis=0,
    )
    return pick(cosine), pick(sine)


def turned(cosine, sine, real, imag):
    return cosine * real + sine * imag, cosine * imag - sine * real


def sign_rows(start, first, low, high, line):
    row = iota((8, start.shape[1]), 0)
    rows = jnp.broadcast_to(start, row.shape)
    for bit in range(low):
        rows = jnp.where(((row >> bit) & 1) == 1, rows * line(first + bit), rows)
    for bit in range(low, low + high):
        rows = jnp.concatenate([rows, rows * line(first + bit)], axis=0)
    return rows


def flips(positions, bonds):
    first, second = positions[:, 0:bonds], positions[:, 1 : bonds + 1]
    return lambda bit: jnp.where((first == bit) | (second == bit), F32(-1.0), F32(1.0))


def lane_part(positions, bonds):
    ones = jnp.ones((1, bonds), F32)
    return sign_rows(ones, 0, 3, LANE_BITS - 3, flips(positions, bonds)).astype(BF16)


def fields(weights, positions, lanes, device_bits, bonds, row_bits):
    differ = (device_bits >> positions[:, 0:bonds]) ^ (device_bits >> positions[:, 1 : bonds + 1])
    device_sign = (1 - 2 * (differ & 1)).astype(F32)
    line = flips(positions, bonds)
    stacked = jnp.concatenate(
        [sign_rows(w * device_sign, LANE_BITS, 3, row_bits - 3, line).astype(BF16) for w in weights],
        axis=0,
    )
    out = lax.dot_general(
        stacked, lanes, (((1,), (1,)), ((), ())), preferred_element_type=F32
    )
    rows = 2**row_bits
    return [out[k * rows : (k + 1) * rows] for k in range(len(weights))]


def energy(real, imag, field):
    return jnp.sum((real * real + imag * imag) * field)


def in_lanes(parts):
    lane = iota((1, LANES), 1)
    row = jnp.zeros((1, LANES), F32)
    for k, part in enumerate(parts):
        row = jnp.where(lane == k, part, row)
    return row


def evens(ref):
    half = ref.shape[0] // 2
    return ref[pl.ds(0, half, stride=2), :], ref[pl.ds(1, half, stride=2), :]


def take_blocks(ref, blocks, height, kept):
    def part(component):
        return jnp.concatenate(
            [ref[pl.ds(2 * k + component, blocks, stride=height), :] for k in range(kept)], axis=0
        )

    return part(0), part(1)


def put_blocks(ref, blocks, height, kept, real, imag):
    for k in range(kept):
        here = slice(k * blocks, (k + 1) * blocks)
        ref[pl.ds(2 * k, blocks, stride=height), :] = real[here]
        ref[pl.ds(2 * k + 1, blocks, stride=height), :] = imag[here]


def by_rows(gates, real, imag):
    both = product(gates, split(jnp.concatenate([real, imag], axis=1)))
    return both[:, :LANES], both[:, LANES:]


def by_blocks(gates, real, imag):
    size = gates[0].shape[0]
    pieces = [p[k : k + size] for p in (real, imag) for k in range(0, real.shape[0], size)]
    out = product(gates, split(jnp.concatenate(pieces, axis=1)))
    pieces = [out[:, k * LANES : (k + 1) * LANES] for k in range(len(pieces))]
    half = len(pieces) // 2
    return jnp.concatenate(pieces[:half], axis=0), jnp.concatenate(pieces[half:], axis=0)


def by_lanes(gates, real, imag):
    rows = real.shape[0]
    both = product(split(jnp.concatenate([real, imag], axis=0)), gates)
    return both[:rows], both[rows:]


def across(values, step):
    place = iota((8, LANES), 1) ^ step
    return jnp.concatenate(
        [
            jnp.take_along_axis(values[k : k + 8], place, axis=1, mode="promise_in_bounds")
            for k in range(0, values.shape[0], 8)
        ],
        axis=0,
    )


def swap(buffer, plan_ref, slots):
    for i in range(SWAPS):
        @pl.when(i < plan_ref[0, SWAPPED])
        def _(i=i):
            height = 2 ** (slots - 1 - i)
            place = plan_ref[0, LANEQ + i]
            step = jnp.left_shift(jnp.int32(1), place)
            if height == 4:
                tiles = buffer[...].reshape(-1, 8, LANES)
                other = pltpu.roll(tiles, 4, 1)
                one = (iota((1, 8, LANES), 2) >> place) & 1
                same = one == (iota((1, 8, LANES), 1) >> 2)
                moved = across(other.reshape(-1, LANES), step).reshape(tiles.shape)
                buffer[...] = jnp.where(same, tiles, moved).reshape(buffer.shape)
                return
            whole = buffer[...].reshape(-1, 2, height, LANES)
            low, high = whole[:, 0].reshape(-1, LANES), whole[:, 1].reshape(-1, LANES)
            one = ((iota((1, LANES), 1) >> place) & 1) == 1
            crossed = across(jnp.where(one, low, high), step)
            new_low, new_high = jnp.where(one, crossed, low), jnp.where(one, high, crossed)
            pairs = (new_low.reshape(-1, 1, height, LANES), new_high.reshape(-1, 1, height, LANES))
            buffer[...] = jnp.concatenate(pairs, axis=1).reshape(buffer.shape)


class Plan:
    def __init__(self, local_bits, global_bits):
        self.local_bits, self.global_bits = local_bits, global_bits
        self.qubits = local_bits + global_bits
        self.row_bits = local_bits - LANE_BITS
        self.rows = 2**self.row_bits
        self.blocks = 2**global_bits
        self.kept_bits = self.row_bits - global_bits
        self.kept = 2**self.kept_bits
        self.bonds = self.qubits - 1


def choose(plan, chain_ref, plan_ref):
    order = [chain_ref[0, k] for k in range(plan.qubits)]
    away = [(q >= plan.local_bits).astype(jnp.int32) for q in order]
    free = jnp.int32(0)
    for k, q in enumerate(order):
        near = away[k]
        if k:
            near = near | away[k - 1]
        if k + 1 < plan.qubits:
            near = near | away[k + 1]
        free = free | jnp.left_shift(1 - near, q)
    bit = lambda q: (free >> q) & 1
    row_qubits = range(LANE_BITS, plan.local_bits)
    free_rows = sum(bit(q) for q in row_qubits)
    slots = plan.global_bits
    free_lanes = sum(bit(q) for q in range(LANE_BITS))
    swapped = jnp.minimum(jnp.minimum(free_lanes, SWAPS), jnp.maximum(slots - free_rows, 0))
    late = jnp.maximum(slots - swapped - free_rows, 0)
    seen = jnp.int32(0)
    for k, q in enumerate(row_qubits):
        held = k - seen
        rank = jnp.where(bit(q) == 1, late + seen, jnp.where(held < late, held, free_rows + held))
        plan_ref[0, ROWQ + rank] = jnp.int32(q)
        seen = seen + bit(q)
    for i in range(SWAPS):
        plan_ref[0, LANEQ + i] = jnp.int32(-1)
    seen = jnp.int32(0)
    for q in range(LANE_BITS):
        taken = (bit(q) == 1) & (seen < swapped)
        plan_ref[0, jnp.where(taken, LANEQ + seen, SPARE)] = jnp.int32(q)
        seen = seen + bit(q)
    plan_ref[0, SWAPPED] = swapped
    plan_ref[0, LATE] = late


def touches(plan, chain, plan_ref, rows_from, rows_to, lanes):
    hit = jnp.zeros(chain.shape, jnp.int32)
    for b in range(plan.global_bits):
        wanted = (b >= rows_from) & (b < rows_to)
        hit = hit | (chain == jnp.where(wanted, plan_ref[0, ROWQ + b], -1)).astype(jnp.int32)
    if lanes:
        for i in range(SWAPS):
            hit = hit | (chain == plan_ref[0, LANEQ + i]).astype(jnp.int32)
    return (hit[:, 0 : plan.bonds] | hit[:, 1 : plan.bonds + 1]).astype(F32)


def ordered_positions(plan, chain, plan_ref):
    places = chain
    for b in range(plan.row_bits):
        places = jnp.where(chain == plan_ref[0, ROWQ + b], LANE_BITS + b, places)
    return places


def moved_positions(plan, chain, plan_ref):
    slots, swapped = plan.global_bits, plan_ref[0, SWAPPED]
    places = jnp.where(chain >= plan.local_bits, chain - plan.local_bits + LANE_BITS, chain)
    for b in range(plan.row_bits):
        target = jnp.int32(LANE_BITS + b)
        if b < slots:
            target = jnp.int32(plan.local_bits + b)
            i = slots - 1 - b
            if i < SWAPS:
                target = jnp.where(i < swapped, plan_ref[0, LANEQ + i], target)
        places = jnp.where(chain == plan_ref[0, ROWQ + b], target, places)
    for i in range(SWAPS):
        places = jnp.where(chain == plan_ref[0, LANEQ + i], plan.local_bits + slots - 1 - i, places)
    return places


def row_ones(plan, device):
    tile = bit_count(iota((8, LANES), 0), 3) + bit_count(iota((8, LANES), 1), LANE_BITS)
    tile = tile + bit_count(device, plan.global_bits)
    return jnp.concatenate([tile + k.bit_count() for k in range(plan.rows // 8)], axis=0)


def first_kernel(plan, *refs):
    sources, (out_ref, sums_ref, plan_ref, buffer), held = refs[:6], refs[6:10], refs[10:16]
    table_ref, semaphores = refs[16:]
    copies = [pltpu.make_async_copy(s, h, semaphores.at[k]) for k, (s, h) in enumerate(zip(sources, held))]
    for copy in copies:
        copy.start()
    for k, values in enumerate(angle_tables()):
        for at, value in enumerate(values):
            table_ref[k, at] = F32(value)
    for copy in copies[:-1]:
        copy.wait()
    rotation_ref, order_ref, chain_ref, coupling_ref, bond_ref, amps_ref = held
    device = lax.axis_index("amp")
    bonds, rows = plan.bonds, plan.rows
    choose(plan, order_ref, plan_ref)
    chain = chain_ref[...]
    device_bits = device << plan.local_bits
    bond_signs = (2 * bond_ref[...] - 1).astype(F32)
    lanes = lane_part(chain, bonds)
    (steps,) = fields(
        [(coupling_ref[0:1, :] + 1).astype(F32) * bond_signs],
        chain, lanes, device_bits, bonds, plan.row_bits,
    )
    steps = steps + (UNITS // 2) * row_ones(plan, device).astype(F32)
    pair = lambda layer, q, keep=None: pair_of(layer, rotation_ref, table_ref, q, keep)

    copies[-1].wait()
    real, imag = evens(amps_ref)
    norm = jnp.sum(real * real + imag * imag)
    real, imag = turned(*looked_up(steps), real, imag)
    ranked = [plan_ref[0, ROWQ + b] for b in range(plan.row_bits)]
    row_gate = gate([(q - LANE_BITS, *pair(0, q)) for q in ranked], rows)
    lane_gate = gate(lane_bits([pair(0, q) for q in range(LANE_BITS)]), LANES)
    real, imag = by_rows(split(row_gate), real, imag)
    real, imag = by_lanes(split(lane_gate), real, imag)

    late, slots = plan_ref[0, LATE], plan.global_bits - plan_ref[0, SWAPPED]
    early = touches(plan, chain, plan_ref, late, slots, True)
    weight = early * bond_signs
    steps, signs = fields(
        [(coupling_ref[1:2, :] + 1).astype(F32) * weight, weight],
        ordered_positions(plan, chain, plan_ref), lanes, device_bits, bonds, plan.row_bits,
    )
    sums_ref[...] = in_lanes([norm, energy(real, imag, signs)])
    real, imag = turned(*looked_up(steps), real, imag)
    bits = []
    for b in range(plan.global_bits):
        leaving, i = ranked[b], plan.global_bits - 1 - b
        if i < SWAPS:
            leaving = jnp.where(b >= slots, plan_ref[0, LANEQ + i], leaving)
        bits.append((b, *pair(1, leaving, b >= late)))
    leave_gate = split(gate(bits, plan.blocks))
    buffer[...] = jnp.concatenate([real, imag], axis=0)
    swap(buffer, plan_ref, plan.global_bits)
    real, imag = by_blocks(leave_gate, buffer[:rows], buffer[rows:])
    put_blocks(out_ref, plan.blocks, 2 * plan.kept, plan.kept, real, imag)


def prepare_kernel(
    plan, rotation_ref, table_ref, plan_ref, chain_ref, coupling_ref, bond_ref,
    mode_ref, cosine_ref, sine_ref, before_ref, after_ref, late_ref, turn_ref, *gate_refs,
):
    late_rows = plan_ref[0, LATE]
    mode_ref[0, 0] = jnp.minimum(late_rows, 2)
    device = lax.axis_index("amp")
    bonds, rows, slots = plan.bonds, plan.rows, plan.global_bits
    chain = chain_ref[...]
    bond_signs = (2 * bond_ref[...] - 1).astype(F32)
    rest = bond_signs * (1.0 - touches(plan, chain, plan_ref, late_rows, slots - plan_ref[0, SWAPPED], True))
    after_trade = jnp.where(late_rows >= 2, late_rows, 0)
    late = bond_signs * touches(plan, chain, plan_ref, 0, after_trade, False)
    moved = moved_positions(plan, chain, plan_ref)
    device_bits = device << plan.local_bits
    steps, before_ref[...], after_ref[...] = fields(
        [(coupling_ref[1:2, :] + 1).astype(F32) * rest, rest, bond_signs - late],
        moved, lane_part(moved, bonds), device_bits, bonds, plan.row_bits,
    )
    cosine_ref[...], sine_ref[...] = looked_up(steps)
    (late_ref[...],) = fields([late], chain, lane_part(chain, bonds), device_bits, bonds, plan.row_bits)
    pair = lambda layer, q, keep=None: pair_of(layer, rotation_ref, table_ref, q, keep)
    ranked = [plan_ref[0, ROWQ + b] for b in range(plan.row_bits)]
    cosine, sine = pair(1, ranked[0])
    turn_ref[...] = in_lanes([cosine, jnp.where((device & 1) == 1, -sine, sine)])
    far = [plan.local_bits + b for b in range(slots)]
    lane_pairs = []
    for q in range(LANE_BITS):
        held = jnp.int32(q)
        for i in range(SWAPS):
            held = jnp.where(plan_ref[0, LANEQ + i] == q, ranked[slots - 1 - i], held)
        lane_pairs.append(pair(1, held))
    back = []
    for b in range(plan.row_bits):
        cosine, sine = pair(1, ranked[b], b < after_trade)
        back.append((ranked[b] - LANE_BITS, cosine, -sine))
    gates = [
        gate([(b, *pair(0, q)) for b, q in enumerate(far)], plan.blocks),
        gate([(b, *pair(1, q)) for b, q in enumerate(far + ranked[slots:])], rows),
        gate(lane_bits(lane_pairs), LANES),
        gate(back, rows).T,
    ]
    for k, made in enumerate(gates):
        gate_refs[2 * k][...], gate_refs[2 * k + 1][...] = split(made)


def middle(plan, state_ref, cosine_ref, sine_ref, before_ref, gates):
    ga, gb, ha, hb, la, lb = gates
    real, imag = take_blocks(state_ref, plan.blocks, 2 * plan.kept, plan.kept)
    real, imag = by_blocks((ga[...], gb[...]), real, imag)
    before = energy(real, imag, before_ref[...])
    real, imag = turned(cosine_ref[...], sine_ref[...], real, imag)
    real, imag = by_rows((ha[...], hb[...]), real, imag)
    return *by_lanes((la[...], lb[...]), real, imag), before


def pack(plan, out_ref, real, imag, sums):
    blocks, kept = plan.blocks, plan.kept
    height = 2 * kept + 1
    put_blocks(out_ref, blocks, height, kept, real, imag)
    out_ref[pl.ds(2 * kept, blocks, stride=height), :] = jnp.broadcast_to(sums, (blocks, LANES))


def middle_kernel(plan, state_ref, cosine_ref, sine_ref, before_ref, after_ref, sums_ref, *refs):
    real, imag, before = middle(plan, state_ref, cosine_ref, sine_ref, before_ref, refs[:6])
    after = energy(real, imag, after_ref[...])
    pack(plan, refs[6], real, imag, sums_ref[...] + in_lanes([F32(0.0), before, after]))


def open_kernel(plan, state_ref, cosine_ref, sine_ref, before_ref, sums_ref, *refs):
    gates, (out_ref, sums_out_ref) = refs[:6], refs[6:]
    real, imag, before = middle(plan, state_ref, cosine_ref, sine_ref, before_ref, gates)
    out_ref[...] = jnp.concatenate([real, imag], axis=0)
    sums_out_ref[...] = sums_ref[...] + in_lanes([F32(0.0), before])


def close_kernel(plan, own_ref, other_ref, turn_ref, after_ref, sums_ref, out_ref):
    both = turn_ref[0:1, 0:1] * own_ref[...] + turn_ref[0:1, 1:2] * other_ref[...]
    real, imag = both[: plan.rows], both[plan.rows :]
    after = energy(real, imag, after_ref[...])
    pack(plan, out_ref, real, imag, sums_ref[...] + in_lanes([F32(0.0), F32(0.0), after]))


def last_kernel(plan, plan_ref, state_ref, ga, gb, *refs):
    late_ref, (out_ref, energies_ref, *late_out_ref, buffer) = refs[:-3][:1], refs[-4 if len(refs) == 5 else -3 :]
    device = lax.axis_index("amp")
    blocks, kept, rows = plan.blocks, plan.kept, plan.rows
    height = 2 * kept + 1
    sums = jnp.sum(state_ref[pl.ds(2 * kept, blocks, stride=height), :], axis=0, keepdims=True)
    amps = float(2**plan.qubits)
    mean = sums[:, 0:1] / amps + 1e-06
    factor = 1.0 / jnp.sqrt(mean)
    square = factor * factor / amps
    energies_ref[...] = sums[:, 1 : 1 + LAYERS] * square
    real, imag = take_blocks(state_ref, blocks, height, kept)
    buffer[...] = jnp.concatenate([real, imag], axis=0)
    swap(buffer, plan_ref, plan.global_bits)
    real, imag = by_rows((ga[...], gb[...]), buffer[:rows], buffer[rows:])
    if late_ref:
        late_out_ref[0][...] = in_lanes([0.0, energy(real, imag, late_ref[0][...])])[:, 0:LAYERS] * square
    ones = row_ones(plan, device)
    odd = (ones & 1) == 1
    real, imag = jnp.where(odd, imag, real), jnp.where(odd, real, imag)
    real = jnp.where(((ones + 1) & 2) == 2, -factor, factor) * real
    imag = jnp.where((ones & 2) == 2, -factor, factor) * imag
    out_ref[pl.ds(0, rows, stride=2), :] = real
    out_ref[pl.ds(1, rows, stride=2), :] = imag


def spec(space):
    return pl.BlockSpec(memory_space=space)


def call(kernel, shapes, scalars, arrays, name, spaces=None, scratch=(), near=0, held=(), far=(), plan=None):
    kept = len(arrays) - near
    arrays = tuple(
        pltpu.with_memory_space_constraint(a, pltpu.VMEM) if k >= kept else a
        for k, a in enumerate(arrays)
    )
    if plan is not None:
        scalars = (*scalars, pltpu.with_memory_space_constraint(plan, pltpu.SMEM))
    spaces = spaces or (pltpu.VMEM,) * len(shapes)
    shapes = tuple(
        spaces[k](s.shape, s.dtype) if k in held else pltpu.HBM(s.shape, s.dtype) if k in far else s
        for k, s in enumerate(shapes)
    )
    return pl.pallas_call(
        kernel,
        out_shape=shapes,
        in_specs=[spec(pltpu.SMEM)] * len(scalars) + [spec(pltpu.VMEM)] * len(arrays),
        out_specs=tuple(spec(s) for s in spaces),
        scratch_shapes=scratch,
        name=name,
    )(*scalars, *arrays)


def first_call(plan, rotation, chain, coupling, bond, state):
    sources = (rotation, chain, chain, coupling, bond, state)
    spaces = (pltpu.SMEM,) * 2 + (pltpu.VMEM,) * 4
    outs = (pltpu.VMEM, pltpu.VMEM, pltpu.SMEM)
    return pl.pallas_call(
        lambda *refs: first_kernel(plan, *refs),
        out_shape=(
            pltpu.VMEM(state.shape, F32), pltpu.VMEM((1, LANES), F32), pltpu.SMEM((1, PLAN), jnp.int32),
        ),
        in_specs=[spec(pl.ANY)] * len(sources),
        out_specs=tuple(spec(s) for s in outs),
        scratch_shapes=[pltpu.VMEM(state.shape, F32)]
        + [space(a.shape, a.dtype) for space, a in zip(spaces, sources)]
        + [pltpu.SMEM((2, ANGLES), F32), pltpu.SemaphoreType.DMA((len(sources),))],
        name="first",
    )(*sources)


def local(amplitudes, coupling_index, rotation_index, chain_order, bond_sign):
    local_bits = amplitudes.shape[1].bit_length() - 1
    size = lax.axis_size("amp")
    plan = Plan(local_bits, size.bit_length() - 1)
    rows = plan.rows
    shape = jax.ShapeDtypeStruct
    bind = lambda kernel: lambda *refs: kernel(plan, *refs)

    state = amplitudes.reshape(2, rows, LANES).transpose(1, 0, 2).reshape(2 * rows, LANES)
    table = jnp.asarray(angle_tables())
    chain, bond = chain_order.reshape(1, -1), bond_sign.reshape(1, -1)
    small = (chain, coupling_index, bond)
    whole = shape((2 * rows, LANES), F32)
    field, line = shape((rows, LANES), F32), shape((1, LANES), F32)
    square_of = lambda n: shape((n, n), BF16)
    buffer = (pltpu.VMEM((2 * rows, LANES), F32),)

    state, sums, chosen = first_call(plan, rotation_index, chain, coupling_index, bond, state)
    sizes = (size, rows, LANES, rows)
    made = call(
        bind(prepare_kernel),
        (shape((1, 1), jnp.int32),) + (field,) * 5 + (line,)
        + tuple(square_of(n) for n in sizes for _ in range(2)),
        (rotation_index, table), small, "prepare",
        (pltpu.SMEM,) + (pltpu.VMEM,) * 14, held=range(1, 15), plan=chosen,
    )
    mode, fields_made, late, turn, gates = made[0], made[1:5], made[5], made[6], made[7:]
    state = lax.all_to_all(state.reshape(size, 2 * plan.kept, LANES), "amp", 0, 0, tiled=True)
    state = state.reshape(2 * rows, LANES)
    height = 2 * plan.kept + 1
    pair = shape((1, LAYERS), F32)

    packed = (shape((size * height, LANES), F32),)

    def straight(state, sums, turn, made):
        return call(
            bind(middle_kernel), packed, (), (state, *made[:4], sums, *made[4:10]),
            "middle", near=12, held=(0,),
        )

    def paired(state, sums, turn, made):
        own, sums = call(
            bind(open_kernel), (whole, line), (),
            (state, *made[:3], sums, *made[4:10]), "open", near=11, held=(0, 1),
        )
        other = lax.ppermute(own, "amp", [(k, k ^ 1) for k in range(size)])
        return call(
            bind(close_kernel), packed, (),
            (own, other, turn, made[3], sums), "close", near=5, held=(0,),
        )

    def end(middle_of, state, sums, turn, chosen, made, *late):
        (state,) = middle_of(state, sums, turn, made)
        state = lax.all_to_all(state.reshape(size, height, 1, LANES), "amp", 0, 0, tiled=True)
        return call(
            bind(last_kernel), (whole, pair) + (pair,) * len(late), (),
            (state.reshape(size * height, LANES), *made[10:], *late), "last",
            scratch=buffer, near=3 + len(late), far=() if late else (0, 1), plan=chosen,
        )

    def apart(final):
        return final.reshape(rows, 2, LANES).transpose(1, 0, 2).reshape(2, rows * LANES)

    def none_late(*operands):
        final, energies = end(straight, *operands[:-1])
        return apart(final), energies.reshape(LAYERS)

    def one_late(*operands):
        final, energies = end(paired, *operands[:-1])
        return apart(final), energies.reshape(LAYERS)

    def more_late(*operands):
        final, energies, extra = end(straight, *operands)
        sent = jnp.broadcast_to(extra[None], (size, 1, LAYERS))
        total = energies + lax.all_to_all(sent, "amp", 0, 0, tiled=True).sum(axis=0)
        return apart(final), total.reshape(LAYERS)

    return lax.switch(
        mode[0, 0], (none_late, one_late, more_late),
        state, sums, turn, chosen, (*fields_made, *gates), late,
    )


def solution(mesh):
    in_specs = (P(None, ("rep", "amp")), P("rep", None), P("rep", None), P(), P())
    out_specs = (P(None, ("rep", "amp")), P("rep"))
    return jax.shard_map(local, mesh=mesh, in_specs=in_specs, out_specs=out_specs, check_vma=False)
```

```python
import numpy as np
import jax
import jax.numpy as jnp
from jax import lax
from jax.experimental import pallas as pl
from jax.experimental.pallas import tpu as pltpu
from jax.sharding import PartitionSpec as P

LAYERS = 2
ANGLES = 16
UNITS = 2 * (ANGLES + 1)
LANE_BITS = 7
LANES = 128

F32 = jnp.float32
BF16 = jnp.bfloat16


def angle_tables():
    steps = (np.arange(ANGLES, dtype=np.float64) + 1.0) * (np.pi / UNITS)
    return np.stack([np.cos(steps), np.sin(steps)]).astype(np.float32)


def iota(shape, dimension):
    return lax.broadcasted_iota(jnp.int32, shape, dimension)


def bit_count(values, width):
    total = values & 1
    for bit in range(1, width):
        total = total + ((values >> bit) & 1)
    return total


def split(values):
    high = values.astype(BF16)
    return high, (values - high.astype(F32)).astype(BF16)


def dot(left, right):
    return jnp.dot(left, right, preferred_element_type=F32)


def product(left, right):
    return dot(
        jnp.concatenate([left[0], left[0], left[1]], axis=1),
        jnp.concatenate([right[0], right[1], right[0]], axis=0),
    )


SWAPS = 4
ROWQ, LANEQ, SWAPPED, LATE, SPARE, PLAN = 0, 8, 12, 13, 14, 16


def gate(bits, width):
    column = iota((1, width), 1)
    lines = []
    for place, cosine, sine in bits:
        one = ((column >> place) & 1) == 1
        lines.append((jnp.where(one, sine, cosine), jnp.where(one, cosine, -sine)))
    row = iota((8, width), 0)
    matrix = None
    for bit, (zero_line, one_line) in enumerate(lines[:3]):
        factor = jnp.where(((row >> bit) & 1) == 1, one_line, zero_line)
        matrix = factor if matrix is None else matrix * factor
    for zero_line, one_line in lines[3:]:
        matrix = jnp.concatenate([matrix * zero_line, matrix * one_line], axis=0)
    return matrix


def lane_bits(pairs):
    return [(place, cosine, -sine) for place, (cosine, sine) in enumerate(pairs)]


def pair_of(layer, rotation_ref, table_ref, qubit, keep=None):
    index = rotation_ref[layer, qubit]
    cosine, sine = table_ref[0, index], table_ref[1, index]
    if keep is None:
        return cosine, sine
    return jnp.where(keep, cosine, F32(1.0)), jnp.where(keep, sine, F32(0.0))


def cos_sin(steps):
    quarter = UNITS // 2
    turns = jnp.floor(steps * (1.0 / quarter) + 0.5)
    angle = (steps - turns * quarter) * (np.pi / UNITS)
    square = angle * angle
    sine = angle * (
        1.0 + square * (-1.0 / 6 + square * (1.0 / 120 + square * (-1.0 / 5040 + square * (1.0 / 362880))))
    )
    cosine = 1.0 + square * (
        -0.5 + square * (1.0 / 24 + square * (-1.0 / 720 + square * (1.0 / 40320)))
    )
    turns = turns.astype(jnp.int32)
    odd = (turns & 1) == 1
    cosine, sine = jnp.where(odd, sine, cosine), jnp.where(odd, cosine, sine)
    return (
        jnp.where(((turns + 1) & 2) == 2, -cosine, cosine),
        jnp.where((turns & 2) == 2, -sine, sine),
    )


def looked_up(steps):
    period = 2 * UNITS
    place = (steps - period * jnp.floor(steps * (1.0 / period) + 0.25 / period)).astype(jnp.int32)
    cosine, sine = cos_sin(iota((8, LANES), 1).astype(F32))
    tiles = place.reshape(-1, 8, LANES)
    pick = lambda table: jnp.concatenate(
        [jnp.take_along_axis(table, tiles[k], axis=1, mode="promise_in_bounds") for k in range(tiles.shape[0])],
        axis=0,
    )
    return pick(cosine), pick(sine)


def turned(cosine, sine, real, imag):
    return cosine * real + sine * imag, cosine * imag - sine * real


def sign_rows(start, first, low, high, line):
    row = iota((8, start.shape[1]), 0)
    rows = jnp.broadcast_to(start, row.shape)
    for bit in range(low):
        rows = jnp.where(((row >> bit) & 1) == 1, rows * line(first + bit), rows)
    for bit in range(low, low + high):
        rows = jnp.concatenate([rows, rows * line(first + bit)], axis=0)
    return rows


def flips(positions, bonds):
    first, second = positions[:, 0:bonds], positions[:, 1 : bonds + 1]
    return lambda bit: jnp.where((first == bit) | (second == bit), F32(-1.0), F32(1.0))


def lane_part(positions, bonds):
    ones = jnp.ones((1, bonds), F32)
    return sign_rows(ones, 0, 3, LANE_BITS - 3, flips(positions, bonds)).astype(BF16)


def fields(weights, positions, lanes, device_bits, bonds, row_bits):
    differ = (device_bits >> positions[:, 0:bonds]) ^ (device_bits >> positions[:, 1 : bonds + 1])
    device_sign = (1 - 2 * (differ & 1)).astype(F32)
    line = flips(positions, bonds)
    stacked = jnp.concatenate(
        [sign_rows(w * device_sign, LANE_BITS, 3, row_bits - 3, line).astype(BF16) for w in weights],
        axis=0,
    )
    out = lax.dot_general(
        stacked, lanes, (((1,), (1,)), ((), ())), preferred_element_type=F32
    )
    rows = 2**row_bits
    return [out[k * rows : (k + 1) * rows] for k in range(len(weights))]


def energy(real, imag, field):
    values = jnp.sum(((real * real + imag * imag) * field).reshape(-1, 8, LANES), axis=0)
    return jnp.sum(jnp.sum(values, axis=0, keepdims=True), axis=1, keepdims=True)


def in_lanes(parts):
    lane = iota((1, LANES), 1)
    row = jnp.zeros((1, LANES), F32)
    for k, part in enumerate(parts):
        row = jnp.where(lane == k, part, row)
    return row


def evens(ref):
    half = ref.shape[0] // 2
    return ref[pl.ds(0, half, stride=2), :], ref[pl.ds(1, half, stride=2), :]


def take_blocks(ref, blocks, height, kept):
    def part(component):
        return jnp.concatenate(
            [ref[pl.ds(2 * k + component, blocks, stride=height), :] for k in range(kept)], axis=0
        )

    return part(0), part(1)


def put_blocks(ref, blocks, height, kept, real, imag):
    for k in range(kept):
        here = slice(k * blocks, (k + 1) * blocks)
        ref[pl.ds(2 * k, blocks, stride=height), :] = real[here]
        ref[pl.ds(2 * k + 1, blocks, stride=height), :] = imag[here]


def by_rows(gates, real, imag):
    both = product(gates, split(jnp.concatenate([real, imag], axis=1)))
    return both[:, :LANES], both[:, LANES:]


def by_blocks(gates, real, imag):
    size = gates[0].shape[0]
    pieces = [p[k : k + size] for p in (real, imag) for k in range(0, real.shape[0], size)]
    out = product(gates, split(jnp.concatenate(pieces, axis=1)))
    pieces = [out[:, k * LANES : (k + 1) * LANES] for k in range(len(pieces))]
    half = len(pieces) // 2
    return jnp.concatenate(pieces[:half], axis=0), jnp.concatenate(pieces[half:], axis=0)


def by_lanes(gates, real, imag):
    rows = real.shape[0]
    both = product(split(jnp.concatenate([real, imag], axis=0)), gates)
    return both[:rows], both[rows:]


def swap(plan, load, buffer, plan_ref):
    tiles = plan.blocks // 8
    top = tiles.bit_length() - 2
    lane, row = iota((8, LANES), 1), iota((8, LANES), 0)
    steps = []
    for i in range(SWAPS):
        taken = i < plan_ref[0, SWAPPED]
        steps.append(jnp.where(taken, jnp.left_shift(jnp.int32(1), plan_ref[0, LANEQ + i] & 7), 0))
    ones = [(lane & step) != 0 for step in steps]
    places = [lane ^ step for step in steps]
    cross = lambda value, i: jnp.take_along_axis(value, places[i], axis=1, mode="promise_in_bounds")
    for part in range(2 * plan.kept):
        values = [load(part, at) for at in range(tiles)]
        for i in range(top + 1):
            bit = 1 << (top - i)
            for low in range(tiles):
                if low & bit:
                    continue
                first, second = values[low], values[low | bit]
                crossed = cross(jnp.where(ones[i], first, second), i)
                values[low] = jnp.where(ones[i], crossed, first)
                values[low | bit] = jnp.where(ones[i], second, crossed)
        for at in range(tiles):
            buffer[pl.ds(part * plan.blocks + at * 8, 8), :] = values[at]

    @pl.when(plan_ref[0, SWAPPED] > top + 1)
    def _():
        same = ones[top + 1] == ((row & 4) != 0)
        for at in range(0, buffer.shape[0], 8):
            value = buffer[pl.ds(at, 8), :]
            buffer[pl.ds(at, 8), :] = jnp.where(same, value, cross(pltpu.roll(value, 4, 0), top + 1))


class Plan:
    def __init__(self, local_bits, global_bits):
        self.local_bits, self.global_bits = local_bits, global_bits
        self.qubits = local_bits + global_bits
        self.row_bits = local_bits - LANE_BITS
        self.rows = 2**self.row_bits
        self.blocks = 2**global_bits
        self.kept_bits = self.row_bits - global_bits
        self.kept = 2**self.kept_bits
        self.bonds = self.qubits - 1


def choose(plan, chain_ref, plan_ref):
    order = [chain_ref[0, k] for k in range(plan.qubits)]
    away = [(q >= plan.local_bits).astype(jnp.int32) for q in order]
    free = jnp.int32(0)
    for k, q in enumerate(order):
        near = away[k]
        if k:
            near = near | away[k - 1]
        if k + 1 < plan.qubits:
            near = near | away[k + 1]
        free = free | jnp.left_shift(1 - near, q)
    bit = lambda q: (free >> q) & 1
    row_qubits = range(LANE_BITS, plan.local_bits)
    free_rows = sum(bit(q) for q in row_qubits)
    slots = plan.global_bits
    free_lanes = sum(bit(q) for q in range(LANE_BITS))
    swapped = jnp.minimum(jnp.minimum(free_lanes, SWAPS), jnp.maximum(slots - free_rows, 0))
    late = jnp.maximum(slots - swapped - free_rows, 0)
    seen = jnp.int32(0)
    for k, q in enumerate(row_qubits):
        held = k - seen
        rank = jnp.where(bit(q) == 1, late + seen, jnp.where(held < late, held, free_rows + held))
        plan_ref[0, ROWQ + rank] = jnp.int32(q)
        seen = seen + bit(q)
    for i in range(SWAPS):
        plan_ref[0, LANEQ + i] = jnp.int32(-1)
    seen = jnp.int32(0)
    for q in range(LANE_BITS):
        taken = (bit(q) == 1) & (seen < swapped)
        plan_ref[0, jnp.where(taken, LANEQ + seen, SPARE)] = jnp.int32(q)
        seen = seen + bit(q)
    plan_ref[0, SWAPPED] = swapped
    plan_ref[0, LATE] = late


def touches(plan, chain, plan_ref, rows_from, rows_to, lanes):
    hit = jnp.zeros(chain.shape, jnp.int32)
    for b in range(plan.global_bits):
        wanted = (b >= rows_from) & (b < rows_to)
        hit = hit | (chain == jnp.where(wanted, plan_ref[0, ROWQ + b], -1)).astype(jnp.int32)
    if lanes:
        for i in range(SWAPS):
            hit = hit | (chain == plan_ref[0, LANEQ + i]).astype(jnp.int32)
    return (hit[:, 0 : plan.bonds] | hit[:, 1 : plan.bonds + 1]).astype(F32)


def ordered_positions(plan, chain, plan_ref):
    places = chain
    for b in range(plan.row_bits):
        places = jnp.where(chain == plan_ref[0, ROWQ + b], LANE_BITS + b, places)
    return places


def moved_positions(plan, chain, plan_ref):
    slots, swapped = plan.global_bits, plan_ref[0, SWAPPED]
    places = jnp.where(chain >= plan.local_bits, chain - plan.local_bits + LANE_BITS, chain)
    for b in range(plan.row_bits):
        target = jnp.int32(LANE_BITS + b)
        if b < slots:
            target = jnp.int32(plan.local_bits + b)
            i = slots - 1 - b
            if i < SWAPS:
                target = jnp.where(i < swapped, plan_ref[0, LANEQ + i], target)
        places = jnp.where(chain == plan_ref[0, ROWQ + b], target, places)
    for i in range(SWAPS):
        places = jnp.where(chain == plan_ref[0, LANEQ + i], plan.local_bits + slots - 1 - i, places)
    return places


def row_ones(plan, device):
    tile = bit_count(iota((8, LANES), 0), 3) + bit_count(iota((8, LANES), 1), LANE_BITS)
    tile = tile + bit_count(device, plan.global_bits)
    return jnp.concatenate([tile + k.bit_count() for k in range(plan.rows // 8)], axis=0)


def first_kernel(plan, *refs):
    sources, (out_ref, sums_ref, plan_ref, buffer), held = refs[:6], refs[6:10], refs[10:16]
    table_ref, semaphores = refs[16:]
    copies = [pltpu.make_async_copy(s, h, semaphores.at[k]) for k, (s, h) in enumerate(zip(sources, held))]
    for copy in copies:
        copy.start()
    for k, values in enumerate(angle_tables()):
        for at, value in enumerate(values):
            table_ref[k, at] = F32(value)
    for copy in copies[:-1]:
        copy.wait()
    rotation_ref, order_ref, chain_ref, coupling_ref, bond_ref, amps_ref = held
    device = lax.axis_index("amp")
    bonds, rows = plan.bonds, plan.rows
    choose(plan, order_ref, plan_ref)
    chain = chain_ref[...]
    device_bits = device << plan.local_bits
    bond_signs = (2 * bond_ref[...] - 1).astype(F32)
    lanes = lane_part(chain, bonds)
    (steps,) = fields(
        [(coupling_ref[0:1, :] + 1).astype(F32) * bond_signs],
        chain, lanes, device_bits, bonds, plan.row_bits,
    )
    steps = steps + (UNITS // 2) * row_ones(plan, device).astype(F32)
    pair = lambda layer, q, keep=None: pair_of(layer, rotation_ref, table_ref, q, keep)

    copies[-1].wait()
    real, imag = evens(amps_ref)
    norm = energy(real, imag, 1.0)
    real, imag = turned(*looked_up(steps), real, imag)
    ranked = [plan_ref[0, ROWQ + b] for b in range(plan.row_bits)]
    row_gate = gate([(q - LANE_BITS, *pair(0, q)) for q in ranked], rows)
    lane_gate = gate(lane_bits([pair(0, q) for q in range(LANE_BITS)]), LANES)
    real, imag = by_rows(split(row_gate), real, imag)
    real, imag = by_lanes(split(lane_gate), real, imag)

    late, slots = plan_ref[0, LATE], plan.global_bits - plan_ref[0, SWAPPED]
    early = touches(plan, chain, plan_ref, late, slots, True)
    weight = early * bond_signs
    steps, signs = fields(
        [(coupling_ref[1:2, :] + 1).astype(F32) * weight, weight],
        ordered_positions(plan, chain, plan_ref), lanes, device_bits, bonds, plan.row_bits,
    )
    sums_ref[...] = in_lanes([norm, energy(real, imag, signs)])
    real, imag = turned(*looked_up(steps), real, imag)
    bits = []
    for b in range(plan.global_bits):
        leaving, i = ranked[b], plan.global_bits - 1 - b
        if i < SWAPS:
            leaving = jnp.where(b >= slots, plan_ref[0, LANEQ + i], leaving)
        bits.append((b, *pair(1, leaving, b >= late)))
    leave_gate = split(gate(bits, plan.blocks))
    whole = jnp.concatenate([real, imag], axis=0)
    held_tile = lambda part, at: whole[part * plan.blocks + at * 8 :][:8]
    swap(plan, held_tile, buffer, plan_ref)
    real, imag = by_blocks(leave_gate, buffer[:rows], buffer[rows:])
    put_blocks(out_ref, plan.blocks, 2 * plan.kept, plan.kept, real, imag)


def prepare_kernel(
    plan, rotation_ref, table_ref, plan_ref, chain_ref, coupling_ref, bond_ref,
    mode_ref, cosine_ref, sine_ref, before_ref, after_ref, late_ref, turn_ref, *gate_refs,
):
    late_rows = plan_ref[0, LATE]
    mode_ref[0, 0] = jnp.minimum(late_rows, 2)
    device = lax.axis_index("amp")
    bonds, rows, slots = plan.bonds, plan.rows, plan.global_bits
    chain = chain_ref[...]
    bond_signs = (2 * bond_ref[...] - 1).astype(F32)
    rest = bond_signs * (1.0 - touches(plan, chain, plan_ref, late_rows, slots - plan_ref[0, SWAPPED], True))
    after_trade = jnp.where(late_rows >= 2, late_rows, 0)
    late = bond_signs * touches(plan, chain, plan_ref, 0, after_trade, False)
    moved = moved_positions(plan, chain, plan_ref)
    device_bits = device << plan.local_bits
    steps, before_ref[...], after_ref[...] = fields(
        [(coupling_ref[1:2, :] + 1).astype(F32) * rest, rest, bond_signs - late],
        moved, lane_part(moved, bonds), device_bits, bonds, plan.row_bits,
    )
    cosine_ref[...], sine_ref[...] = looked_up(steps)
    (late_ref[...],) = fields([late], chain, lane_part(chain, bonds), device_bits, bonds, plan.row_bits)
    pair = lambda layer, q, keep=None: pair_of(layer, rotation_ref, table_ref, q, keep)
    ranked = [plan_ref[0, ROWQ + b] for b in range(plan.row_bits)]
    cosine, sine = pair(1, ranked[0])
    turn_ref[...] = in_lanes([cosine, jnp.where((device & 1) == 1, -sine, sine)])
    far = [plan.local_bits + b for b in range(slots)]
    lane_pairs = []
    for q in range(LANE_BITS):
        held = jnp.int32(q)
        for i in range(SWAPS):
            held = jnp.where(plan_ref[0, LANEQ + i] == q, ranked[slots - 1 - i], held)
        lane_pairs.append(pair(1, held))
    back = []
    for b in range(plan.row_bits):
        cosine, sine = pair(1, ranked[b], b < after_trade)
        back.append((ranked[b] - LANE_BITS, cosine, -sine))
    gates = [
        gate([(b, *pair(0, q)) for b, q in enumerate(far)], plan.blocks),
        gate([(b, *pair(1, q)) for b, q in enumerate(far + ranked[slots:])], rows),
        gate(lane_bits(lane_pairs), LANES),
        gate(back, rows).T,
    ]
    for k, made in enumerate(gates):
        gate_refs[2 * k][...], gate_refs[2 * k + 1][...] = split(made)


def middle(plan, state_ref, cosine_ref, sine_ref, before_ref, gates):
    ga, gb, ha, hb, la, lb = gates
    real, imag = take_blocks(state_ref, plan.blocks, 2 * plan.kept, plan.kept)
    real, imag = by_blocks((ga[...], gb[...]), real, imag)
    before = energy(real, imag, before_ref[...])
    real, imag = turned(cosine_ref[...], sine_ref[...], real, imag)
    real, imag = by_rows((ha[...], hb[...]), real, imag)
    return *by_lanes((la[...], lb[...]), real, imag), before


def pack(plan, out_ref, real, imag, sums):
    blocks, kept = plan.blocks, plan.kept
    height = 2 * kept + 1
    put_blocks(out_ref, blocks, height, kept, real, imag)
    out_ref[pl.ds(2 * kept, blocks, stride=height), :] = jnp.broadcast_to(sums, (blocks, LANES))


def middle_kernel(plan, state_ref, cosine_ref, sine_ref, before_ref, after_ref, sums_ref, *refs):
    real, imag, before = middle(plan, state_ref, cosine_ref, sine_ref, before_ref, refs[:6])
    after = energy(real, imag, after_ref[...])
    pack(plan, refs[6], real, imag, sums_ref[...] + in_lanes([F32(0.0), before, after]))


def open_kernel(plan, state_ref, cosine_ref, sine_ref, before_ref, sums_ref, *refs):
    gates, (out_ref, sums_out_ref) = refs[:6], refs[6:]
    real, imag, before = middle(plan, state_ref, cosine_ref, sine_ref, before_ref, gates)
    out_ref[...] = jnp.concatenate([real, imag], axis=0)
    sums_out_ref[...] = sums_ref[...] + in_lanes([F32(0.0), before])


def close_kernel(plan, own_ref, other_ref, turn_ref, after_ref, sums_ref, out_ref):
    both = turn_ref[0:1, 0:1] * own_ref[...] + turn_ref[0:1, 1:2] * other_ref[...]
    real, imag = both[: plan.rows], both[plan.rows :]
    after = energy(real, imag, after_ref[...])
    pack(plan, out_ref, real, imag, sums_ref[...] + in_lanes([F32(0.0), F32(0.0), after]))


def last_kernel(plan, plan_ref, state_ref, ga, gb, *refs):
    late_ref, (out_ref, energies_ref, *late_out_ref, buffer) = refs[:-3][:1], refs[-4 if len(refs) == 5 else -3 :]
    device = lax.axis_index("amp")
    blocks, kept, rows = plan.blocks, plan.kept, plan.rows
    height = 2 * kept + 1
    sums = jnp.sum(state_ref[pl.ds(2 * kept, blocks, stride=height), :], axis=0, keepdims=True)
    amps = float(2**plan.qubits)
    mean = sums[:, 0:1] / amps + 1e-06
    factor = 1.0 / jnp.sqrt(mean)
    square = factor * factor / amps
    energies_ref[...] = sums[:, 1 : 1 + LAYERS] * square

    def came(part, at):
        component, k = divmod(part, kept)
        return state_ref[pl.ds(2 * k + component + 8 * height * at, 8, stride=height), :]

    swap(plan, came, buffer, plan_ref)
    real, imag = by_rows((ga[...], gb[...]), buffer[:rows], buffer[rows:])
    if late_ref:
        late_out_ref[0][...] = in_lanes([0.0, energy(real, imag, late_ref[0][...])])[:, 0:LAYERS] * square
    ones = row_ones(plan, device)
    odd = (ones & 1) == 1
    real, imag = jnp.where(odd, imag, real), jnp.where(odd, real, imag)
    real = jnp.where(((ones + 1) & 2) == 2, -factor, factor) * real
    imag = jnp.where((ones & 2) == 2, -factor, factor) * imag
    out_ref[pl.ds(0, rows, stride=2), :] = real
    out_ref[pl.ds(1, rows, stride=2), :] = imag


def spec(space):
    return pl.BlockSpec(memory_space=space)


def call(kernel, shapes, scalars, arrays, name, spaces=None, scratch=(), near=0, held=(), far=(), plan=None):
    kept = len(arrays) - near
    arrays = tuple(
        pltpu.with_memory_space_constraint(a, pltpu.VMEM) if k >= kept else a
        for k, a in enumerate(arrays)
    )
    if plan is not None:
        scalars = (*scalars, pltpu.with_memory_space_constraint(plan, pltpu.SMEM))
    spaces = spaces or (pltpu.VMEM,) * len(shapes)
    shapes = tuple(
        spaces[k](s.shape, s.dtype) if k in held else pltpu.HBM(s.shape, s.dtype) if k in far else s
        for k, s in enumerate(shapes)
    )
    return pl.pallas_call(
        kernel,
        out_shape=shapes,
        in_specs=[spec(pltpu.SMEM)] * len(scalars) + [spec(pltpu.VMEM)] * len(arrays),
        out_specs=tuple(spec(s) for s in spaces),
        scratch_shapes=scratch,
        name=name,
    )(*scalars, *arrays)


def first_call(plan, rotation, chain, coupling, bond, state):
    sources = (rotation, chain, chain, coupling, bond, state)
    spaces = (pltpu.SMEM,) * 2 + (pltpu.VMEM,) * 4
    outs = (pltpu.VMEM, pltpu.VMEM, pltpu.SMEM)
    return pl.pallas_call(
        lambda *refs: first_kernel(plan, *refs),
        out_shape=(
            pltpu.VMEM(state.shape, F32), pltpu.VMEM((1, LANES), F32), pltpu.SMEM((1, PLAN), jnp.int32),
        ),
        in_specs=[spec(pl.ANY)] * len(sources),
        out_specs=tuple(spec(s) for s in outs),
        scratch_shapes=[pltpu.VMEM(state.shape, F32)]
        + [space(a.shape, a.dtype) for space, a in zip(spaces, sources)]
        + [pltpu.SMEM((2, ANGLES), F32), pltpu.SemaphoreType.DMA((len(sources),))],
        name="first",
    )(*sources)


def local(amplitudes, coupling_index, rotation_index, chain_order, bond_sign):
    local_bits = amplitudes.shape[1].bit_length() - 1
    size = lax.axis_size("amp")
    plan = Plan(local_bits, size.bit_length() - 1)
    rows = plan.rows
    shape = jax.ShapeDtypeStruct
    bind = lambda kernel: lambda *refs: kernel(plan, *refs)

    state = amplitudes.reshape(2, rows, LANES).transpose(1, 0, 2).reshape(2 * rows, LANES)
    table = jnp.asarray(angle_tables())
    chain, bond = chain_order.reshape(1, -1), bond_sign.reshape(1, -1)
    small = (chain, coupling_index, bond)
    whole = shape((2 * rows, LANES), F32)
    field, line = shape((rows, LANES), F32), shape((1, LANES), F32)
    square_of = lambda n: shape((n, n), BF16)
    buffer = (pltpu.VMEM((2 * rows, LANES), F32),)

    state, sums, chosen = first_call(plan, rotation_index, chain, coupling_index, bond, state)
    sizes = (size, rows, LANES, rows)
    made = call(
        bind(prepare_kernel),
        (shape((1, 1), jnp.int32),) + (field,) * 5 + (line,)
        + tuple(square_of(n) for n in sizes for _ in range(2)),
        (rotation_index, table), small, "prepare",
        (pltpu.SMEM,) + (pltpu.VMEM,) * 14, held=range(1, 15), plan=chosen,
    )
    mode, fields_made, late, turn, gates = made[0], made[1:5], made[5], made[6], made[7:]
    state = lax.all_to_all(state.reshape(size, 2 * plan.kept, LANES), "amp", 0, 0, tiled=True)
    state = state.reshape(2 * rows, LANES)
    height = 2 * plan.kept + 1
    pair = shape((1, LAYERS), F32)

    packed = (shape((size * height, LANES), F32),)

    def straight(state, sums, turn, made):
        return call(
            bind(middle_kernel), packed, (), (state, *made[:4], sums, *made[4:10]),
            "middle", near=12, held=(0,),
        )

    def paired(state, sums, turn, made):
        own, sums = call(
            bind(open_kernel), (whole, line), (),
            (state, *made[:3], sums, *made[4:10]), "open", near=11, held=(0, 1),
        )
        other = lax.ppermute(own, "amp", [(k, k ^ 1) for k in range(size)])
        return call(
            bind(close_kernel), packed, (),
            (own, other, turn, made[3], sums), "close", near=5, held=(0,),
        )

    def end(middle_of, state, sums, turn, chosen, made, *late):
        (state,) = middle_of(state, sums, turn, made)
        state = lax.all_to_all(state.reshape(size, height, 1, LANES), "amp", 0, 0, tiled=True)
        return call(
            bind(last_kernel), (whole, pair) + (pair,) * len(late), (),
            (state.reshape(size * height, LANES), *made[10:], *late), "last",
            scratch=buffer, near=3 + len(late), far=() if late else (0, 1), plan=chosen,
        )

    def apart(final):
        return final.reshape(rows, 2, LANES).transpose(1, 0, 2).reshape(2, rows * LANES)

    def none_late(*operands):
        final, energies = end(straight, *operands[:-1])
        return apart(final), energies.reshape(LAYERS)

    def one_late(*operands):
        final, energies = end(paired, *operands[:-1])
        return apart(final), energies.reshape(LAYERS)

    def more_late(*operands):
        final, energies, extra = end(straight, *operands)
        sent = jnp.broadcast_to(extra[None], (size, 1, LAYERS))
        total = energies + lax.all_to_all(sent, "amp", 0, 0, tiled=True).sum(axis=0)
        return apart(final), total.reshape(LAYERS)

    return lax.switch(
        mode[0, 0], (none_late, one_late, more_late),
        state, sums, turn, chosen, (*fields_made, *gates), late,
    )


def solution(mesh):
    in_specs = (P(None, ("rep", "amp")), P("rep", None), P("rep", None), P(), P())
    out_specs = (P(None, ("rep", "amp")), P("rep"))
    return jax.shard_map(local, mesh=mesh, in_specs=in_specs, out_specs=out_specs, check_vma=False)
```

```python
import numpy as np
import jax
import jax.numpy as jnp
from jax import lax
from jax.experimental import pallas as pl
from jax.experimental.pallas import tpu as pltpu
from jax.sharding import PartitionSpec as P

LAYERS = 2
ANGLES = 16
UNITS = 2 * (ANGLES + 1)
LANE_BITS = 7
LANES = 128

F32 = jnp.float32
BF16 = jnp.bfloat16


def angle_tables():
    steps = (np.arange(ANGLES, dtype=np.float64) + 1.0) * (np.pi / UNITS)
    return np.stack([np.cos(steps), np.sin(steps)]).astype(np.float32)


def iota(shape, dimension):
    return lax.broadcasted_iota(jnp.int32, shape, dimension)


def bit_count(values, width):
    total = values & 1
    for bit in range(1, width):
        total = total + ((values >> bit) & 1)
    return total


def split(values):
    high = values.astype(BF16)
    return high, (values - high.astype(F32)).astype(BF16)


def dot(left, right):
    return jnp.dot(left, right, preferred_element_type=F32)


def product(left, right):
    return dot(
        jnp.concatenate([left[0], left[0], left[1]], axis=1),
        jnp.concatenate([right[0], right[1], right[0]], axis=0),
    )


SWAPS = 4
ROWQ, LANEQ, SWAPPED, LATE, SPARE, PLAN = 0, 8, 12, 13, 14, 16


def gate(bits, width):
    column = iota((1, width), 1)
    lines = []
    for place, cosine, sine in bits:
        one = ((column >> place) & 1) == 1
        lines.append((jnp.where(one, sine, cosine), jnp.where(one, cosine, -sine)))
    row = iota((8, width), 0)
    matrix = None
    for bit, (zero_line, one_line) in enumerate(lines[:3]):
        factor = jnp.where(((row >> bit) & 1) == 1, one_line, zero_line)
        matrix = factor if matrix is None else matrix * factor
    for zero_line, one_line in lines[3:]:
        matrix = jnp.concatenate([matrix * zero_line, matrix * one_line], axis=0)
    return matrix


def lane_bits(pairs):
    return [(place, cosine, -sine) for place, (cosine, sine) in enumerate(pairs)]


def pair_of(layer, rotation_ref, table_ref, qubit, keep=None):
    index = rotation_ref[layer, qubit]
    cosine, sine = table_ref[0, index], table_ref[1, index]
    if keep is None:
        return cosine, sine
    return jnp.where(keep, cosine, F32(1.0)), jnp.where(keep, sine, F32(0.0))


def cos_sin(steps):
    quarter = UNITS // 2
    turns = jnp.floor(steps * (1.0 / quarter) + 0.5)
    angle = (steps - turns * quarter) * (np.pi / UNITS)
    square = angle * angle
    sine = angle * (
        1.0 + square * (-1.0 / 6 + square * (1.0 / 120 + square * (-1.0 / 5040 + square * (1.0 / 362880))))
    )
    cosine = 1.0 + square * (
        -0.5 + square * (1.0 / 24 + square * (-1.0 / 720 + square * (1.0 / 40320)))
    )
    turns = turns.astype(jnp.int32)
    odd = (turns & 1) == 1
    cosine, sine = jnp.where(odd, sine, cosine), jnp.where(odd, cosine, sine)
    return (
        jnp.where(((turns + 1) & 2) == 2, -cosine, cosine),
        jnp.where((turns & 2) == 2, -sine, sine),
    )


def looked_up(steps):
    period = 2 * UNITS
    place = (steps - period * jnp.floor(steps * (1.0 / period) + 0.25 / period)).astype(jnp.int32)
    cosine, sine = cos_sin(iota((8, LANES), 1).astype(F32))
    tiles = place.reshape(-1, 8, LANES)
    pick = lambda table: jnp.concatenate(
        [jnp.take_along_axis(table, tiles[k], axis=1, mode="promise_in_bounds") for k in range(tiles.shape[0])],
        axis=0,
    )
    return pick(cosine), pick(sine)


def turned(cosine, sine, real, imag):
    return cosine * real + sine * imag, cosine * imag - sine * real


def sign_rows(start, first, low, high, line):
    row = iota((8, start.shape[1]), 0)
    rows = jnp.broadcast_to(start, row.shape)
    for bit in range(low):
        rows = jnp.where(((row >> bit) & 1) == 1, rows * line(first + bit), rows)
    for bit in range(low, low + high):
        rows = jnp.concatenate([rows, rows * line(first + bit)], axis=0)
    return rows


def flips(positions, bonds):
    first, second = positions[:, 0:bonds], positions[:, 1 : bonds + 1]
    return lambda bit: jnp.where((first == bit) | (second == bit), F32(-1.0), F32(1.0))


def lane_part(positions, bonds):
    ones = jnp.ones((1, bonds), F32)
    return sign_rows(ones, 0, 3, LANE_BITS - 3, flips(positions, bonds)).astype(BF16)


def fields(weights, positions, lanes, device_bits, bonds, row_bits):
    differ = (device_bits >> positions[:, 0:bonds]) ^ (device_bits >> positions[:, 1 : bonds + 1])
    device_sign = (1 - 2 * (differ & 1)).astype(F32)
    line = flips(positions, bonds)
    stacked = jnp.concatenate(
        [sign_rows(w * device_sign, LANE_BITS, 3, row_bits - 3, line).astype(BF16) for w in weights],
        axis=0,
    )
    out = lax.dot_general(
        stacked, lanes, (((1,), (1,)), ((), ())), preferred_element_type=F32
    )
    rows = 2**row_bits
    return [out[k * rows : (k + 1) * rows] for k in range(len(weights))]


def energy(real, imag, field):
    values = jnp.sum(((real * real + imag * imag) * field).reshape(-1, 8, LANES), axis=0)
    return jnp.sum(jnp.sum(values, axis=0, keepdims=True), axis=1, keepdims=True)


def in_lanes(parts):
    lane = iota((1, LANES), 1)
    row = jnp.zeros((1, LANES), F32)
    for k, part in enumerate(parts):
        row = jnp.where(lane == k, part, row)
    return row


def evens(ref):
    half = ref.shape[0] // 2
    return ref[pl.ds(0, half, stride=2), :], ref[pl.ds(1, half, stride=2), :]


def take_blocks(ref, blocks, height, kept):
    def part(component):
        return jnp.concatenate(
            [ref[pl.ds(2 * k + component, blocks, stride=height), :] for k in range(kept)], axis=0
        )

    return part(0), part(1)


def put_blocks(ref, blocks, height, kept, real, imag):
    for k in range(kept):
        here = slice(k * blocks, (k + 1) * blocks)
        ref[pl.ds(2 * k, blocks, stride=height), :] = real[here]
        ref[pl.ds(2 * k + 1, blocks, stride=height), :] = imag[here]


def by_rows(gates, real, imag):
    both = product(gates, split(jnp.concatenate([real, imag], axis=1)))
    return both[:, :LANES], both[:, LANES:]


def by_blocks(gates, real, imag):
    size = gates[0].shape[0]
    pieces = [p[k : k + size] for p in (real, imag) for k in range(0, real.shape[0], size)]
    out = product(gates, split(jnp.concatenate(pieces, axis=1)))
    pieces = [out[:, k * LANES : (k + 1) * LANES] for k in range(len(pieces))]
    half = len(pieces) // 2
    return jnp.concatenate(pieces[:half], axis=0), jnp.concatenate(pieces[half:], axis=0)


def by_lanes(gates, real, imag):
    rows = real.shape[0]
    both = product(split(jnp.concatenate([real, imag], axis=0)), gates)
    return both[:rows], both[rows:]


def swap(plan, load, buffer, plan_ref):
    tiles = plan.blocks // 8
    top = tiles.bit_length() - 2
    lane, row = iota((8, LANES), 1), iota((8, LANES), 0)
    steps = []
    for i in range(SWAPS):
        taken = i < plan_ref[0, SWAPPED]
        steps.append(jnp.where(taken, jnp.left_shift(jnp.int32(1), plan_ref[0, LANEQ + i] & 7), 0))
    ones = [(lane & step) != 0 for step in steps]
    places = [lane ^ step for step in steps]
    cross = lambda value, i: jnp.take_along_axis(value, places[i], axis=1, mode="promise_in_bounds")
    for part in range(2 * plan.kept):
        values = [load(part, at) for at in range(tiles)]
        for i in range(top + 1):
            bit = 1 << (top - i)
            for low in range(tiles):
                if low & bit:
                    continue
                first, second = values[low], values[low | bit]
                crossed = cross(jnp.where(ones[i], first, second), i)
                values[low] = jnp.where(ones[i], crossed, first)
                values[low | bit] = jnp.where(ones[i], second, crossed)
        for at in range(tiles):
            buffer[pl.ds(part * plan.blocks + at * 8, 8), :] = values[at]

    @pl.when(plan_ref[0, SWAPPED] > top + 1)
    def _():
        same = ones[top + 1] == ((row & 4) != 0)
        for at in range(0, buffer.shape[0], 8):
            value = buffer[pl.ds(at, 8), :]
            buffer[pl.ds(at, 8), :] = jnp.where(same, value, cross(pltpu.roll(value, 4, 0), top + 1))


class Plan:
    def __init__(self, local_bits, global_bits):
        self.local_bits, self.global_bits = local_bits, global_bits
        self.qubits = local_bits + global_bits
        self.row_bits = local_bits - LANE_BITS
        self.rows = 2**self.row_bits
        self.blocks = 2**global_bits
        self.kept_bits = self.row_bits - global_bits
        self.kept = 2**self.kept_bits
        self.bonds = self.qubits - 1


def choose(plan, chain_ref, plan_ref):
    order = [chain_ref[0, k] for k in range(plan.qubits)]
    away = [(q >= plan.local_bits).astype(jnp.int32) for q in order]
    free = jnp.int32(0)
    for k, q in enumerate(order):
        near = away[k]
        if k:
            near = near | away[k - 1]
        if k + 1 < plan.qubits:
            near = near | away[k + 1]
        free = free | jnp.left_shift(1 - near, q)
    bit = lambda q: (free >> q) & 1
    row_qubits = range(LANE_BITS, plan.local_bits)
    free_rows = sum(bit(q) for q in row_qubits)
    slots = plan.global_bits
    free_lanes = sum(bit(q) for q in range(LANE_BITS))
    swapped = jnp.minimum(jnp.minimum(free_lanes, SWAPS), jnp.maximum(slots - free_rows, 0))
    late = jnp.maximum(slots - swapped - free_rows, 0)
    seen = jnp.int32(0)
    for k, q in enumerate(row_qubits):
        held = k - seen
        rank = jnp.where(bit(q) == 1, late + seen, jnp.where(held < late, held, free_rows + held))
        plan_ref[0, ROWQ + rank] = jnp.int32(q)
        seen = seen + bit(q)
    for i in range(SWAPS):
        plan_ref[0, LANEQ + i] = jnp.int32(-1)
    seen = jnp.int32(0)
    for q in range(LANE_BITS):
        taken = (bit(q) == 1) & (seen < swapped)
        plan_ref[0, jnp.where(taken, LANEQ + seen, SPARE)] = jnp.int32(q)
        seen = seen + bit(q)
    plan_ref[0, SWAPPED] = swapped
    plan_ref[0, LATE] = late


def touches(plan, chain, plan_ref, rows_from, rows_to, lanes):
    hit = jnp.zeros(chain.shape, jnp.int32)
    for b in range(plan.global_bits):
        wanted = (b >= rows_from) & (b < rows_to)
        hit = hit | (chain == jnp.where(wanted, plan_ref[0, ROWQ + b], -1)).astype(jnp.int32)
    if lanes:
        for i in range(SWAPS):
            hit = hit | (chain == plan_ref[0, LANEQ + i]).astype(jnp.int32)
    return (hit[:, 0 : plan.bonds] | hit[:, 1 : plan.bonds + 1]).astype(F32)


def ordered_positions(plan, chain, plan_ref):
    places = chain
    for b in range(plan.row_bits):
        places = jnp.where(chain == plan_ref[0, ROWQ + b], LANE_BITS + b, places)
    return places


def moved_positions(plan, chain, plan_ref):
    slots, swapped = plan.global_bits, plan_ref[0, SWAPPED]
    places = jnp.where(chain >= plan.local_bits, chain - plan.local_bits + LANE_BITS, chain)
    for b in range(plan.row_bits):
        target = jnp.int32(LANE_BITS + b)
        if b < slots:
            target = jnp.int32(plan.local_bits + b)
            i = slots - 1 - b
            if i < SWAPS:
                target = jnp.where(i < swapped, plan_ref[0, LANEQ + i], target)
        places = jnp.where(chain == plan_ref[0, ROWQ + b], target, places)
    for i in range(SWAPS):
        places = jnp.where(chain == plan_ref[0, LANEQ + i], plan.local_bits + slots - 1 - i, places)
    return places


def tile_ones(plan, device):
    tile = bit_count(iota((8, LANES), 0), 3) + bit_count(iota((8, LANES), 1), LANE_BITS)
    return tile + bit_count(device, plan.global_bits)


def per_tile(plan, tiles):
    return jnp.concatenate([tiles[k.bit_count() % len(tiles)] for k in range(plan.rows // 8)], axis=0)


def first_kernel(plan, *refs):
    sources, (out_ref, sums_ref, plan_ref, buffer), held = refs[:6], refs[6:10], refs[10:16]
    table_ref, semaphores = refs[16:]
    copies = [pltpu.make_async_copy(s, h, semaphores.at[k]) for k, (s, h) in enumerate(zip(sources, held))]
    for copy in copies:
        copy.start()
    for k, values in enumerate(angle_tables()):
        for at, value in enumerate(values):
            table_ref[k, at] = F32(value)
    for copy in copies[:-1]:
        copy.wait()
    rotation_ref, order_ref, chain_ref, coupling_ref, bond_ref, amps_ref = held
    device = lax.axis_index("amp")
    bonds, rows = plan.bonds, plan.rows
    choose(plan, order_ref, plan_ref)
    chain = chain_ref[...]
    device_bits = device << plan.local_bits
    bond_signs = (2 * bond_ref[...] - 1).astype(F32)
    lanes = lane_part(chain, bonds)
    (steps,) = fields(
        [(coupling_ref[0:1, :] + 1).astype(F32) * bond_signs],
        chain, lanes, device_bits, bonds, plan.row_bits,
    )
    ones = (UNITS // 2) * tile_ones(plan, device).astype(F32)
    steps = steps + per_tile(plan, [ones + (UNITS // 2) * k for k in range(4)])
    pair = lambda layer, q, keep=None: pair_of(layer, rotation_ref, table_ref, q, keep)

    copies[-1].wait()
    real, imag = evens(amps_ref)
    norm = energy(real, imag, 1.0)
    real, imag = turned(*looked_up(steps), real, imag)
    ranked = [plan_ref[0, ROWQ + b] for b in range(plan.row_bits)]
    row_gate = gate([(q - LANE_BITS, *pair(0, q)) for q in ranked], rows)
    lane_gate = gate(lane_bits([pair(0, q) for q in range(LANE_BITS)]), LANES)
    real, imag = by_rows(split(row_gate), real, imag)
    real, imag = by_lanes(split(lane_gate), real, imag)

    late, slots = plan_ref[0, LATE], plan.global_bits - plan_ref[0, SWAPPED]
    early = touches(plan, chain, plan_ref, late, slots, True)
    weight = early * bond_signs
    steps, signs = fields(
        [(coupling_ref[1:2, :] + 1).astype(F32) * weight, weight],
        ordered_positions(plan, chain, plan_ref), lanes, device_bits, bonds, plan.row_bits,
    )
    sums_ref[...] = in_lanes([norm, energy(real, imag, signs)])
    real, imag = turned(*looked_up(steps), real, imag)
    bits = []
    for b in range(plan.global_bits):
        leaving, i = ranked[b], plan.global_bits - 1 - b
        if i < SWAPS:
            leaving = jnp.where(b >= slots, plan_ref[0, LANEQ + i], leaving)
        bits.append((b, *pair(1, leaving, b >= late)))
    leave_gate = split(gate(bits, plan.blocks))
    whole = jnp.concatenate([real, imag], axis=0)
    held_tile = lambda part, at: whole[part * plan.blocks + at * 8 :][:8]
    swap(plan, held_tile, buffer, plan_ref)
    real, imag = by_blocks(leave_gate, buffer[:rows], buffer[rows:])
    put_blocks(out_ref, plan.blocks, 2 * plan.kept, plan.kept, real, imag)


def prepare_kernel(
    plan, rotation_ref, table_ref, plan_ref, chain_ref, coupling_ref, bond_ref,
    mode_ref, cosine_ref, sine_ref, before_ref, after_ref, late_ref, turn_ref, *gate_refs,
):
    late_rows = plan_ref[0, LATE]
    mode_ref[0, 0] = jnp.minimum(late_rows, 2)
    device = lax.axis_index("amp")
    bonds, rows, slots = plan.bonds, plan.rows, plan.global_bits
    chain = chain_ref[...]
    bond_signs = (2 * bond_ref[...] - 1).astype(F32)
    rest = bond_signs * (1.0 - touches(plan, chain, plan_ref, late_rows, slots - plan_ref[0, SWAPPED], True))
    after_trade = jnp.where(late_rows >= 2, late_rows, 0)
    late = bond_signs * touches(plan, chain, plan_ref, 0, after_trade, False)
    moved = moved_positions(plan, chain, plan_ref)
    device_bits = device << plan.local_bits
    steps, before_ref[...], after_ref[...] = fields(
        [(coupling_ref[1:2, :] + 1).astype(F32) * rest, rest, bond_signs - late],
        moved, lane_part(moved, bonds), device_bits, bonds, plan.row_bits,
    )
    cosine_ref[...], sine_ref[...] = looked_up(steps)
    (late_ref[...],) = fields([late], chain, lane_part(chain, bonds), device_bits, bonds, plan.row_bits)
    pair = lambda layer, q, keep=None: pair_of(layer, rotation_ref, table_ref, q, keep)
    ranked = [plan_ref[0, ROWQ + b] for b in range(plan.row_bits)]
    cosine, sine = pair(1, ranked[0])
    turn_ref[...] = in_lanes([cosine, jnp.where((device & 1) == 1, -sine, sine)])
    far = [plan.local_bits + b for b in range(slots)]
    lane_pairs = []
    for q in range(LANE_BITS):
        held = jnp.int32(q)
        for i in range(SWAPS):
            held = jnp.where(plan_ref[0, LANEQ + i] == q, ranked[slots - 1 - i], held)
        lane_pairs.append(pair(1, held))
    back = []
    for b in range(plan.row_bits):
        cosine, sine = pair(1, ranked[b], b < after_trade)
        back.append((ranked[b] - LANE_BITS, cosine, -sine))
    gates = [
        gate([(b, *pair(0, q)) for b, q in enumerate(far)], plan.blocks),
        gate([(b, *pair(1, q)) for b, q in enumerate(far + ranked[slots:])], rows),
        gate(lane_bits(lane_pairs), LANES),
        gate(back, rows).T,
    ]
    for k, made in enumerate(gates):
        gate_refs[2 * k][...], gate_refs[2 * k + 1][...] = split(made)


def middle(plan, state_ref, cosine_ref, sine_ref, before_ref, gates):
    ga, gb, ha, hb, la, lb = gates
    real, imag = take_blocks(state_ref, plan.blocks, 2 * plan.kept, plan.kept)
    real, imag = by_blocks((ga[...], gb[...]), real, imag)
    before = energy(real, imag, before_ref[...])
    real, imag = turned(cosine_ref[...], sine_ref[...], real, imag)
    real, imag = by_rows((ha[...], hb[...]), real, imag)
    return *by_lanes((la[...], lb[...]), real, imag), before


def pack(plan, out_ref, real, imag, sums):
    blocks, kept = plan.blocks, plan.kept
    height = 2 * kept + 1
    put_blocks(out_ref, blocks, height, kept, real, imag)
    out_ref[pl.ds(2 * kept, blocks, stride=height), :] = jnp.broadcast_to(sums, (blocks, LANES))


def middle_kernel(plan, state_ref, cosine_ref, sine_ref, before_ref, after_ref, sums_ref, *refs):
    real, imag, before = middle(plan, state_ref, cosine_ref, sine_ref, before_ref, refs[:6])
    after = energy(real, imag, after_ref[...])
    pack(plan, refs[6], real, imag, sums_ref[...] + in_lanes([F32(0.0), before, after]))


def open_kernel(plan, state_ref, cosine_ref, sine_ref, before_ref, sums_ref, *refs):
    gates, (out_ref, sums_out_ref) = refs[:6], refs[6:]
    real, imag, before = middle(plan, state_ref, cosine_ref, sine_ref, before_ref, gates)
    out_ref[...] = jnp.concatenate([real, imag], axis=0)
    sums_out_ref[...] = sums_ref[...] + in_lanes([F32(0.0), before])


def close_kernel(plan, own_ref, other_ref, turn_ref, after_ref, sums_ref, out_ref):
    both = turn_ref[0:1, 0:1] * own_ref[...] + turn_ref[0:1, 1:2] * other_ref[...]
    real, imag = both[: plan.rows], both[plan.rows :]
    after = energy(real, imag, after_ref[...])
    pack(plan, out_ref, real, imag, sums_ref[...] + in_lanes([F32(0.0), F32(0.0), after]))


def last_kernel(plan, plan_ref, state_ref, ga, gb, *refs):
    late_ref, (out_ref, energies_ref, *late_out_ref, buffer) = refs[:-3][:1], refs[-4 if len(refs) == 5 else -3 :]
    device = lax.axis_index("amp")
    blocks, kept, rows = plan.blocks, plan.kept, plan.rows
    height = 2 * kept + 1
    sums = jnp.sum(state_ref[pl.ds(2 * kept, blocks, stride=height), :], axis=0, keepdims=True)
    amps = float(2**plan.qubits)
    mean = sums[:, 0:1] / amps + 1e-06
    factor = 1.0 / jnp.sqrt(mean)
    square = factor * factor / amps
    energies_ref[...] = sums[:, 1 : 1 + LAYERS] * square

    def came(part, at):
        component, k = divmod(part, kept)
        return state_ref[pl.ds(2 * k + component + 8 * height * at, 8, stride=height), :]

    swap(plan, came, buffer, plan_ref)
    real, imag = by_rows((ga[...], gb[...]), buffer[:rows], buffer[rows:])
    if late_ref:
        late_out_ref[0][...] = in_lanes([0.0, energy(real, imag, late_ref[0][...])])[:, 0:LAYERS] * square
    ones = tile_ones(plan, device)
    scale = jnp.where(((ones + 1) & 2) == 2, -factor, factor)
    odd = (ones & 1) == 1
    same, other = jnp.where(odd, 0.0, scale), jnp.where(odd, scale, 0.0)
    cosine = per_tile(plan, [same, other, -same, -other])
    sine = per_tile(plan, [other, -same, -other, same])
    real, imag = turned(cosine, sine, real, imag)
    out_ref[pl.ds(0, rows, stride=2), :] = real
    out_ref[pl.ds(1, rows, stride=2), :] = imag


def spec(space):
    return pl.BlockSpec(memory_space=space)


def call(kernel, shapes, scalars, arrays, name, spaces=None, scratch=(), near=0, held=(), far=(), plan=None):
    kept = len(arrays) - near
    arrays = tuple(
        pltpu.with_memory_space_constraint(a, pltpu.VMEM) if k >= kept else a
        for k, a in enumerate(arrays)
    )
    if plan is not None:
        scalars = (*scalars, pltpu.with_memory_space_constraint(plan, pltpu.SMEM))
    spaces = spaces or (pltpu.VMEM,) * len(shapes)
    shapes = tuple(
        spaces[k](s.shape, s.dtype) if k in held else pltpu.HBM(s.shape, s.dtype) if k in far else s
        for k, s in enumerate(shapes)
    )
    return pl.pallas_call(
        kernel,
        out_shape=shapes,
        in_specs=[spec(pltpu.SMEM)] * len(scalars) + [spec(pltpu.VMEM)] * len(arrays),
        out_specs=tuple(spec(s) for s in spaces),
        scratch_shapes=scratch,
        name=name,
    )(*scalars, *arrays)


def first_call(plan, rotation, chain, coupling, bond, state):
    sources = (rotation, chain, chain, coupling, bond, state)
    spaces = (pltpu.SMEM,) * 2 + (pltpu.VMEM,) * 4
    outs = (pltpu.VMEM, pltpu.VMEM, pltpu.SMEM)
    return pl.pallas_call(
        lambda *refs: first_kernel(plan, *refs),
        out_shape=(
            pltpu.VMEM(state.shape, F32), pltpu.VMEM((1, LANES), F32), pltpu.SMEM((1, PLAN), jnp.int32),
        ),
        in_specs=[spec(pl.ANY)] * len(sources),
        out_specs=tuple(spec(s) for s in outs),
        scratch_shapes=[pltpu.VMEM(state.shape, F32)]
        + [space(a.shape, a.dtype) for space, a in zip(spaces, sources)]
        + [pltpu.SMEM((2, ANGLES), F32), pltpu.SemaphoreType.DMA((len(sources),))],
        name="first",
    )(*sources)


def local(amplitudes, coupling_index, rotation_index, chain_order, bond_sign):
    local_bits = amplitudes.shape[1].bit_length() - 1
    size = lax.axis_size("amp")
    plan = Plan(local_bits, size.bit_length() - 1)
    rows = plan.rows
    shape = jax.ShapeDtypeStruct
    bind = lambda kernel: lambda *refs: kernel(plan, *refs)

    state = amplitudes.reshape(2, rows, LANES).transpose(1, 0, 2).reshape(2 * rows, LANES)
    table = jnp.asarray(angle_tables())
    chain, bond = chain_order.reshape(1, -1), bond_sign.reshape(1, -1)
    small = (chain, coupling_index, bond)
    whole = shape((2 * rows, LANES), F32)
    field, line = shape((rows, LANES), F32), shape((1, LANES), F32)
    square_of = lambda n: shape((n, n), BF16)
    buffer = (pltpu.VMEM((2 * rows, LANES), F32),)

    state, sums, chosen = first_call(plan, rotation_index, chain, coupling_index, bond, state)
    sizes = (size, rows, LANES, rows)
    made = call(
        bind(prepare_kernel),
        (shape((1, 1), jnp.int32),) + (field,) * 5 + (line,)
        + tuple(square_of(n) for n in sizes for _ in range(2)),
        (rotation_index, table), small, "prepare",
        (pltpu.SMEM,) + (pltpu.VMEM,) * 14, held=range(1, 15), plan=chosen,
    )
    mode, fields_made, late, turn, gates = made[0], made[1:5], made[5], made[6], made[7:]
    state = lax.all_to_all(state.reshape(size, 2 * plan.kept, LANES), "amp", 0, 0, tiled=True)
    state = state.reshape(2 * rows, LANES)
    height = 2 * plan.kept + 1
    pair = shape((1, LAYERS), F32)

    packed = (shape((size * height, LANES), F32),)

    def straight(state, sums, turn, made):
        return call(
            bind(middle_kernel), packed, (), (state, *made[:4], sums, *made[4:10]),
            "middle", near=12, held=(0,),
        )

    def paired(state, sums, turn, made):
        own, sums = call(
            bind(open_kernel), (whole, line), (),
            (state, *made[:3], sums, *made[4:10]), "open", near=11, held=(0, 1),
        )
        other = lax.ppermute(own, "amp", [(k, k ^ 1) for k in range(size)])
        return call(
            bind(close_kernel), packed, (),
            (own, other, turn, made[3], sums), "close", near=5, held=(0,),
        )

    def end(middle_of, state, sums, turn, chosen, made, *late):
        (state,) = middle_of(state, sums, turn, made)
        state = lax.all_to_all(state.reshape(size, height, 1, LANES), "amp", 0, 0, tiled=True)
        return call(
            bind(last_kernel), (whole, pair) + (pair,) * len(late), (),
            (state.reshape(size * height, LANES), *made[10:], *late), "last",
            scratch=buffer, near=3 + len(late), far=() if late else (0, 1), plan=chosen,
        )

    def apart(final):
        return final.reshape(rows, 2, LANES).transpose(1, 0, 2).reshape(2, rows * LANES)

    def none_late(*operands):
        final, energies = end(straight, *operands[:-1])
        return apart(final), energies.reshape(LAYERS)

    def one_late(*operands):
        final, energies = end(paired, *operands[:-1])
        return apart(final), energies.reshape(LAYERS)

    def more_late(*operands):
        final, energies, extra = end(straight, *operands)
        sent = jnp.broadcast_to(extra[None], (size, 1, LAYERS))
        total = energies + lax.all_to_all(sent, "amp", 0, 0, tiled=True).sum(axis=0)
        return apart(final), total.reshape(LAYERS)

    return lax.switch(
        mode[0, 0], (none_late, one_late, more_late),
        state, sums, turn, chosen, (*fields_made, *gates), late,
    )


def solution(mesh):
    in_specs = (P(None, ("rep", "amp")), P("rep", None), P("rep", None), P(), P())
    out_specs = (P(None, ("rep", "amp")), P("rep"))
    return jax.shard_map(local, mesh=mesh, in_specs=in_specs, out_specs=out_specs, check_vma=False)
```

```python
import numpy as np
import jax
import jax.numpy as jnp
from jax import lax
from jax.experimental import pallas as pl
from jax.experimental.pallas import tpu as pltpu
from jax.sharding import PartitionSpec as P

LAYERS = 2
ANGLES = 16
UNITS = 2 * (ANGLES + 1)
LANE_BITS = 7
LANES = 128

F32 = jnp.float32
BF16 = jnp.bfloat16


def angle_tables():
    steps = (np.arange(ANGLES, dtype=np.float64) + 1.0) * (np.pi / UNITS)
    return np.stack([np.cos(steps), np.sin(steps)]).astype(np.float32)


def iota(shape, dimension):
    return lax.broadcasted_iota(jnp.int32, shape, dimension)


def bit_count(values, width):
    total = values & 1
    for bit in range(1, width):
        total = total + ((values >> bit) & 1)
    return total


def split(values):
    high = values.astype(BF16)
    return high, (values - high.astype(F32)).astype(BF16)


def dot(left, right):
    return jnp.dot(left, right, preferred_element_type=F32)


def product(left, right):
    return dot(
        jnp.concatenate([left[0], left[0], left[1]], axis=1),
        jnp.concatenate([right[0], right[1], right[0]], axis=0),
    )


SWAPS = 4
ROWQ, LANEQ, SWAPPED, LATE, SPARE, PLAN = 0, 8, 12, 13, 14, 16


def gate(bits, width):
    column = iota((1, width), 1)
    lines = []
    for place, cosine, sine in bits:
        one = ((column >> place) & 1) == 1
        lines.append((jnp.where(one, sine, cosine), jnp.where(one, cosine, -sine)))
    row = iota((8, width), 0)
    matrix = None
    for bit, (zero_line, one_line) in enumerate(lines[:3]):
        factor = jnp.where(((row >> bit) & 1) == 1, one_line, zero_line)
        matrix = factor if matrix is None else matrix * factor
    for zero_line, one_line in lines[3:]:
        matrix = jnp.concatenate([matrix * zero_line, matrix * one_line], axis=0)
    return matrix


def lane_bits(pairs):
    return [(place, cosine, -sine) for place, (cosine, sine) in enumerate(pairs)]


def pair_of(layer, rotation_ref, table_ref, qubit, keep=None):
    index = rotation_ref[layer, qubit]
    cosine, sine = table_ref[0, index], table_ref[1, index]
    if keep is None:
        return cosine, sine
    return jnp.where(keep, cosine, F32(1.0)), jnp.where(keep, sine, F32(0.0))


def cos_sin(steps):
    quarter = UNITS // 2
    turns = jnp.floor(steps * (1.0 / quarter) + 0.5)
    angle = (steps - turns * quarter) * (np.pi / UNITS)
    square = angle * angle
    sine = angle * (
        1.0 + square * (-1.0 / 6 + square * (1.0 / 120 + square * (-1.0 / 5040 + square * (1.0 / 362880))))
    )
    cosine = 1.0 + square * (
        -0.5 + square * (1.0 / 24 + square * (-1.0 / 720 + square * (1.0 / 40320)))
    )
    turns = turns.astype(jnp.int32)
    odd = (turns & 1) == 1
    cosine, sine = jnp.where(odd, sine, cosine), jnp.where(odd, cosine, sine)
    return (
        jnp.where(((turns + 1) & 2) == 2, -cosine, cosine),
        jnp.where((turns & 2) == 2, -sine, sine),
    )


def looked_up(steps):
    period = 2 * UNITS
    place = (steps - period * jnp.floor(steps * (1.0 / period) + 0.25 / period)).astype(jnp.int32)
    cosine, sine = cos_sin(iota((8, LANES), 1).astype(F32))
    tiles = place.reshape(-1, 8, LANES)
    pick = lambda table: jnp.concatenate(
        [jnp.take_along_axis(table, tiles[k], axis=1, mode="promise_in_bounds") for k in range(tiles.shape[0])],
        axis=0,
    )
    return pick(cosine), pick(sine)


def turned(cosine, sine, real, imag):
    return cosine * real + sine * imag, cosine * imag - sine * real


def sign_rows(start, first, low, high, line):
    row = iota((8, start.shape[1]), 0)
    rows = jnp.broadcast_to(start, row.shape)
    for bit in range(low):
        rows = jnp.where(((row >> bit) & 1) == 1, rows * line(first + bit), rows)
    for bit in range(low, low + high):
        rows = jnp.concatenate([rows, rows * line(first + bit)], axis=0)
    return rows


def flips(positions, bonds):
    first, second = positions[:, 0:bonds], positions[:, 1 : bonds + 1]
    return lambda bit: jnp.where((first == bit) | (second == bit), F32(-1.0), F32(1.0))


def lane_part(positions, bonds):
    ones = jnp.ones((1, bonds), F32)
    return sign_rows(ones, 0, 3, LANE_BITS - 3, flips(positions, bonds)).astype(BF16)


def fields(weights, positions, lanes, device_bits, bonds, row_bits):
    differ = (device_bits >> positions[:, 0:bonds]) ^ (device_bits >> positions[:, 1 : bonds + 1])
    device_sign = (1 - 2 * (differ & 1)).astype(F32)
    line = flips(positions, bonds)
    stacked = jnp.concatenate(
        [sign_rows(w * device_sign, LANE_BITS, 3, row_bits - 3, line).astype(BF16) for w in weights],
        axis=0,
    )
    out = lax.dot_general(
        stacked, lanes, (((1,), (1,)), ((), ())), preferred_element_type=F32
    )
    rows = 2**row_bits
    return [out[k * rows : (k + 1) * rows] for k in range(len(weights))]


def energy(real, imag, field):
    values = jnp.sum(((real * real + imag * imag) * field).reshape(-1, 8, LANES), axis=0)
    return jnp.sum(jnp.sum(values, axis=0, keepdims=True), axis=1, keepdims=True)


def in_lanes(parts):
    lane = iota((1, LANES), 1)
    row = jnp.zeros((1, LANES), F32)
    for k, part in enumerate(parts):
        row = jnp.where(lane == k, part, row)
    return row


def evens(ref):
    half = ref.shape[0] // 2
    return ref[pl.ds(0, half, stride=2), :], ref[pl.ds(1, half, stride=2), :]


def take_blocks(ref, blocks, height, kept):
    def part(component):
        return jnp.concatenate(
            [ref[pl.ds(2 * k + component, blocks, stride=height), :] for k in range(kept)], axis=0
        )

    return part(0), part(1)


def put_blocks(ref, blocks, height, kept, real, imag):
    for k in range(kept):
        here = slice(k * blocks, (k + 1) * blocks)
        ref[pl.ds(2 * k, blocks, stride=height), :] = real[here]
        ref[pl.ds(2 * k + 1, blocks, stride=height), :] = imag[here]


def by_rows(gates, real, imag):
    both = product(gates, split(jnp.concatenate([real, imag], axis=1)))
    return both[:, :LANES], both[:, LANES:]


def by_blocks(gates, real, imag):
    size = gates[0].shape[0]
    pieces = [p[k : k + size] for p in (real, imag) for k in range(0, real.shape[0], size)]
    out = product(gates, split(jnp.concatenate(pieces, axis=1)))
    pieces = [out[:, k * LANES : (k + 1) * LANES] for k in range(len(pieces))]
    half = len(pieces) // 2
    return jnp.concatenate(pieces[:half], axis=0), jnp.concatenate(pieces[half:], axis=0)


def by_lanes(gates, real, imag):
    rows = real.shape[0]
    both = product(split(jnp.concatenate([real, imag], axis=0)), gates)
    return both[:rows], both[rows:]


def swap(plan, load, buffer, plan_ref):
    tiles = plan.blocks // 8
    top = tiles.bit_length() - 2
    lane, row = iota((8, LANES), 1), iota((8, LANES), 0)
    steps = []
    for i in range(SWAPS):
        taken = i < plan_ref[0, SWAPPED]
        steps.append(jnp.where(taken, jnp.left_shift(jnp.int32(1), plan_ref[0, LANEQ + i] & 7), 0))
    ones = [(lane & step) != 0 for step in steps]
    places = [lane ^ step for step in steps]
    cross = lambda value, i: jnp.take_along_axis(value, places[i], axis=1, mode="promise_in_bounds")
    for part in range(2 * plan.kept):
        values = [load(part, at) for at in range(tiles)]
        for i in range(top + 1):
            bit = 1 << (top - i)
            for low in range(tiles):
                if low & bit:
                    continue
                first, second = values[low], values[low | bit]
                crossed = cross(jnp.where(ones[i], first, second), i)
                values[low] = jnp.where(ones[i], crossed, first)
                values[low | bit] = jnp.where(ones[i], second, crossed)
        for at in range(tiles):
            buffer[pl.ds(part * plan.blocks + at * 8, 8), :] = values[at]

    @pl.when(plan_ref[0, SWAPPED] > top + 1)
    def _():
        same = ones[top + 1] == ((row & 4) != 0)
        for at in range(0, buffer.shape[0], 8):
            value = buffer[pl.ds(at, 8), :]
            buffer[pl.ds(at, 8), :] = jnp.where(same, value, cross(pltpu.roll(value, 4, 0), top + 1))


class Plan:
    def __init__(self, local_bits, global_bits):
        self.local_bits, self.global_bits = local_bits, global_bits
        self.qubits = local_bits + global_bits
        self.row_bits = local_bits - LANE_BITS
        self.rows = 2**self.row_bits
        self.blocks = 2**global_bits
        self.kept_bits = self.row_bits - global_bits
        self.kept = 2**self.kept_bits
        self.bonds = self.qubits - 1


def choose(plan, chain_ref, plan_ref):
    order = [chain_ref[0, k] for k in range(plan.qubits)]
    away = [(q >= plan.local_bits).astype(jnp.int32) for q in order]
    free = jnp.int32(0)
    for k, q in enumerate(order):
        near = away[k]
        if k:
            near = near | away[k - 1]
        if k + 1 < plan.qubits:
            near = near | away[k + 1]
        free = free | jnp.left_shift(1 - near, q)
    bit = lambda q: (free >> q) & 1
    row_qubits = range(LANE_BITS, plan.local_bits)
    free_rows = sum(bit(q) for q in row_qubits)
    slots = plan.global_bits
    free_lanes = sum(bit(q) for q in range(LANE_BITS))
    swapped = jnp.minimum(jnp.minimum(free_lanes, SWAPS), jnp.maximum(slots - free_rows, 0))
    late = jnp.maximum(slots - swapped - free_rows, 0)
    seen = jnp.int32(0)
    for k, q in enumerate(row_qubits):
        held = k - seen
        rank = jnp.where(bit(q) == 1, late + seen, jnp.where(held < late, held, free_rows + held))
        plan_ref[0, ROWQ + rank] = jnp.int32(q)
        seen = seen + bit(q)
    for i in range(SWAPS):
        plan_ref[0, LANEQ + i] = jnp.int32(-1)
    seen = jnp.int32(0)
    for q in range(LANE_BITS):
        taken = (bit(q) == 1) & (seen < swapped)
        plan_ref[0, jnp.where(taken, LANEQ + seen, SPARE)] = jnp.int32(q)
        seen = seen + bit(q)
    plan_ref[0, SWAPPED] = swapped
    plan_ref[0, LATE] = late


def touches(plan, chain, plan_ref, rows_from, rows_to, lanes):
    hit = jnp.zeros(chain.shape, jnp.int32)
    for b in range(plan.global_bits):
        wanted = (b >= rows_from) & (b < rows_to)
        hit = hit | (chain == jnp.where(wanted, plan_ref[0, ROWQ + b], -1)).astype(jnp.int32)
    if lanes:
        for i in range(SWAPS):
            hit = hit | (chain == plan_ref[0, LANEQ + i]).astype(jnp.int32)
    return (hit[:, 0 : plan.bonds] | hit[:, 1 : plan.bonds + 1]).astype(F32)


def ordered_positions(plan, chain, plan_ref):
    places = chain
    for b in range(plan.row_bits):
        places = jnp.where(chain == plan_ref[0, ROWQ + b], LANE_BITS + b, places)
    return places


def moved_positions(plan, chain, plan_ref):
    slots, swapped = plan.global_bits, plan_ref[0, SWAPPED]
    places = jnp.where(chain >= plan.local_bits, chain - plan.local_bits + LANE_BITS, chain)
    for b in range(plan.row_bits):
        target = jnp.int32(LANE_BITS + b)
        if b < slots:
            target = jnp.int32(plan.local_bits + b)
            i = slots - 1 - b
            if i < SWAPS:
                target = jnp.where(i < swapped, plan_ref[0, LANEQ + i], target)
        places = jnp.where(chain == plan_ref[0, ROWQ + b], target, places)
    for i in range(SWAPS):
        places = jnp.where(chain == plan_ref[0, LANEQ + i], plan.local_bits + slots - 1 - i, places)
    return places


def tile_ones(plan, device):
    tile = bit_count(iota((8, LANES), 0), 3) + bit_count(iota((8, LANES), 1), LANE_BITS)
    return tile + bit_count(device, plan.global_bits)


def per_tile(plan, tiles):
    return jnp.concatenate([tiles[k.bit_count() % len(tiles)] for k in range(plan.rows // 8)], axis=0)


def first_kernel(plan, *refs):
    sources, (out_ref, sums_ref, plan_ref, buffer), held = refs[:6], refs[6:10], refs[10:16]
    table_ref, semaphores = refs[16:]
    copies = [pltpu.make_async_copy(s, h, semaphores.at[k]) for k, (s, h) in enumerate(zip(sources, held))]
    for copy in copies:
        copy.start()
    for k, values in enumerate(angle_tables()):
        for at, value in enumerate(values):
            table_ref[k, at] = F32(value)
    for copy in copies[:-1]:
        copy.wait()
    rotation_ref, order_ref, chain_ref, coupling_ref, bond_ref, amps_ref = held
    device = lax.axis_index("amp")
    bonds, rows = plan.bonds, plan.rows
    chain = chain_ref[...]
    device_bits = device << plan.local_bits
    bond_signs = (2 * bond_ref[...] - 1).astype(F32)
    lanes = lane_part(chain, bonds)
    (steps,) = fields(
        [(coupling_ref[0:1, :] + 1).astype(F32) * bond_signs],
        chain, lanes, device_bits, bonds, plan.row_bits,
    )
    ones = (UNITS // 2) * tile_ones(plan, device).astype(F32)
    steps = steps + per_tile(plan, [ones + (UNITS // 2) * k for k in range(4)])
    pair = lambda layer, q, keep=None: pair_of(layer, rotation_ref, table_ref, q, keep)

    choose(plan, order_ref, plan_ref)
    copies[-1].wait()
    real, imag = evens(amps_ref)
    norm = energy(real, imag, 1.0)
    real, imag = turned(*looked_up(steps), real, imag)
    ranked = [plan_ref[0, ROWQ + b] for b in range(plan.row_bits)]
    row_gate = gate([(q - LANE_BITS, *pair(0, q)) for q in ranked], rows)
    lane_gate = gate(lane_bits([pair(0, q) for q in range(LANE_BITS)]), LANES)
    real, imag = by_rows(split(row_gate), real, imag)
    real, imag = by_lanes(split(lane_gate), real, imag)

    late, slots = plan_ref[0, LATE], plan.global_bits - plan_ref[0, SWAPPED]
    early = touches(plan, chain, plan_ref, late, slots, True)
    weight = early * bond_signs
    steps, signs = fields(
        [(coupling_ref[1:2, :] + 1).astype(F32) * weight, weight],
        ordered_positions(plan, chain, plan_ref), lanes, device_bits, bonds, plan.row_bits,
    )
    sums_ref[...] = in_lanes([norm, energy(real, imag, signs)])
    real, imag = turned(*looked_up(steps), real, imag)
    bits = []
    for b in range(plan.global_bits):
        leaving, i = ranked[b], plan.global_bits - 1 - b
        if i < SWAPS:
            leaving = jnp.where(b >= slots, plan_ref[0, LANEQ + i], leaving)
        bits.append((b, *pair(1, leaving, b >= late)))
    leave_gate = split(gate(bits, plan.blocks))
    whole = jnp.concatenate([real, imag], axis=0)
    held_tile = lambda part, at: whole[part * plan.blocks + at * 8 :][:8]
    swap(plan, held_tile, buffer, plan_ref)
    real, imag = by_blocks(leave_gate, buffer[:rows], buffer[rows:])
    put_blocks(out_ref, plan.blocks, 2 * plan.kept, plan.kept, real, imag)


def prepare_kernel(
    plan, rotation_ref, table_ref, plan_ref, chain_ref, coupling_ref, bond_ref,
    mode_ref, cosine_ref, sine_ref, before_ref, after_ref, late_ref, turn_ref, *gate_refs,
):
    late_rows = plan_ref[0, LATE]
    mode_ref[0, 0] = jnp.minimum(late_rows, 2)
    device = lax.axis_index("amp")
    bonds, rows, slots = plan.bonds, plan.rows, plan.global_bits
    chain = chain_ref[...]
    bond_signs = (2 * bond_ref[...] - 1).astype(F32)
    rest = bond_signs * (1.0 - touches(plan, chain, plan_ref, late_rows, slots - plan_ref[0, SWAPPED], True))
    after_trade = jnp.where(late_rows >= 2, late_rows, 0)
    late = bond_signs * touches(plan, chain, plan_ref, 0, after_trade, False)
    moved = moved_positions(plan, chain, plan_ref)
    device_bits = device << plan.local_bits
    steps, before_ref[...], after_ref[...] = fields(
        [(coupling_ref[1:2, :] + 1).astype(F32) * rest, rest, bond_signs - late],
        moved, lane_part(moved, bonds), device_bits, bonds, plan.row_bits,
    )
    cosine_ref[...], sine_ref[...] = looked_up(steps)
    (late_ref[...],) = fields([late], chain, lane_part(chain, bonds), device_bits, bonds, plan.row_bits)
    pair = lambda layer, q, keep=None: pair_of(layer, rotation_ref, table_ref, q, keep)
    ranked = [plan_ref[0, ROWQ + b] for b in range(plan.row_bits)]
    cosine, sine = pair(1, ranked[0])
    turn_ref[...] = in_lanes([cosine, jnp.where((device & 1) == 1, -sine, sine)])
    far = [plan.local_bits + b for b in range(slots)]
    lane_pairs = []
    for q in range(LANE_BITS):
        held = jnp.int32(q)
        for i in range(SWAPS):
            held = jnp.where(plan_ref[0, LANEQ + i] == q, ranked[slots - 1 - i], held)
        lane_pairs.append(pair(1, held))
    back = []
    for b in range(plan.row_bits):
        cosine, sine = pair(1, ranked[b], b < after_trade)
        back.append((ranked[b] - LANE_BITS, cosine, -sine))
    gates = [
        gate([(b, *pair(0, q)) for b, q in enumerate(far)], plan.blocks),
        gate([(b, *pair(1, q)) for b, q in enumerate(far + ranked[slots:])], rows),
        gate(lane_bits(lane_pairs), LANES),
        gate(back, rows).T,
    ]
    for k, made in enumerate(gates):
        gate_refs[2 * k][...], gate_refs[2 * k + 1][...] = split(made)


def middle(plan, state_ref, cosine_ref, sine_ref, before_ref, gates):
    ga, gb, ha, hb, la, lb = gates
    real, imag = take_blocks(state_ref, plan.blocks, 2 * plan.kept, plan.kept)
    real, imag = by_blocks((ga[...], gb[...]), real, imag)
    before = energy(real, imag, before_ref[...])
    real, imag = turned(cosine_ref[...], sine_ref[...], real, imag)
    real, imag = by_rows((ha[...], hb[...]), real, imag)
    return *by_lanes((la[...], lb[...]), real, imag), before


def pack(plan, out_ref, real, imag, sums):
    blocks, kept = plan.blocks, plan.kept
    height = 2 * kept + 1
    put_blocks(out_ref, blocks, height, kept, real, imag)
    out_ref[pl.ds(2 * kept, blocks, stride=height), :] = jnp.broadcast_to(sums, (blocks, LANES))


def middle_kernel(plan, state_ref, cosine_ref, sine_ref, before_ref, after_ref, sums_ref, *refs):
    real, imag, before = middle(plan, state_ref, cosine_ref, sine_ref, before_ref, refs[:6])
    after = energy(real, imag, after_ref[...])
    pack(plan, refs[6], real, imag, sums_ref[...] + in_lanes([F32(0.0), before, after]))


def open_kernel(plan, state_ref, cosine_ref, sine_ref, before_ref, sums_ref, *refs):
    gates, (out_ref, sums_out_ref) = refs[:6], refs[6:]
    real, imag, before = middle(plan, state_ref, cosine_ref, sine_ref, before_ref, gates)
    out_ref[...] = jnp.concatenate([real, imag], axis=0)
    sums_out_ref[...] = sums_ref[...] + in_lanes([F32(0.0), before])


def close_kernel(plan, own_ref, other_ref, turn_ref, after_ref, sums_ref, out_ref):
    both = turn_ref[0:1, 0:1] * own_ref[...] + turn_ref[0:1, 1:2] * other_ref[...]
    real, imag = both[: plan.rows], both[plan.rows :]
    after = energy(real, imag, after_ref[...])
    pack(plan, out_ref, real, imag, sums_ref[...] + in_lanes([F32(0.0), F32(0.0), after]))


def last_kernel(plan, plan_ref, state_ref, ga, gb, *refs):
    late_ref, (out_ref, energies_ref, *late_out_ref, buffer) = refs[:-3][:1], refs[-4 if len(refs) == 5 else -3 :]
    device = lax.axis_index("amp")
    blocks, kept, rows = plan.blocks, plan.kept, plan.rows
    height = 2 * kept + 1
    sums = jnp.sum(state_ref[pl.ds(2 * kept, blocks, stride=height), :], axis=0, keepdims=True)
    amps = float(2**plan.qubits)
    mean = sums[:, 0:1] / amps + 1e-06
    factor = 1.0 / jnp.sqrt(mean)
    square = factor * factor / amps
    energies_ref[...] = sums[:, 1 : 1 + LAYERS] * square

    def came(part, at):
        component, k = divmod(part, kept)
        return state_ref[pl.ds(2 * k + component + 8 * height * at, 8, stride=height), :]

    swap(plan, came, buffer, plan_ref)
    real, imag = by_rows((ga[...], gb[...]), buffer[:rows], buffer[rows:])
    if late_ref:
        late_out_ref[0][...] = in_lanes([0.0, energy(real, imag, late_ref[0][...])])[:, 0:LAYERS] * square
    ones = tile_ones(plan, device)
    scale = jnp.where(((ones + 1) & 2) == 2, -factor, factor)
    odd = (ones & 1) == 1
    same, other = jnp.where(odd, 0.0, scale), jnp.where(odd, scale, 0.0)
    cosine = per_tile(plan, [same, other, -same, -other])
    sine = per_tile(plan, [other, -same, -other, same])
    real, imag = turned(cosine, sine, real, imag)
    out_ref[pl.ds(0, rows, stride=2), :] = real
    out_ref[pl.ds(1, rows, stride=2), :] = imag


def spec(space):
    return pl.BlockSpec(memory_space=space)


def call(kernel, shapes, scalars, arrays, name, spaces=None, scratch=(), near=0, held=(), far=(), plan=None):
    kept = len(arrays) - near
    arrays = tuple(
        pltpu.with_memory_space_constraint(a, pltpu.VMEM) if k >= kept else a
        for k, a in enumerate(arrays)
    )
    if plan is not None:
        scalars = (*scalars, pltpu.with_memory_space_constraint(plan, pltpu.SMEM))
    spaces = spaces or (pltpu.VMEM,) * len(shapes)
    shapes = tuple(
        spaces[k](s.shape, s.dtype) if k in held else pltpu.HBM(s.shape, s.dtype) if k in far else s
        for k, s in enumerate(shapes)
    )
    return pl.pallas_call(
        kernel,
        out_shape=shapes,
        in_specs=[spec(pltpu.SMEM)] * len(scalars) + [spec(pltpu.VMEM)] * len(arrays),
        out_specs=tuple(spec(s) for s in spaces),
        scratch_shapes=scratch,
        name=name,
    )(*scalars, *arrays)


def first_call(plan, rotation, chain, coupling, bond, state):
    sources = (rotation, chain, chain, coupling, bond, state)
    spaces = (pltpu.SMEM,) * 2 + (pltpu.VMEM,) * 4
    outs = (pltpu.VMEM, pltpu.VMEM, pltpu.SMEM)
    return pl.pallas_call(
        lambda *refs: first_kernel(plan, *refs),
        out_shape=(
            pltpu.VMEM(state.shape, F32), pltpu.VMEM((1, LANES), F32), pltpu.SMEM((1, PLAN), jnp.int32),
        ),
        in_specs=[spec(pl.ANY)] * len(sources),
        out_specs=tuple(spec(s) for s in outs),
        scratch_shapes=[pltpu.VMEM(state.shape, F32)]
        + [space(a.shape, a.dtype) for space, a in zip(spaces, sources)]
        + [pltpu.SMEM((2, ANGLES), F32), pltpu.SemaphoreType.DMA((len(sources),))],
        name="first",
    )(*sources)


def local(amplitudes, coupling_index, rotation_index, chain_order, bond_sign):
    local_bits = amplitudes.shape[1].bit_length() - 1
    size = lax.axis_size("amp")
    plan = Plan(local_bits, size.bit_length() - 1)
    rows = plan.rows
    shape = jax.ShapeDtypeStruct
    bind = lambda kernel: lambda *refs: kernel(plan, *refs)

    state = amplitudes.reshape(2, rows, LANES).transpose(1, 0, 2).reshape(2 * rows, LANES)
    table = jnp.asarray(angle_tables())
    chain, bond = chain_order.reshape(1, -1), bond_sign.reshape(1, -1)
    small = (chain, coupling_index, bond)
    whole = shape((2 * rows, LANES), F32)
    field, line = shape((rows, LANES), F32), shape((1, LANES), F32)
    square_of = lambda n: shape((n, n), BF16)
    buffer = (pltpu.VMEM((2 * rows, LANES), F32),)

    state, sums, chosen = first_call(plan, rotation_index, chain, coupling_index, bond, state)
    sizes = (size, rows, LANES, rows)
    made = call(
        bind(prepare_kernel),
        (shape((1, 1), jnp.int32),) + (field,) * 5 + (line,)
        + tuple(square_of(n) for n in sizes for _ in range(2)),
        (rotation_index, table), small, "prepare",
        (pltpu.SMEM,) + (pltpu.VMEM,) * 14, held=range(1, 15), plan=chosen,
    )
    mode, fields_made, late, turn, gates = made[0], made[1:5], made[5], made[6], made[7:]
    state = lax.all_to_all(state.reshape(size, 2 * plan.kept, LANES), "amp", 0, 0, tiled=True)
    state = state.reshape(2 * rows, LANES)
    height = 2 * plan.kept + 1
    pair = shape((1, LAYERS), F32)

    packed = (shape((size * height, LANES), F32),)

    def straight(state, sums, turn, made):
        return call(
            bind(middle_kernel), packed, (), (state, *made[:4], sums, *made[4:10]),
            "middle", near=12, held=(0,),
        )

    def paired(state, sums, turn, made):
        own, sums = call(
            bind(open_kernel), (whole, line), (),
            (state, *made[:3], sums, *made[4:10]), "open", near=11, held=(0, 1),
        )
        other = lax.ppermute(own, "amp", [(k, k ^ 1) for k in range(size)])
        return call(
            bind(close_kernel), packed, (),
            (own, other, turn, made[3], sums), "close", near=5, held=(0,),
        )

    def end(middle_of, state, sums, turn, chosen, made, *late):
        (state,) = middle_of(state, sums, turn, made)
        state = lax.all_to_all(state.reshape(size, height, 1, LANES), "amp", 0, 0, tiled=True)
        return call(
            bind(last_kernel), (whole, pair) + (pair,) * len(late), (),
            (state.reshape(size * height, LANES), *made[10:], *late), "last",
            scratch=buffer, near=3 + len(late), far=() if late else (0, 1), plan=chosen,
        )

    def apart(final):
        return final.reshape(rows, 2, LANES).transpose(1, 0, 2).reshape(2, rows * LANES)

    def none_late(*operands):
        final, energies = end(straight, *operands[:-1])
        return apart(final), energies.reshape(LAYERS)

    def one_late(*operands):
        final, energies = end(paired, *operands[:-1])
        return apart(final), energies.reshape(LAYERS)

    def more_late(*operands):
        final, energies, extra = end(straight, *operands)
        sent = jnp.broadcast_to(extra[None], (size, 1, LAYERS))
        total = energies + lax.all_to_all(sent, "amp", 0, 0, tiled=True).sum(axis=0)
        return apart(final), total.reshape(LAYERS)

    return lax.switch(
        mode[0, 0], (none_late, one_late, more_late),
        state, sums, turn, chosen, (*fields_made, *gates), late,
    )


def solution(mesh):
    in_specs = (P(None, ("rep", "amp")), P("rep", None), P("rep", None), P(), P())
    out_specs = (P(None, ("rep", "amp")), P("rep"))
    return jax.shard_map(local, mesh=mesh, in_specs=in_specs, out_specs=out_specs, check_vma=False)
```
